32 devices in a mesh: gx: 2 (over y), gy: 8 (over z, core), gz: 2 (over x).
Axes of the slice: x: 2, y: 2, z: 4, core: 2. Of those that a mesh axis runs over, the one named last changes fastest.
Arguments:
- starting_kelvin: float32 [16, 32, 2048], P(None, 'gx', ('gy', 'gz')), may hold values from -6 to 6
- substance_label: int32 [16, 32, 2048], P(None, 'gx', ('gy', 'gz')), may hold values from 0 to 3
- voxel_source_patch: int32 [16, 32, 2048], P(None, 'gx', ('gy', 'gz')), may hold values from 0 to 15
- substance_traits: float32 [4, 4], replicated, may hold values from 0.5 to 2
- patch_source_intensity: float32 [16], replicated, may hold values from 0 to 8
Outputs:
- warmed_result: float32 [16, 32, 2048], P(None, 'gx', ('gy', 'gz'))
- solution: float32 [3, 16, 32, 2048], P(None, 'gz', 'gx', 'gy')
- residual: float32 [3, 16, 32, 2048], P(None, 'gz', 'gx', 'gy')
The draws below stay inside these ranges and needn't reach their ends.
All inputs are finite; a program needn't handle non-finite values.
Results may differ from the reference program's by a relative error of at most 0.0029.
Values sent between devices are 32-bit elements; how exact they have to be, the bound alone decides.
No kernel may reach another device: no remote copies, remote signals or barrier semaphores. Data moves between devices by JAX's collectives and lax.ppermute only.
A program may use at most 64 MiB of HBM per device.

```python
import math
import jax
import jax.numpy as jnp

HEIGHT_VOXELS = 16
MATS = 4
TILES = 16
HEAT_STEPS = 2
ITERS = 3
LATERAL_DEPTH = 32
LATERAL_WIDTH = 2048


def with_ends(entries, own_key, low, high):
    longest = entries.shape.index(max(entries.shape))
    spots = []
    for shift in (0, 1):
        where = [jax.random.randint(jax.random.fold_in(own_key, axis), (), 0, length) for axis, length in enumerate(entries.shape)]
        where[longest] = (where[longest] + shift) % entries.shape[longest]
        spots.append(tuple(where))
    return entries.at[spots[0]].set(low).at[spots[1]].set(high)


def shard_levels(key, shape, shards, least, top_value):
    def one(dim, shards_of):
        steps = jax.random.uniform(jax.random.fold_in(jax.random.fold_in(key, 6), dim), (shards_of,), jnp.float32, least / len(shards), top_value / len(shards))
        return jnp.repeat(jnp.exp(steps), shape[dim] // shards_of).reshape((-1,) + (1,) * (len(shape) - dim - 1))

    gain = one(*shards[0])
    for cut in shards[1:]:
        gain = gain * one(*cut)
    return gain


def scatter_about(stream_key, extent, spread, limit, cuts=(), held_as=jnp.bfloat16):
    entries = spread * jax.random.normal(stream_key, extent, jnp.float32)
    if cuts:
        entries = entries * shard_levels(stream_key, extent, cuts, -0.22, 0.18)
    return jnp.clip(entries, -limit, limit).astype(held_as)


def setup_inputs(seed: int = 0) -> dict:
    arg_keys = jax.random.split(jax.random.key(seed), 6)
    return {
        "starting_kelvin": scatter_about(arg_keys[0], (HEIGHT_VOXELS, LATERAL_DEPTH, LATERAL_WIDTH), 1.0, 6.0, ((1, 2), (2, 16)), jnp.float32),
        "substance_label": with_ends(jax.random.randint(arg_keys[1], (HEIGHT_VOXELS, LATERAL_DEPTH, LATERAL_WIDTH), 0, MATS), jax.random.fold_in(arg_keys[1], 1), 0, MATS - 1).astype(jnp.int32),
        "voxel_source_patch": with_ends(jax.random.randint(arg_keys[2], (HEIGHT_VOXELS, LATERAL_DEPTH, LATERAL_WIDTH), 0, TILES), jax.random.fold_in(arg_keys[2], 1), 0, TILES - 1).astype(jnp.int32),
        "substance_traits": jnp.clip(jnp.exp(jax.random.uniform(arg_keys[3], (4, MATS), jnp.float32, math.log(0.5), math.log(2.0))), 0.5, 2.0),
        "patch_source_intensity": jnp.clip(jax.random.uniform(arg_keys[4], (TILES,), jnp.float32, 0.0, 8.0), 0.0, 8.0),
    }


time_step = 0.03
anchor_scale = 0.5
strain_gain = 2.0


def lookup(identity, table, count):
    summed = jnp.zeros(identity.shape, jnp.float32)
    for number in range(count):
        summed = summed + jnp.where(identity == number, table[number], jnp.float32(0.0))
    return summed


def conduct(own, other):
    return 2.0 * own * other / jnp.maximum(own + other, 0.25)


def heat_step(padded_temp, padded_cond, power, inverse_cap):
    centre = padded_temp[:, 1:-1, 1:-1]
    own = padded_cond[:, 1:-1, 1:-1]
    layers, rows, columns = centre.shape
    heat_flux = jnp.zeros_like(centre)
    for row_offset, column_offset in ((0, 1), (2, 1), (1, 0), (1, 2)):
        neighbour = padded_temp[:, row_offset:row_offset + rows, column_offset:column_offset + columns]
        other = padded_cond[:, row_offset:row_offset + rows, column_offset:column_offset + columns]
        heat_flux = heat_flux + conduct(own, other) * (neighbour - centre)
    vertical_temp = jnp.pad(centre, ((1, 1), (0, 0), (0, 0)))
    vertical_cond = jnp.pad(own, ((1, 1), (0, 0), (0, 0)))
    for layer_offset in (0, 2):
        other = vertical_cond[layer_offset:layer_offset + layers]
        neighbour = vertical_temp[layer_offset:layer_offset + layers]
        heat_flux = heat_flux + conduct(own, other) * (neighbour - centre)
    return centre + time_step * inverse_cap * (heat_flux + power)


def neighbour_offsets():
    listed = []
    for along_z in (-1, 0, 1):
        for along_x in (-1, 0, 1):
            for along_y in (-1, 0, 1):
                if along_z != 0 or along_x != 0 or along_y != 0:
                    listed.append((along_z, along_x, along_y))
    return listed


def apply_operator(field, padded_field, modulus, padded_modulus):
    layers, rows, columns = modulus.shape
    parts = [anchor_scale * modulus * field[0], anchor_scale * modulus * field[1], anchor_scale * modulus * field[2]]
    for along_z, along_x, along_y in neighbour_offsets():
        length_sq = along_z * along_z + along_x * along_x + along_y * along_y
        window = (slice(1 + along_z, 1 + along_z + layers), slice(1 + along_x, 1 + along_x + rows), slice(1 + along_y, 1 + along_y + columns))
        weight = (0.5 / length_sq) * (modulus + padded_modulus[window])
        change = [field[index_c] - padded_field[index_c][window] for index_c in range(3)]
        projected = (along_z * change[0] + along_x * change[1] + along_y * change[2]) / length_sq
        for index_c, direction_part in enumerate((along_z, along_x, along_y)):
            parts[index_c] = parts[index_c] + weight * (0.5 * change[index_c] + direction_part * projected)
    return jnp.stack(parts)


def thermal_load(modulus, padded_modulus, strain, padded_strain):
    layers, rows, columns = modulus.shape
    parts = [jnp.zeros_like(modulus), jnp.zeros_like(modulus), jnp.zeros_like(modulus)]
    for along_z, along_x, along_y in neighbour_offsets():
        length_sq = along_z * along_z + along_x * along_x + along_y * along_y
        window = (slice(1 + along_z, 1 + along_z + layers), slice(1 + along_x, 1 + along_x + rows), slice(1 + along_y, 1 + along_y + columns))
        weight = (0.5 / length_sq) * (modulus + padded_modulus[window])
        pushing = weight * (0.5 * (strain + padded_strain[window]))
        for index_c, direction_part in enumerate((along_z, along_x, along_y)):
            if direction_part != 0:
                parts[index_c] = parts[index_c] - strain_gain * direction_part * pushing
    return jnp.stack(parts)


def reference(starting_kelvin, substance_label, voxel_source_patch, substance_traits, patch_source_intensity):
    diffusive_coefficient = lookup(substance_label, substance_traits[0], MATS)
    inverse_cap = 1.0 / lookup(substance_label, substance_traits[1], MATS)
    power = lookup(voxel_source_patch, patch_source_intensity, TILES)
    cycle = ((0, 0), (1, 1), (1, 1))
    padded_cond = jnp.pad(diffusive_coefficient, cycle)
    warmed_result = starting_kelvin
    for number in range(HEAT_STEPS):
        warmed_result = heat_step(jnp.pad(warmed_result, cycle), padded_cond, power, inverse_cap)
    modulus = lookup(substance_label, substance_traits[2], MATS)
    strain = lookup(substance_label, substance_traits[3], MATS) * warmed_result
    padded_modulus = jnp.pad(modulus, 1)
    load = thermal_load(modulus, padded_modulus, strain, jnp.pad(strain, 1))
    solution = jnp.zeros_like(load)
    residual = load
    direction = load
    norm_now = jnp.sum(residual * residual)
    shell = ((0, 0), (1, 1), (1, 1), (1, 1))
    for number in range(ITERS):
        image = apply_operator(direction, jnp.pad(direction, shell), modulus, padded_modulus)
        alpha = norm_now / jnp.sum(direction * image)
        solution = solution + alpha * direction
        residual = residual - alpha * image
        norm_next = jnp.sum(residual * residual)
        direction = residual + (norm_next / norm_now) * direction
        norm_now = norm_next
    return warmed_result, solution, residual
```

```python
import functools

import jax
import jax.numpy as jnp
from jax import lax
from jax.experimental import pallas as pl
from jax.experimental.pallas import tpu as pltpu
from jax.sharding import PartitionSpec as P

ITERS = 3
HEAT_STEPS = 2
HALO = 8
LANES = 128
PAD = 8
AXES = ("gx", "gy", "gz")

time_step = 0.03
anchor_scale = 0.5
strain_gain = 2.0
CENTRE = 55.0 / 9.0

f32 = jnp.float32


def half_roll(x):
    return pltpu.roll(x, LANES // 2, 1)


def lane_of(shape):
    return lax.broadcasted_iota(jnp.int32, shape, 1)


def pack_rows_kernel(where_ref, temp, label, patch, out):
    layers, rows, _ = temp.shape
    half = layers // 2
    theirs = 1 - where_ref[2]
    lane = lane_of((rows, LANES))
    in_half = (lane // (LANES // 2)) == theirs
    base = LANES // 2 - HALO * theirs
    for a, ref in enumerate((temp, label, patch)):
        for l in range(half):
            low = ref[l].astype(f32)
            high = ref[l + half].astype(f32)
            out[a, l] = jnp.where(in_half, low, half_roll(high))
        near = jnp.zeros((rows, LANES), f32)
        for l in range(layers):
            moved = pltpu.roll(ref[l].astype(f32), (HALO * l - base) % LANES, 1)
            near = jnp.where((lane // HALO) == l, moved, near)
        out[a, half] = near


def pack_far_kernel(where_ref, temp, label, patch, got, out):
    layers, rows, _ = temp.shape
    half = layers // 2
    gx = where_ref[0]
    pos = where_ref[2]
    lane = lane_of((rows, LANES))
    base = (LANES - HALO) * pos
    own = pl.multiple_of(gx * rows, rows)
    other = pl.multiple_of((1 - gx) * rows, rows)
    for a, ref in enumerate((temp, label, patch)):
        mine = jnp.zeros((rows, LANES), f32)
        theirs = jnp.zeros((rows, LANES), f32)
        for l in range(layers):
            here = (lane // HALO) == l
            moved = pltpu.roll(ref[l].astype(f32), (HALO * l - base) % LANES, 1)
            mine = jnp.where(here, moved, mine)
            extra = 0 if l < half else LANES // 2
            moved = pltpu.roll(got[a, l % half], (HALO * l - base + extra) % LANES, 1)
            theirs = jnp.where(here, moved, theirs)
        out[a, pl.ds(own, rows), :] = mine
        out[a, pl.ds(other, rows), :] = theirs


def picks(ref, index, l, row):
    def at(dz, dx):
        if index is None:
            return ref[l + 1 + dz, PAD + row + dx : PAD + row + dx + 8, :]
        return ref[index[0], index[1], l + 1 + dz, PAD + row + dx : PAD + row + dx + 8, :]

    out = {}
    for dx in (-1, 0, 1):
        up, mid, down = at(1, dx), at(0, dx), at(-1, dx)
        out["F", dx] = mid
        out["G", dx] = up + down
        out["H", dx] = up - down
    res = {}
    for k in "FGH":
        res[k] = out[k, 0]
        res["E" + k] = out[k, 1] + out[k, -1]
        res["D" + k] = out[k, 1] - out[k, -1]
    return res


def along_lanes(base, even, odd):
    total = base
    if odd is None:
        return total + pltpu.roll(even, LANES - 1, 1) + pltpu.roll(even, 1, 1)
    if even is None:
        return total + pltpu.roll(odd, LANES - 1, 1) - pltpu.roll(odd, 1, 1)
    return total + pltpu.roll(even + odd, LANES - 1, 1) + pltpu.roll(even - odd, 1, 1)


S9 = 5.0 / 36.0
S18 = 1.0 / 18.0
S6 = 1.0 / 6.0


def full_stencil(z, x, y):
    base0 = 0.25 * (z["EF"] + z["EG"]) + 0.75 * z["G"] + 0.125 * x["DH"]
    even0 = 0.25 * (z["F"] + z["G"]) + 0.125 * z["EF"] + S9 * z["EG"] + S18 * x["DH"]
    odd0 = 0.125 * y["H"] + S18 * y["EH"]
    base1 = 0.75 * x["EF"] + 0.25 * (x["G"] + x["EG"]) + 0.125 * z["DH"]
    even1 = 0.25 * (x["F"] + x["EF"]) + 0.125 * x["G"] + S9 * x["EG"] + S18 * z["DH"]
    odd1 = 0.125 * y["DF"] + S18 * y["DG"]
    base2 = 0.25 * (y["EF"] + y["G"]) + 0.125 * y["EG"]
    even2 = 0.75 * y["F"] + 0.25 * (y["EF"] + y["G"]) + S9 * y["EG"]
    odd2 = 0.125 * (x["DF"] + z["H"]) + S18 * (x["DG"] + z["EH"])
    return (
        along_lanes(base0, even0, odd0),
        along_lanes(base1, even1, odd1),
        along_lanes(base2, even2, odd2),
    )


def matrix_stencil(m):
    zz = along_lanes(
        0.25 * (m["EF"] + m["EG"]) + 0.75 * m["G"],
        0.25 * (m["F"] + m["G"]) + 0.125 * m["EF"] + S9 * m["EG"],
        None,
    )
    xx = along_lanes(
        0.75 * m["EF"] + 0.25 * (m["G"] + m["EG"]),
        0.25 * (m["F"] + m["EF"]) + 0.125 * m["G"] + S9 * m["EG"],
        None,
    )
    yy = along_lanes(
        0.25 * (m["EF"] + m["G"]) + 0.125 * m["EG"],
        0.75 * m["F"] + 0.25 * (m["EF"] + m["G"]) + S9 * m["EG"],
        None,
    )
    zx = along_lanes(0.125 * m["DH"], S18 * m["DH"], None)
    odd_zy = 0.125 * m["H"] + S18 * m["EH"]
    odd_xy = 0.125 * m["DF"] + S18 * m["DG"]
    zy = pltpu.roll(odd_zy, LANES - 1, 1) - pltpu.roll(odd_zy, 1, 1)
    xy = pltpu.roll(odd_xy, LANES - 1, 1) - pltpu.roll(odd_xy, 1, 1)
    return zz, xx, yy, zx, zy, xy


def gradient_stencil(f):
    gz = along_lanes(0.5 * f["H"] + 0.25 * f["EH"], 0.25 * f["H"] + S6 * f["EH"], None)
    gx = along_lanes(0.5 * f["DF"] + 0.25 * f["DG"], 0.25 * f["DF"] + S6 * f["DG"], None)
    odd = 0.5 * f["F"] + 0.25 * (f["G"] + f["EF"]) + S6 * f["EG"]
    gy = pltpu.roll(odd, LANES - 1, 1) - pltpu.roll(odd, 1, 1)
    return gz, gx, gy


def conduct(own, other):
    return 2.0 * own * other / jnp.maximum(own + other, 0.25)


def choose(label, values):
    out = jnp.zeros(label.shape, f32)
    for k, v in enumerate(values):
        out = jnp.where(label == float(k), v, out)
    return out


def solve_kernel(
    where_ref, traits, intensity, temp, label, patch, got, far,
    warm_out, v_out, mom_out,
    cond, temp_a, temp_b, cap, power, gz, gx, gy, mod, expand, strain, prod, mats, inside, u, w,
):
    layers, rows, _ = temp.shape
    full = far.shape[1]
    half = layers // 2
    me = where_ref[0]
    pos = where_ref[2]
    paired = where_ref[3] > 0
    tiles = range(0, full, 8)
    count = traits.shape[1]
    sources = intensity.shape[0]
    own = pl.multiple_of(me * rows, rows)
    other = pl.multiple_of((1 - me) * rows, rows)
    near_base = LANES // 2 - HALO * pos
    far_base = (LANES - HALO) * (1 - pos)
    lane_r = lane_of((rows, LANES))
    near_lanes = (lane_r // HALO) == (near_base // HALO)
    lane_f = lane_of((full, LANES))
    far_lanes = (lane_f // HALO) == (far_base // HALO)

    mean_mod = traits[2, 0]
    for k in range(1, count):
        mean_mod = mean_mod + traits[2, k]
    scale = jnp.full((8, LANES), mean_mod * ((anchor_scale + 2.0 * CENTRE) / count), f32)
    inv_scale = 1.0 / scale
    cond_t = [traits[0, k] for k in range(count)]
    cap_t = [time_step / jnp.full((8, LANES), traits[1, k], f32) for k in range(count)]
    mod_t = [traits[2, k] for k in range(count)]
    exp_t = [traits[3, k] for k in range(count)]
    pow_t = [intensity[k] for k in range(sources)]

    zero_tile = jnp.zeros((full + 2 * PAD, LANES), f32)
    for ref in (cond, temp_a, temp_b, mod, strain, prod):
        ref[0] = zero_tile
        ref[layers + 1] = zero_tile
    for ref in (u, w):
        for b in range(ref.shape[0]):
            for c in range(3):
                ref[b, c, 0] = zero_tile
                ref[b, c, layers + 1] = zero_tile
    gz[0] = jnp.zeros((full, LANES), f32)
    edge = jnp.zeros((PAD, LANES), f32)

    def window(l, _):
        for ref in (cond, temp_a, temp_b, mod, strain, prod, gx):
            ref[l + 1, 0:PAD] = edge
            ref[l + 1, PAD + full : 2 * PAD + full] = edge
        for ref in (u, w):
            for b in range(ref.shape[0]):
                for c in range(3):
                    ref[b, c, l + 1, 0:PAD] = edge
                    ref[b, c, l + 1, PAD + full : 2 * PAD + full] = edge
        for a, (ref, dest) in enumerate(((temp, temp_a), (label, temp_b), (patch, cond))):
            mine = ref[l].astype(f32)
            packed = got[a, lax.rem(l, half)]
            theirs = jnp.where(l < half, packed, half_roll(packed))
            near = pltpu.roll(got[a, half], (near_base - HALO * l + 2 * LANES) % LANES, 1)
            theirs = jnp.where(near_lanes, near, theirs)
            dest[l + 1, pl.ds(PAD + own, rows), :] = mine
            dest[l + 1, pl.ds(PAD + other, rows), :] = theirs
            edge_cols = pltpu.roll(far[a], (far_base - HALO * l + 2 * LANES) % LANES, 1)
            if a == 1:
                edge_cols = jnp.where(paired, edge_cols, -1.0)
            old = dest[l + 1, PAD : PAD + full, :]
            dest[l + 1, PAD : PAD + full, :] = jnp.where(far_lanes, edge_cols, old)
        for r in tiles:
            here = slice(PAD + r, PAD + r + 8)
            there = slice(r, r + 8)
            lab = temp_b[l + 1, here, :]
            src = cond[l + 1, here, :]
            cond[l + 1, here, :] = choose(lab, cond_t)
            cap[l, there, :] = choose(lab, cap_t)
            mod[l + 1, here, :] = choose(lab, mod_t)
            expand[l, there, :] = choose(lab, exp_t)
            power[l, there, :] = choose(src, pow_t)
            if r == 0:
                inside[...] = jnp.where(lab >= 0.0, 1.0, 0.0)
        return 0

    lax.fori_loop(0, layers, window, 0)

    def faces(l, _):
        for r in tiles:
            here = slice(PAD + r, PAD + r + 8)
            a = cond[l + 1, here, :]
            gz[l + 1, r : r + 8, :] = conduct(a, cond[l + 2, here, :])
            gx[l + 1, here, :] = conduct(a, cond[l + 1, PAD + r + 1 : PAD + r + 9, :])
            gy[l, r : r + 8, :] = conduct(a, pltpu.roll(a, LANES - 1, 1))
        return 0

    lax.fori_loop(0, layers, faces, 0)

    def heat(src, dst, last):
        def step(l, _):
            for r in tiles:
                here = slice(PAD + r, PAD + r + 8)
                there = slice(r, r + 8)
                t = src[l + 1, here, :]
                flux = gz[l + 1, there, :] * (src[l + 2, here, :] - t)
                flux += gz[l, there, :] * (src[l, here, :] - t)
                flux += gx[l + 1, here, :] * (src[l + 1, PAD + r + 1 : PAD + r + 9, :] - t)
                flux += gx[l + 1, PAD + r - 1 : PAD + r + 7, :] * (
                    src[l + 1, PAD + r - 1 : PAD + r + 7, :] - t
                )
                side = gy[l, there, :] * (pltpu.roll(t, LANES - 1, 1) - t)
                flux += side - pltpu.roll(side, 1, 1)
                new = t + cap[l, there, :] * (flux + power[l, there, :])
                if last:
                    warm_out[l, there, :] = new
                    s = expand[l, there, :] * new
                    strain[l + 1, here, :] = s
                    prod[l + 1, here, :] = s * mod[l + 1, here, :]
                else:
                    dst[l + 1, here, :] = new
            return 0

        lax.fori_loop(0, layers, step, 0)

    heat(temp_a, temp_b, False)
    heat(temp_b, None, True)

    mine8 = (lane_of((8, LANES)) // (LANES // 2)) == pos

    def loads(l, acc):
        for r in tiles:
            here = slice(PAD + r, PAD + r + 8)
            there = slice(r, r + 8)
            s = picks(strain, None, l, r)
            m = picks(mod, None, l, r)
            q = picks(prod, None, l, r)
            gs, gm, gq = gradient_stencil(s), gradient_stencil(m), gradient_stencil(q)
            for k, entry in enumerate(matrix_stencil(m)):
                mats[k, l, there, :] = entry * inv_scale
            keep = inside[...]
            for c in range(3):
                v = (-0.5 * strain_gain) * (m["F"] * gs[c] + s["F"] * gm[c] + gq[c]) * keep
                u[0, c, l + 1, here, :] = v
                w[0, c, l + 1, here, :] = v * m["F"]
                v_out[0, c, l, there, :] = v
                acc = acc + jnp.where(mine8, v * v, 0.0)
        return acc

    zero = jnp.zeros((8, LANES), f32)
    moments = [lax.fori_loop(0, layers, loads, zero)]

    def power_step(number, src, dst):
        def step(l, accs):
            cross, square = accs
            for r in tiles:
                here = slice(PAD + r, PAD + r + 8)
                there = slice(r, r + 8)
                uz, ux, uy = (picks(u, (src, c), l, r) for c in range(3))
                old = (uz["F"], ux["F"], uy["F"])
                cu = full_stencil(uz, ux, uy)
                wz, wx, wy = (picks(w, (src, c), l, r) for c in range(3))
                weighted = (wz["F"], wx["F"], wy["F"])
                cw = full_stencil(wz, wx, wy)
                zz, xx, yy, zx, zy, xy = (mats[k, l, there, :] for k in range(6))
                mixed = (
                    zz * old[0] + zx * old[1] + zy * old[2],
                    zx * old[0] + xx * old[1] + xy * old[2],
                    zy * old[0] + xy * old[1] + yy * old[2],
                )
                m = mod[l + 1, here, :]
                keep = inside[...]
                for c in range(3):
                    inner = (anchor_scale + CENTRE) * weighted[c] - m * cu[c] - cw[c]
                    v = (inner * inv_scale + mixed[c] - old[c]) * keep
                    v_out[number, c, l, there, :] = v
                    if dst is not None:
                        u[dst, c, l + 1, here, :] = v
                        w[dst, c, l + 1, here, :] = v * m
                    own_v = jnp.where(mine8, v, 0.0)
                    cross = cross + own_v * old[c]
                    square = square + own_v * own_v
            return cross, square

        return lax.fori_loop(0, layers, step, (zero, zero))

    for number in range(1, ITERS + 1):
        src = (number - 1) % 2
        dst = number % 2 if number < ITERS else None
        cross, square = power_step(number, src, dst)
        moments.append(cross)
        if number < ITERS:
            moments.append(square)

    lane1 = lane_of((1, LANES))
    row = jnp.zeros((1, LANES), f32)
    for k, part in enumerate(moments):
        row = jnp.where(lane1 == k, jnp.sum(part), row)
    for k in range(mom_out.shape[0]):
        mom_out[k] = row


def coefficients(mu, scale):
    def inner(a, b):
        total = None
        for i, x in enumerate(a):
            for j, y in enumerate(b):
                term = x * y * mu[i + j]
                total = term if total is None else total + term
        return total

    def added(a, b):
        out = []
        for k in range(max(len(a), len(b))):
            if k >= len(a):
                out.append(b[k])
            elif k >= len(b):
                out.append(a[k])
            else:
                out.append(a[k] + b[k])
        return out

    one = jnp.ones_like(mu[0])
    residual = [one]
    direction = [one]
    solution = []
    norm = mu[0]
    for number in range(ITERS):
        image = added(direction, [jnp.zeros_like(one)] + direction)
        alpha = norm / inner(direction, image)
        solution = added(solution, [alpha * d for d in direction])
        residual = added(residual, [-alpha * d for d in image])
        if number + 1 < ITERS:
            following = inner(residual, residual)
            ratio = following / norm
            direction = added(residual, [ratio * d for d in direction])
            norm = following
    return [s / scale for s in solution], residual


def combine_kernel(where_ref, traits, mom, v, warm, *outs):
    layers, full, _ = warm.shape
    rows = outs[0].shape[1]
    half = layers // 2
    quarter = half // 2
    gx, gz, pos = where_ref[0], where_ref[1], where_ref[2]
    total = jnp.sum(mom[:, 0, :], axis=0, keepdims=True)
    lane1 = lane_of((1, LANES))
    shape = (8, LANES)
    mu = [
        jnp.full(shape, jnp.sum(jnp.where(lane1 == k, total, 0.0)), f32) for k in range(2 * ITERS)
    ]
    count = traits.shape[1]
    mean_mod = traits[2, 0]
    for k in range(1, count):
        mean_mod = mean_mod + traits[2, k]
    scale = jnp.full(shape, mean_mod * ((anchor_scale + 2.0 * CENTRE) / count), f32)
    sol, res = coefficients(mu, scale)
    in_half = (lane_of(shape) // (LANES // 2)) == pos

    for number, out in enumerate(outs):
        dx, dz = number % 2, number // 2
        row0 = pl.multiple_of((gx ^ dx) * rows, rows)
        layer0 = (gz ^ dz) * half

        def piece(l, _, out=out, row0=row0, layer0=layer0):
            for r in range(0, rows, 8):
                for c in range(3):
                    made = []
                    for ll in (l, l + quarter):
                        vs = [v[k, c, layer0 + ll, pl.ds(row0 + r, 8), :] for k in range(ITERS + 1)]
                        x = sol[0] * vs[0]
                        y = res[0] * vs[0]
                        for k in range(1, ITERS + 1):
                            if k < ITERS:
                                x = x + sol[k] * vs[k]
                            y = y + res[k] * vs[k]
                        made.append((x, y))
                    for which in (0, 1):
                        out[(3 * which + c) * quarter + l, r : r + 8, :] = jnp.where(
                            in_half, made[0][which], half_roll(made[1][which])
                        )
            return 0

        lax.fori_loop(0, quarter, piece, 0)
        if dz == 0:
            for l in range(half):
                for r in range(0, rows, 8):
                    low = warm[l, pl.ds(row0 + r, 8), :]
                    high = warm[l + half, pl.ds(row0 + r, 8), :]
                    out[6 * quarter + l, r : r + 8, :] = jnp.where(in_half, low, half_roll(high))


def place_kernel(where_ref, mine, over_x, over_z, over_both, warm_out, sol_out, res_out):
    layers, rows, _ = warm_out.shape
    half = layers // 2
    quarter = half // 2
    gz, pos = where_ref[1], where_ref[2]
    half_of = lane_of((rows, LANES)) // (LANES // 2)
    for block, (a, b, p) in enumerate(((mine, over_x, pos), (over_z, over_both, 1 - pos))):
        first = half_of == p
        lanes = pl.ds(pl.multiple_of((gz ^ block) * LANES, LANES), LANES)
        for which, out in enumerate((sol_out, res_out)):
            for c in range(3):
                for l in range(quarter):
                    x = a[(3 * which + c) * quarter + l]
                    y = b[(3 * which + c) * quarter + l]
                    out[c, l, :, lanes] = jnp.where(first, x, y)
                    out[c, l + quarter, :, lanes] = half_roll(jnp.where(first, y, x))
        if block == 0:
            for l in range(half):
                x = a[6 * quarter + l]
                y = b[6 * quarter + l]
                warm_out[l] = jnp.where(first, x, y)
                warm_out[l + half] = half_roll(jnp.where(first, y, x))


def vmem():
    return pl.BlockSpec(memory_space=pltpu.VMEM)


def smem():
    return pl.BlockSpec(memory_space=pltpu.SMEM)


def per_device_fast(temp, label, patch, traits, intensity):
    nx, ny, nz = (lax.axis_size(a) for a in AXES)
    layers, rows, width = temp.shape
    full = rows * nx
    half = layers // 2
    quarter = half // 2
    devices = nx * ny * nz
    gx, gy, gz = (lax.axis_index(a) for a in AXES)
    pos = gx ^ gz
    block = gy * nz + gz
    paired = jnp.where(pos == 0, block > 0, block < ny * nz - 1)
    where_am = jnp.stack([gx, gz, pos, paired.astype(jnp.int32)]).astype(jnp.int32)

    def number(x, b):
        return x * ny * nz + b

    def everywhere(dx, dz):
        return [
            (number(x, y * nz + z), number(x ^ dx, y * nz + (z ^ dz)))
            for x in range(nx) for y in range(ny) for z in range(nz)
        ]

    def side(x, b):
        return x ^ (b % nz)

    chain = []
    for b in range(1, ny * nz):
        left = [x for x in range(nx) if side(x, b - 1) == 1][0]
        right = [x for x in range(nx) if side(x, b) == 0][0]
        chain += [(number(left, b - 1), number(right, b)), (number(right, b), number(left, b - 1))]

    sds = lambda *s: jax.ShapeDtypeStruct(s, f32)
    send = pl.pallas_call(
        pack_rows_kernel,
        out_shape=sds(3, half + 1, rows, LANES),
        in_specs=[smem(), vmem(), vmem(), vmem()],
        out_specs=vmem(),
        name="pack_rows",
    )(where_am, temp, label, patch)
    got = lax.ppermute(send, AXES, everywhere(1, 0))
    send = pl.pallas_call(
        pack_far_kernel,
        out_shape=sds(3, full, LANES),
        in_specs=[smem(), vmem(), vmem(), vmem(), vmem()],
        out_specs=vmem(),
        name="pack_far",
    )(where_am, temp, label, patch, got)
    far = lax.ppermute(send, AXES, chain)

    padded = pltpu.VMEM((layers + 2, full + 2 * PAD, LANES), f32)
    plain = pltpu.VMEM((layers, full, LANES), f32)
    vectors = pltpu.VMEM((2, 3, layers + 2, full + 2 * PAD, LANES), f32)
    warm, v, mom = pl.pallas_call(
        solve_kernel,
        out_shape=(
            sds(layers, full, LANES),
            sds(ITERS + 1, 3, layers, full, LANES),
            sds(devices, 1, LANES),
        ),
        in_specs=[smem(), smem(), smem(), vmem(), vmem(), vmem(), vmem(), vmem()],
        out_specs=(vmem(), vmem(), vmem()),
        scratch_shapes=[
            padded, padded, padded, plain, plain,
            pltpu.VMEM((layers + 1, full, LANES), f32), padded, plain,
            padded, plain, padded, padded,
            pltpu.VMEM((6, layers, full, LANES), f32),
            pltpu.VMEM((8, LANES), f32),
            vectors, vectors,
        ],
        name="solve",
    )(where_am, traits, intensity, temp, label, patch, got, far)
    mom = lax.all_to_all(mom, AXES, 0, 0, tiled=True)
    big = 6 * quarter + half
    mine, to_x, to_z, to_both = pl.pallas_call(
        combine_kernel,
        out_shape=(
            sds(big, rows, LANES), sds(big, rows, LANES),
            sds(6 * quarter, rows, LANES), sds(6 * quarter, rows, LANES),
        ),
        in_specs=[smem(), smem(), vmem(), vmem(), vmem()],
        out_specs=(vmem(),) * 4,
        name="combine",
    )(where_am, traits, mom, v, warm)
    from_x = lax.ppermute(to_x, AXES, everywhere(1, 0))
    from_z = lax.ppermute(to_z, AXES, everywhere(0, 1))
    from_both = lax.ppermute(to_both, AXES, everywhere(1, 1))
    return pl.pallas_call(
        place_kernel,
        out_shape=(
            sds(layers, rows, width),
            sds(3, half, rows, nz * width),
            sds(3, half, rows, nz * width),
        ),
        in_specs=[smem(), vmem(), vmem(), vmem(), vmem()],
        out_specs=(vmem(),) * 3,
        name="place",
    )(where_am, mine, from_x, from_z, from_both)


def padded(value, sides, width):
    for axis, dim in sides:
        devices, length = (lax.axis_size(axis), value.shape[dim])
        up = [(i, (i + 1) % devices) for i in range(devices - 1)]
        down = [(j, i) for i, j in up]
        last = lax.slice_in_dim(value, length - width, length, axis=dim)
        initial = lax.slice_in_dim(value, 0, width, axis=dim)
        before = lax.ppermute(last, axis, up)
        after = lax.ppermute(initial, axis, down)
        value = jnp.concatenate([before, value, after], axis=dim)
    return value


def lookup(identity, table, count):
    summed = jnp.zeros(identity.shape, jnp.float32)
    for number in range(count):
        summed = summed + jnp.where(identity == number, table[number], jnp.float32(0.0))
    return summed


def heat_step(padded_temp, padded_cond, power, inverse_cap):
    centre = padded_temp[:, 1:-1, 1:-1]
    own = padded_cond[:, 1:-1, 1:-1]
    layers, rows, columns = centre.shape
    heat_flux = jnp.zeros_like(centre)
    for row_offset, column_offset in ((0, 1), (2, 1), (1, 0), (1, 2)):
        neighbour = padded_temp[
            :, row_offset : row_offset + rows, column_offset : column_offset + columns
        ]
        other = padded_cond[
            :, row_offset : row_offset + rows, column_offset : column_offset + columns
        ]
        heat_flux = heat_flux + conduct(own, other) * (neighbour - centre)
    vertical_temp = jnp.pad(centre, ((1, 1), (0, 0), (0, 0)))
    vertical_cond = jnp.pad(own, ((1, 1), (0, 0), (0, 0)))
    for layer_offset in (0, 2):
        other = vertical_cond[layer_offset : layer_offset + layers]
        neighbour = vertical_temp[layer_offset : layer_offset + layers]
        heat_flux = heat_flux + conduct(own, other) * (neighbour - centre)
    return centre + time_step * inverse_cap * (heat_flux + power)


def neighbour_offsets():
    listed = []
    for along_z in (-1, 0, 1):
        for along_x in (-1, 0, 1):
            for along_y in (-1, 0, 1):
                if along_z != 0 or along_x != 0 or along_y != 0:
                    listed.append((along_z, along_x, along_y))
    return listed


def apply_operator(field, padded_field, modulus, padded_modulus):
    layers, rows, columns = modulus.shape
    parts = [
        anchor_scale * modulus * field[0],
        anchor_scale * modulus * field[1],
        anchor_scale * modulus * field[2],
    ]
    for along_z, along_x, along_y in neighbour_offsets():
        length_sq = along_z * along_z + along_x * along_x + along_y * along_y
        window = (
            slice(1 + along_z, 1 + along_z + layers),
            slice(1 + along_x, 1 + along_x + rows),
            slice(1 + along_y, 1 + along_y + columns),
        )
        weight = 0.5 / length_sq * (modulus + padded_modulus[window])
        change = [field[index_c] - padded_field[index_c][window] for index_c in range(3)]
        projected = (along_z * change[0] + along_x * change[1] + along_y * change[2]) / length_sq
        for index_c, direction_part in enumerate((along_z, along_x, along_y)):
            parts[index_c] = parts[index_c] + weight * (
                0.5 * change[index_c] + direction_part * projected
            )
    return jnp.stack(parts)


def thermal_load(modulus, padded_modulus, strain, padded_strain):
    layers, rows, columns = modulus.shape
    parts = [jnp.zeros_like(modulus), jnp.zeros_like(modulus), jnp.zeros_like(modulus)]
    for along_z, along_x, along_y in neighbour_offsets():
        length_sq = along_z * along_z + along_x * along_x + along_y * along_y
        window = (
            slice(1 + along_z, 1 + along_z + layers),
            slice(1 + along_x, 1 + along_x + rows),
            slice(1 + along_y, 1 + along_y + columns),
        )
        weight = 0.5 / length_sq * (modulus + padded_modulus[window])
        pushing = weight * (0.5 * (strain + padded_strain[window]))
        for index_c, direction_part in enumerate((along_z, along_x, along_y)):
            if direction_part != 0:
                parts[index_c] = parts[index_c] - strain_gain * direction_part * pushing
    return jnp.stack(parts)


def two_products(residual, image):
    return lax.psum((jnp.sum(residual * residual), jnp.sum(residual * image)), ("gx", "gy", "gz"))


def per_device_plain(
    starting_kelvin, substance_label, voxel_source_patch, substance_traits, patch_source_intensity
):
    count = substance_traits.shape[1]
    diffusive_coefficient = lookup(substance_label, substance_traits[0], count)
    inverse_cap = 1.0 / lookup(substance_label, substance_traits[1], count)
    power = lookup(voxel_source_patch, patch_source_intensity, patch_source_intensity.shape[0])
    padded_array = padded(
        jnp.stack([starting_kelvin, diffusive_coefficient]), (("gx", 2), (("gy", "gz"), 3)), 1
    )
    padded_cond = padded_array[1]
    warmed_result = heat_step(padded_array[0], padded_cond, power, inverse_cap)
    number = 0
    extended = padded(warmed_result, (("gx", 1), (("gy", "gz"), 2)), 1)
    warmed_result = heat_step(extended, padded_cond, power, inverse_cap)
    modulus = lookup(substance_label, substance_traits[2], count)
    strain = lookup(substance_label, substance_traits[3], count) * warmed_result
    fields = jnp.stack([modulus, strain])
    vertical_cycle = ((0, 0), (1, 1), (0, 0), (0, 0))
    padded_fields = jnp.pad(padded(fields, (("gx", 2), (("gy", "gz"), 3)), 1), vertical_cycle)

    def extend(field):
        return jnp.pad(padded(field, (("gx", 2), (("gy", "gz"), 3)), 1), vertical_cycle)

    modulus = fields[0]
    padded_modulus = padded_fields[0]
    load = thermal_load(modulus, padded_modulus, fields[1], padded_fields[1])

    def operate(field):
        return apply_operator(field, extend(field), modulus, padded_modulus)

    solution = jnp.zeros_like(load)
    residual = load
    image = operate(residual)
    norm_now, product = two_products(residual, image)
    alpha = norm_now / product
    direction, along_image = (residual, image)
    for number in range(ITERS):
        solution = solution + alpha * direction
        residual = residual - alpha * along_image
        if number + 1 < ITERS:
            image = operate(residual)
            norm_next, product = two_products(residual, image)
            ratio = norm_next / norm_now
            alpha = norm_next / (product - ratio * norm_next / alpha)
            direction = residual + ratio * direction
            along_image = image + ratio * along_image
            norm_now = norm_next
    joined = lax.all_to_all(
        jnp.concatenate([solution, residual]), "gz", split_axis=1, concat_axis=3, tiled=True
    )
    solution = joined[:3]
    residual = joined[3:]
    return (warmed_result, solution, residual)


def solution(mesh):
    in_specs = (
        P(None, "gx", ("gy", "gz")),
        P(None, "gx", ("gy", "gz")),
        P(None, "gx", ("gy", "gz")),
        P(),
        P(),
    )
    out_specs = (P(None, "gx", ("gy", "gz")), P(None, "gz", "gx", "gy"), P(None, "gz", "gx", "gy"))

    def per_device(temp, label, patch, traits, intensity):
        layers, rows, width = temp.shape
        fits = (
            mesh.shape["gx"] == 2
            and mesh.shape["gz"] == 2
            and width == LANES
            and layers % 4 == 0
            and layers * HALO <= LANES
            and rows % 8 == 0
        )
        run = per_device_fast if fits else per_device_plain
        return run(temp, label, patch, traits, intensity)

    return jax.shard_map(
        per_device, mesh=mesh, in_specs=in_specs, out_specs=out_specs, check_vma=False
    )
```

```python
import functools

import jax
import jax.numpy as jnp
from jax import lax
from jax.experimental import pallas as pl
from jax.experimental.pallas import tpu as pltpu
from jax.sharding import PartitionSpec as P

ITERS = 3
HEAT_STEPS = 2
HALO = 8
LANES = 128
PAD = 8
AXES = ("gx", "gy", "gz")

time_step = 0.03
anchor_scale = 0.5
strain_gain = 2.0
CENTRE = 55.0 / 9.0

f32 = jnp.float32


def half_roll(x):
    return pltpu.roll(x, LANES // 2, 1)


def lane_of(shape):
    return lax.broadcasted_iota(jnp.int32, shape, 1)


def pack_rows_kernel(where_ref, temp, label, patch, out):
    layers, rows, _ = temp.shape
    half = layers // 2
    theirs = 1 - where_ref[2]
    lane = lane_of((rows, LANES))
    in_half = (lane // (LANES // 2)) == theirs
    base = LANES // 2 - HALO * theirs
    for a, ref in enumerate((temp, label, patch)):
        for l in range(half):
            low = ref[l].astype(f32)
            high = ref[l + half].astype(f32)
            out[a, l] = jnp.where(in_half, low, half_roll(high))
        near = jnp.zeros((rows, LANES), f32)
        for l in range(layers):
            moved = pltpu.roll(ref[l].astype(f32), (HALO * l - base) % LANES, 1)
            near = jnp.where((lane // HALO) == l, moved, near)
        out[a, half] = near


def pack_far_kernel(where_ref, temp, label, patch, got, out):
    layers, rows, _ = temp.shape
    half = layers // 2
    gx = where_ref[0]
    pos = where_ref[2]
    lane = lane_of((rows, LANES))
    base = (LANES - HALO) * pos
    own = pl.multiple_of(gx * rows, rows)
    other = pl.multiple_of((1 - gx) * rows, rows)
    for a, ref in enumerate((temp, label, patch)):
        mine = jnp.zeros((rows, LANES), f32)
        theirs = jnp.zeros((rows, LANES), f32)
        for l in range(layers):
            here = (lane // HALO) == l
            moved = pltpu.roll(ref[l].astype(f32), (HALO * l - base) % LANES, 1)
            mine = jnp.where(here, moved, mine)
            extra = 0 if l < half else LANES // 2
            moved = pltpu.roll(got[a, l % half], (HALO * l - base + extra) % LANES, 1)
            theirs = jnp.where(here, moved, theirs)
        out[a, pl.ds(own, rows), :] = mine
        out[a, pl.ds(other, rows), :] = theirs


def picks(ref, index, l, row):
    def at(dz, dx):
        if index is None:
            return ref[l + 1 + dz, PAD + row + dx : PAD + row + dx + 8, :]
        return ref[index[0], index[1], l + 1 + dz, PAD + row + dx : PAD + row + dx + 8, :]

    out = {}
    for dx in (-1, 0, 1):
        up, mid, down = at(1, dx), at(0, dx), at(-1, dx)
        out["F", dx] = mid
        out["G", dx] = up + down
        out["H", dx] = up - down
    res = {}
    for k in "FGH":
        res[k] = out[k, 0]
        res["E" + k] = out[k, 1] + out[k, -1]
        res["D" + k] = out[k, 1] - out[k, -1]
    return res


def along_lanes(base, even, odd):
    total = base
    if odd is None:
        return total + pltpu.roll(even, LANES - 1, 1) + pltpu.roll(even, 1, 1)
    if even is None:
        return total + pltpu.roll(odd, LANES - 1, 1) - pltpu.roll(odd, 1, 1)
    return total + pltpu.roll(even + odd, LANES - 1, 1) + pltpu.roll(even - odd, 1, 1)


S9 = 5.0 / 36.0
S18 = 1.0 / 18.0
S6 = 1.0 / 6.0


def full_stencil(z, x, y):
    base0 = 0.25 * (z["EF"] + z["EG"]) + 0.75 * z["G"] + 0.125 * x["DH"]
    even0 = 0.25 * (z["F"] + z["G"]) + 0.125 * z["EF"] + S9 * z["EG"] + S18 * x["DH"]
    odd0 = 0.125 * y["H"] + S18 * y["EH"]
    base1 = 0.75 * x["EF"] + 0.25 * (x["G"] + x["EG"]) + 0.125 * z["DH"]
    even1 = 0.25 * (x["F"] + x["EF"]) + 0.125 * x["G"] + S9 * x["EG"] + S18 * z["DH"]
    odd1 = 0.125 * y["DF"] + S18 * y["DG"]
    base2 = 0.25 * (y["EF"] + y["G"]) + 0.125 * y["EG"]
    even2 = 0.75 * y["F"] + 0.25 * (y["EF"] + y["G"]) + S9 * y["EG"]
    odd2 = 0.125 * (x["DF"] + z["H"]) + S18 * (x["DG"] + z["EH"])
    return (
        along_lanes(base0, even0, odd0),
        along_lanes(base1, even1, odd1),
        along_lanes(base2, even2, odd2),
    )


def matrix_stencil(m):
    zz = along_lanes(
        0.25 * (m["EF"] + m["EG"]) + 0.75 * m["G"],
        0.25 * (m["F"] + m["G"]) + 0.125 * m["EF"] + S9 * m["EG"],
        None,
    )
    xx = along_lanes(
        0.75 * m["EF"] + 0.25 * (m["G"] + m["EG"]),
        0.25 * (m["F"] + m["EF"]) + 0.125 * m["G"] + S9 * m["EG"],
        None,
    )
    yy = along_lanes(
        0.25 * (m["EF"] + m["G"]) + 0.125 * m["EG"],
        0.75 * m["F"] + 0.25 * (m["EF"] + m["G"]) + S9 * m["EG"],
        None,
    )
    zx = along_lanes(0.125 * m["DH"], S18 * m["DH"], None)
    odd_zy = 0.125 * m["H"] + S18 * m["EH"]
    odd_xy = 0.125 * m["DF"] + S18 * m["DG"]
    zy = pltpu.roll(odd_zy, LANES - 1, 1) - pltpu.roll(odd_zy, 1, 1)
    xy = pltpu.roll(odd_xy, LANES - 1, 1) - pltpu.roll(odd_xy, 1, 1)
    return zz, xx, yy, zx, zy, xy


def gradient_stencil(f):
    gz = along_lanes(0.5 * f["H"] + 0.25 * f["EH"], 0.25 * f["H"] + S6 * f["EH"], None)
    gx = along_lanes(0.5 * f["DF"] + 0.25 * f["DG"], 0.25 * f["DF"] + S6 * f["DG"], None)
    odd = 0.5 * f["F"] + 0.25 * (f["G"] + f["EF"]) + S6 * f["EG"]
    gy = pltpu.roll(odd, LANES - 1, 1) - pltpu.roll(odd, 1, 1)
    return gz, gx, gy


def conduct(own, other):
    return 2.0 * own * other / jnp.maximum(own + other, 0.25)


def choose(label, values):
    out = jnp.zeros(label.shape, f32)
    for k, v in enumerate(values):
        out = jnp.where(label == float(k), v, out)
    return out


def solve_kernel(
    where_ref, traits, intensity, temp, label, patch, got, far,
    warm_out, v_out, mom_out,
    cond, temp_a, temp_b, cap, power, gz, gx, gy, mod, expand, strain, prod, mats, inside, u, w,
):
    layers, rows, _ = temp.shape
    full = far.shape[1]
    half = layers // 2
    me = where_ref[0]
    pos = where_ref[2]
    paired = where_ref[3] > 0
    tiles = range(0, full, 8)
    count = traits.shape[1]
    sources = intensity.shape[0]
    own = pl.multiple_of(me * rows, rows)
    other = pl.multiple_of((1 - me) * rows, rows)
    near_base = LANES // 2 - HALO * pos
    far_base = (LANES - HALO) * (1 - pos)
    lane_r = lane_of((rows, LANES))
    near_lanes = (lane_r // HALO) == (near_base // HALO)
    lane_f = lane_of((full, LANES))
    far_lanes = (lane_f // HALO) == (far_base // HALO)

    mean_mod = traits[2, 0]
    for k in range(1, count):
        mean_mod = mean_mod + traits[2, k]
    scale = jnp.full((8, LANES), mean_mod * ((anchor_scale + 2.0 * CENTRE) / count), f32)
    inv_scale = 1.0 / scale
    cond_t = [traits[0, k] for k in range(count)]
    cap_t = [time_step / jnp.full((8, LANES), traits[1, k], f32) for k in range(count)]
    mod_t = [traits[2, k] for k in range(count)]
    exp_t = [traits[3, k] for k in range(count)]
    pow_t = [intensity[k] for k in range(sources)]

    zero_tile = jnp.zeros((full + 2 * PAD, LANES), f32)
    for ref in (cond, temp_a, temp_b, mod, strain, prod):
        ref[0] = zero_tile
        ref[layers + 1] = zero_tile
    for ref in (u, w):
        for b in range(ref.shape[0]):
            for c in range(3):
                ref[b, c, 0] = zero_tile
                ref[b, c, layers + 1] = zero_tile
    gz[0] = jnp.zeros((full, LANES), f32)
    edge = jnp.zeros((PAD, LANES), f32)

    def window(l, _):
        for ref in (cond, temp_a, temp_b, mod, strain, prod, gx):
            ref[l + 1, 0:PAD] = edge
            ref[l + 1, PAD + full : 2 * PAD + full] = edge
        for ref in (u, w):
            for b in range(ref.shape[0]):
                for c in range(3):
                    ref[b, c, l + 1, 0:PAD] = edge
                    ref[b, c, l + 1, PAD + full : 2 * PAD + full] = edge
        for a, (ref, dest) in enumerate(((temp, temp_a), (label, temp_b), (patch, cond))):
            mine = ref[l].astype(f32)
            packed = got[a, lax.rem(l, half)]
            theirs = jnp.where(l < half, packed, half_roll(packed))
            near = pltpu.roll(got[a, half], (near_base - HALO * l + 2 * LANES) % LANES, 1)
            theirs = jnp.where(near_lanes, near, theirs)
            dest[l + 1, pl.ds(PAD + own, rows), :] = mine
            dest[l + 1, pl.ds(PAD + other, rows), :] = theirs
            edge_cols = pltpu.roll(far[a], (far_base - HALO * l + 2 * LANES) % LANES, 1)
            if a == 1:
                edge_cols = jnp.where(paired, edge_cols, -1.0)
            old = dest[l + 1, PAD : PAD + full, :]
            dest[l + 1, PAD : PAD + full, :] = jnp.where(far_lanes, edge_cols, old)
        for r in tiles:
            here = slice(PAD + r, PAD + r + 8)
            there = slice(r, r + 8)
            lab = temp_b[l + 1, here, :]
            src = cond[l + 1, here, :]
            cond[l + 1, here, :] = choose(lab, cond_t)
            cap[l, there, :] = choose(lab, cap_t)
            mod[l + 1, here, :] = choose(lab, mod_t)
            expand[l, there, :] = choose(lab, exp_t)
            power[l, there, :] = choose(src, pow_t)
            if r == 0:
                inside[...] = jnp.where(lab >= 0.0, 1.0, 0.0)
        return 0

    lax.fori_loop(0, layers, window, 0)

    def faces(l, _):
        for r in tiles:
            here = slice(PAD + r, PAD + r + 8)
            a = cond[l + 1, here, :]
            gz[l + 1, r : r + 8, :] = conduct(a, cond[l + 2, here, :])
            gx[l + 1, here, :] = conduct(a, cond[l + 1, PAD + r + 1 : PAD + r + 9, :])
            gy[l, r : r + 8, :] = conduct(a, pltpu.roll(a, LANES - 1, 1))
        return 0

    lax.fori_loop(0, layers, faces, 0)

    def heat(src, dst, last):
        def step(l, _):
            for r in tiles:
                here = slice(PAD + r, PAD + r + 8)
                there = slice(r, r + 8)
                t = src[l + 1, here, :]
                flux = gz[l + 1, there, :] * (src[l + 2, here, :] - t)
                flux += gz[l, there, :] * (src[l, here, :] - t)
                flux += gx[l + 1, here, :] * (src[l + 1, PAD + r + 1 : PAD + r + 9, :] - t)
                flux += gx[l + 1, PAD + r - 1 : PAD + r + 7, :] * (
                    src[l + 1, PAD + r - 1 : PAD + r + 7, :] - t
                )
                side = gy[l, there, :] * (pltpu.roll(t, LANES - 1, 1) - t)
                flux += side - pltpu.roll(side, 1, 1)
                new = t + cap[l, there, :] * (flux + power[l, there, :])
                if last:
                    warm_out[l, there, :] = new
                    s = expand[l, there, :] * new
                    strain[l + 1, here, :] = s
                    prod[l + 1, here, :] = s * mod[l + 1, here, :]
                else:
                    dst[l + 1, here, :] = new
            return 0

        lax.fori_loop(0, layers, step, 0)

    heat(temp_a, temp_b, False)
    heat(temp_b, None, True)

    mine8 = (lane_of((8, LANES)) // (LANES // 2)) == pos

    def loads(l, acc):
        for r in tiles:
            here = slice(PAD + r, PAD + r + 8)
            there = slice(r, r + 8)
            s = picks(strain, None, l, r)
            m = picks(mod, None, l, r)
            q = picks(prod, None, l, r)
            gs, gm, gq = gradient_stencil(s), gradient_stencil(m), gradient_stencil(q)
            for k, entry in enumerate(matrix_stencil(m)):
                mats[k, l, there, :] = entry * inv_scale
            keep = inside[...]
            for c in range(3):
                v = (-0.5 * strain_gain) * (m["F"] * gs[c] + s["F"] * gm[c] + gq[c]) * keep
                u[0, c, l + 1, here, :] = v
                w[0, c, l + 1, here, :] = v * m["F"]
                v_out[0, c, l, there, :] = v
                acc = acc + jnp.where(mine8, v * v, 0.0)
        return acc

    zero = jnp.zeros((8, LANES), f32)
    moments = [lax.fori_loop(0, layers, loads, zero)]

    def power_step(number, src, dst):
        def step(l, accs):
            cross, square = accs
            for r in tiles:
                here = slice(PAD + r, PAD + r + 8)
                there = slice(r, r + 8)
                uz, ux, uy = (picks(u, (src, c), l, r) for c in range(3))
                old = (uz["F"], ux["F"], uy["F"])
                cu = full_stencil(uz, ux, uy)
                wz, wx, wy = (picks(w, (src, c), l, r) for c in range(3))
                weighted = (wz["F"], wx["F"], wy["F"])
                cw = full_stencil(wz, wx, wy)
                zz, xx, yy, zx, zy, xy = (mats[k, l, there, :] for k in range(6))
                mixed = (
                    zz * old[0] + zx * old[1] + zy * old[2],
                    zx * old[0] + xx * old[1] + xy * old[2],
                    zy * old[0] + xy * old[1] + yy * old[2],
                )
                m = mod[l + 1, here, :]
                keep = inside[...]
                for c in range(3):
                    inner = (anchor_scale + CENTRE) * weighted[c] - m * cu[c] - cw[c]
                    v = (inner * inv_scale + mixed[c] - old[c]) * keep
                    v_out[number, c, l, there, :] = v
                    if dst is not None:
                        u[dst, c, l + 1, here, :] = v
                        w[dst, c, l + 1, here, :] = v * m
                    own_v = jnp.where(mine8, v, 0.0)
                    cross = cross + own_v * old[c]
                    square = square + own_v * own_v
            return cross, square

        return lax.fori_loop(0, layers, step, (zero, zero))

    for number in range(1, ITERS + 1):
        src = (number - 1) % 2
        dst = number % 2 if number < ITERS else None
        cross, square = power_step(number, src, dst)
        moments.append(cross)
        if number < ITERS:
            moments.append(square)

    lane1 = lane_of((1, LANES))
    row = jnp.zeros((1, LANES), f32)
    for k, part in enumerate(moments):
        row = jnp.where(lane1 == k, jnp.sum(part), row)
    for k in range(mom_out.shape[0]):
        mom_out[k] = row


def coefficients(mu, scale):
    def inner(a, b):
        total = None
        for i, x in enumerate(a):
            for j, y in enumerate(b):
                term = x * y * mu[i + j]
                total = term if total is None else total + term
        return total

    def added(a, b):
        out = []
        for k in range(max(len(a), len(b))):
            if k >= len(a):
                out.append(b[k])
            elif k >= len(b):
                out.append(a[k])
            else:
                out.append(a[k] + b[k])
        return out

    one = jnp.ones_like(mu[0])
    residual = [one]
    direction = [one]
    solution = []
    norm = mu[0]
    for number in range(ITERS):
        image = added(direction, [jnp.zeros_like(one)] + direction)
        alpha = norm / inner(direction, image)
        solution = added(solution, [alpha * d for d in direction])
        residual = added(residual, [-alpha * d for d in image])
        if number + 1 < ITERS:
            following = inner(residual, residual)
            ratio = following / norm
            direction = added(residual, [ratio * d for d in direction])
            norm = following
    return [s / scale for s in solution], residual


def combine_kernel(where_ref, traits, mom, v, warm, *outs):
    layers, full, _ = warm.shape
    rows = outs[0].shape[1]
    half = layers // 2
    quarter = half // 2
    gx, gz, pos = where_ref[0], where_ref[1], where_ref[2]
    total = jnp.sum(mom[:, 0, :], axis=0, keepdims=True)
    lane1 = lane_of((1, LANES))
    shape = (8, LANES)
    mu = [
        jnp.full(shape, jnp.sum(jnp.where(lane1 == k, total, 0.0)), f32) for k in range(2 * ITERS)
    ]
    count = traits.shape[1]
    mean_mod = traits[2, 0]
    for k in range(1, count):
        mean_mod = mean_mod + traits[2, k]
    scale = jnp.full(shape, mean_mod * ((anchor_scale + 2.0 * CENTRE) / count), f32)
    sol, res = coefficients(mu, scale)
    in_half = (lane_of(shape) // (LANES // 2)) == pos

    for number, out in enumerate(outs):
        dx, dz = number % 2, number // 2
        row0 = pl.multiple_of((gx ^ dx) * rows, rows)
        layer0 = (gz ^ dz) * half

        def piece(l, _, out=out, row0=row0, layer0=layer0):
            for r in range(0, rows, 8):
                for c in range(3):
                    made = []
                    for ll in (l, l + quarter):
                        vs = [v[k, c, layer0 + ll, pl.ds(row0 + r, 8), :] for k in range(ITERS + 1)]
                        x = sol[0] * vs[0]
                        y = res[0] * vs[0]
                        for k in range(1, ITERS + 1):
                            if k < ITERS:
                                x = x + sol[k] * vs[k]
                            y = y + res[k] * vs[k]
                        made.append((x, y))
                    for which in (0, 1):
                        out[(3 * which + c) * quarter + l, r : r + 8, :] = jnp.where(
                            in_half, made[0][which], half_roll(made[1][which])
                        )
            return 0

        lax.fori_loop(0, quarter, piece, 0)
        if dz == 0:
            for l in range(half):
                for r in range(0, rows, 8):
                    low = warm[l, pl.ds(row0 + r, 8), :]
                    high = warm[l + half, pl.ds(row0 + r, 8), :]
                    out[6 * quarter + l, r : r + 8, :] = jnp.where(in_half, low, half_roll(high))


def place_kernel(where_ref, mine, over_x, over_z, over_both, warm_out, sol_out, res_out):
    layers, rows, _ = warm_out.shape
    half = layers // 2
    quarter = half // 2
    gz, pos = where_ref[1], where_ref[2]
    half_of = lane_of((rows, LANES)) // (LANES // 2)
    for block, (a, b, p) in enumerate(((mine, over_x, pos), (over_z, over_both, 1 - pos))):
        first = half_of == p
        lanes = pl.ds(pl.multiple_of((gz ^ block) * LANES, LANES), LANES)
        for which, out in enumerate((sol_out, res_out)):
            for c in range(3):
                for l in range(quarter):
                    x = a[(3 * which + c) * quarter + l]
                    y = b[(3 * which + c) * quarter + l]
                    out[c, l, :, lanes] = jnp.where(first, x, y)
                    out[c, l + quarter, :, lanes] = half_roll(jnp.where(first, y, x))
        if block == 0:
            for l in range(half):
                x = a[6 * quarter + l]
                y = b[6 * quarter + l]
                warm_out[l] = jnp.where(first, x, y)
                warm_out[l + half] = half_roll(jnp.where(first, y, x))


LIMIT = 24 * 1024 * 1024


def params():
    return pltpu.CompilerParams(vmem_limit_bytes=LIMIT)


def vmem():
    return pl.BlockSpec(memory_space=pltpu.VMEM)


def smem():
    return pl.BlockSpec(memory_space=pltpu.SMEM)


def per_device_fast(temp, label, patch, traits, intensity):
    nx, ny, nz = (lax.axis_size(a) for a in AXES)
    layers, rows, width = temp.shape
    full = rows * nx
    half = layers // 2
    quarter = half // 2
    devices = nx * ny * nz
    gx, gy, gz = (lax.axis_index(a) for a in AXES)
    pos = gx ^ gz
    block = gy * nz + gz
    paired = jnp.where(pos == 0, block > 0, block < ny * nz - 1)
    where_am = jnp.stack([gx, gz, pos, paired.astype(jnp.int32)]).astype(jnp.int32)

    def number(x, b):
        return x * ny * nz + b

    def everywhere(dx, dz):
        return [
            (number(x, y * nz + z), number(x ^ dx, y * nz + (z ^ dz)))
            for x in range(nx) for y in range(ny) for z in range(nz)
        ]

    def side(x, b):
        return x ^ (b % nz)

    chain = []
    for b in range(1, ny * nz):
        left = [x for x in range(nx) if side(x, b - 1) == 1][0]
        right = [x for x in range(nx) if side(x, b) == 0][0]
        chain += [(number(left, b - 1), number(right, b)), (number(right, b), number(left, b - 1))]

    sds = lambda *s: jax.ShapeDtypeStruct(s, f32)
    held = lambda *s: pltpu.VMEM(s, f32)
    keep = lambda x: pltpu.with_memory_space_constraint(x, pltpu.VMEM)
    send = pl.pallas_call(
        pack_rows_kernel,
        out_shape=held(3, half + 1, rows, LANES),
        in_specs=[smem(), vmem(), vmem(), vmem()],
        out_specs=vmem(),
        compiler_params=params(),
        name="pack_rows",
    )(where_am, temp, label, patch)
    got = keep(lax.ppermute(send, AXES, everywhere(1, 0)))
    send = pl.pallas_call(
        pack_far_kernel,
        out_shape=held(3, full, LANES),
        in_specs=[smem(), vmem(), vmem(), vmem(), vmem()],
        out_specs=vmem(),
        compiler_params=params(),
        name="pack_far",
    )(where_am, temp, label, patch, got)
    far = keep(lax.ppermute(send, AXES, chain))

    padded = pltpu.VMEM((layers + 2, full + 2 * PAD, LANES), f32)
    plain = pltpu.VMEM((layers, full, LANES), f32)
    vectors = pltpu.VMEM((2, 3, layers + 2, full + 2 * PAD, LANES), f32)
    warm, v, mom = pl.pallas_call(
        solve_kernel,
        out_shape=(
            held(layers, full, LANES),
            held(ITERS + 1, 3, layers, full, LANES),
            held(devices, 1, LANES),
        ),
        in_specs=[smem(), smem(), smem(), vmem(), vmem(), vmem(), vmem(), vmem()],
        out_specs=(vmem(), vmem(), vmem()),
        scratch_shapes=[
            padded, padded, padded, plain, plain,
            pltpu.VMEM((layers + 1, full, LANES), f32), padded, plain,
            padded, plain, padded, padded,
            pltpu.VMEM((6, layers, full, LANES), f32),
            pltpu.VMEM((8, LANES), f32),
            vectors, vectors,
        ],
        compiler_params=params(),
        name="solve",
    )(where_am, traits, intensity, temp, label, patch, got, far)
    mom = keep(lax.all_to_all(mom, AXES, 0, 0, tiled=True))
    big = 6 * quarter + half
    mine, to_x, to_z, to_both = pl.pallas_call(
        combine_kernel,
        out_shape=(
            held(big, rows, LANES), held(big, rows, LANES),
            held(6 * quarter, rows, LANES), held(6 * quarter, rows, LANES),
        ),
        in_specs=[smem(), smem(), vmem(), vmem(), vmem()],
        out_specs=(vmem(),) * 4,
        compiler_params=params(),
        name="combine",
    )(where_am, traits, mom, keep(v), keep(warm))
    from_x = keep(lax.ppermute(to_x, AXES, everywhere(1, 0)))
    from_z = keep(lax.ppermute(to_z, AXES, everywhere(0, 1)))
    from_both = keep(lax.ppermute(to_both, AXES, everywhere(1, 1)))
    return pl.pallas_call(
        place_kernel,
        out_shape=(
            sds(layers, rows, width),
            sds(3, half, rows, nz * width),
            sds(3, half, rows, nz * width),
        ),
        in_specs=[smem(), vmem(), vmem(), vmem(), vmem()],
        out_specs=(vmem(),) * 3,
        compiler_params=params(),
        name="place",
    )(where_am, keep(mine), from_x, from_z, from_both)


def padded(value, sides, width):
    for axis, dim in sides:
        devices, length = (lax.axis_size(axis), value.shape[dim])
        up = [(i, (i + 1) % devices) for i in range(devices - 1)]
        down = [(j, i) for i, j in up]
        last = lax.slice_in_dim(value, length - width, length, axis=dim)
        initial = lax.slice_in_dim(value, 0, width, axis=dim)
        before = lax.ppermute(last, axis, up)
        after = lax.ppermute(initial, axis, down)
        value = jnp.concatenate([before, value, after], axis=dim)
    return value


def lookup(identity, table, count):
    summed = jnp.zeros(identity.shape, jnp.float32)
    for number in range(count):
        summed = summed + jnp.where(identity == number, table[number], jnp.float32(0.0))
    return summed


def heat_step(padded_temp, padded_cond, power, inverse_cap):
    centre = padded_temp[:, 1:-1, 1:-1]
    own = padded_cond[:, 1:-1, 1:-1]
    layers, rows, columns = centre.shape
    heat_flux = jnp.zeros_like(centre)
    for row_offset, column_offset in ((0, 1), (2, 1), (1, 0), (1, 2)):
        neighbour = padded_temp[
            :, row_offset : row_offset + rows, column_offset : column_offset + columns
        ]
        other = padded_cond[
            :, row_offset : row_offset + rows, column_offset : column_offset + columns
        ]
        heat_flux = heat_flux + conduct(own, other) * (neighbour - centre)
    vertical_temp = jnp.pad(centre, ((1, 1), (0, 0), (0, 0)))
    vertical_cond = jnp.pad(own, ((1, 1), (0, 0), (0, 0)))
    for layer_offset in (0, 2):
        other = vertical_cond[layer_offset : layer_offset + layers]
        neighbour = vertical_temp[layer_offset : layer_offset + layers]
        heat_flux = heat_flux + conduct(own, other) * (neighbour - centre)
    return centre + time_step * inverse_cap * (heat_flux + power)


def neighbour_offsets():
    listed = []
    for along_z in (-1, 0, 1):
        for along_x in (-1, 0, 1):
            for along_y in (-1, 0, 1):
                if along_z != 0 or along_x != 0 or along_y != 0:
                    listed.append((along_z, along_x, along_y))
    return listed


def apply_operator(field, padded_field, modulus, padded_modulus):
    layers, rows, columns = modulus.shape
    parts = [
        anchor_scale * modulus * field[0],
        anchor_scale * modulus * field[1],
        anchor_scale * modulus * field[2],
    ]
    for along_z, along_x, along_y in neighbour_offsets():
        length_sq = along_z * along_z + along_x * along_x + along_y * along_y
        window = (
            slice(1 + along_z, 1 + along_z + layers),
            slice(1 + along_x, 1 + along_x + rows),
            slice(1 + along_y, 1 + along_y + columns),
        )
        weight = 0.5 / length_sq * (modulus + padded_modulus[window])
        change = [field[index_c] - padded_field[index_c][window] for index_c in range(3)]
        projected = (along_z * change[0] + along_x * change[1] + along_y * change[2]) / length_sq
        for index_c, direction_part in enumerate((along_z, along_x, along_y)):
            parts[index_c] = parts[index_c] + weight * (
                0.5 * change[index_c] + direction_part * projected
            )
    return jnp.stack(parts)


def thermal_load(modulus, padded_modulus, strain, padded_strain):
    layers, rows, columns = modulus.shape
    parts = [jnp.zeros_like(modulus), jnp.zeros_like(modulus), jnp.zeros_like(modulus)]
    for along_z, along_x, along_y in neighbour_offsets():
        length_sq = along_z * along_z + along_x * along_x + along_y * along_y
        window = (
            slice(1 + along_z, 1 + along_z + layers),
            slice(1 + along_x, 1 + along_x + rows),
            slice(1 + along_y, 1 + along_y + columns),
        )
        weight = 0.5 / length_sq * (modulus + padded_modulus[window])
        pushing = weight * (0.5 * (strain + padded_strain[window]))
        for index_c, direction_part in enumerate((along_z, along_x, along_y)):
            if direction_part != 0:
                parts[index_c] = parts[index_c] - strain_gain * direction_part * pushing
    return jnp.stack(parts)


def two_products(residual, image):
    return lax.psum((jnp.sum(residual * residual), jnp.sum(residual * image)), ("gx", "gy", "gz"))


def per_device_plain(
    starting_kelvin, substance_label, voxel_source_patch, substance_traits, patch_source_intensity
):
    count = substance_traits.shape[1]
    diffusive_coefficient = lookup(substance_label, substance_traits[0], count)
    inverse_cap = 1.0 / lookup(substance_label, substance_traits[1], count)
    power = lookup(voxel_source_patch, patch_source_intensity, patch_source_intensity.shape[0])
    padded_array = padded(
        jnp.stack([starting_kelvin, diffusive_coefficient]), (("gx", 2), (("gy", "gz"), 3)), 1
    )
    padded_cond = padded_array[1]
    warmed_result = heat_step(padded_array[0], padded_cond, power, inverse_cap)
    number = 0
    extended = padded(warmed_result, (("gx", 1), (("gy", "gz"), 2)), 1)
    warmed_result = heat_step(extended, padded_cond, power, inverse_cap)
    modulus = lookup(substance_label, substance_traits[2], count)
    strain = lookup(substance_label, substance_traits[3], count) * warmed_result
    fields = jnp.stack([modulus, strain])
    vertical_cycle = ((0, 0), (1, 1), (0, 0), (0, 0))
    padded_fields = jnp.pad(padded(fields, (("gx", 2), (("gy", "gz"), 3)), 1), vertical_cycle)

    def extend(field):
        return jnp.pad(padded(field, (("gx", 2), (("gy", "gz"), 3)), 1), vertical_cycle)

    modulus = fields[0]
    padded_modulus = padded_fields[0]
    load = thermal_load(modulus, padded_modulus, fields[1], padded_fields[1])

    def operate(field):
        return apply_operator(field, extend(field), modulus, padded_modulus)

    solution = jnp.zeros_like(load)
    residual = load
    image = operate(residual)
    norm_now, product = two_products(residual, image)
    alpha = norm_now / product
    direction, along_image = (residual, image)
    for number in range(ITERS):
        solution = solution + alpha * direction
        residual = residual - alpha * along_image
        if number + 1 < ITERS:
            image = operate(residual)
            norm_next, product = two_products(residual, image)
            ratio = norm_next / norm_now
            alpha = norm_next / (product - ratio * norm_next / alpha)
            direction = residual + ratio * direction
            along_image = image + ratio * along_image
            norm_now = norm_next
    joined = lax.all_to_all(
        jnp.concatenate([solution, residual]), "gz", split_axis=1, concat_axis=3, tiled=True
    )
    solution = joined[:3]
    residual = joined[3:]
    return (warmed_result, solution, residual)


def solution(mesh):
    in_specs = (
        P(None, "gx", ("gy", "gz")),
        P(None, "gx", ("gy", "gz")),
        P(None, "gx", ("gy", "gz")),
        P(),
        P(),
    )
    out_specs = (P(None, "gx", ("gy", "gz")), P(None, "gz", "gx", "gy"), P(None, "gz", "gx", "gy"))

    def per_device(temp, label, patch, traits, intensity):
        layers, rows, width = temp.shape
        fits = (
            mesh.shape["gx"] == 2
            and mesh.shape["gz"] == 2
            and width == LANES
            and layers % 4 == 0
            and layers * HALO <= LANES
            and rows % 8 == 0
        )
        run = per_device_fast if fits else per_device_plain
        return run(temp, label, patch, traits, intensity)

    return jax.shard_map(
        per_device, mesh=mesh, in_specs=in_specs, out_specs=out_specs, check_vma=False
    )
```

```python
import functools

import jax
import jax.numpy as jnp
from jax import lax
from jax.experimental import pallas as pl
from jax.experimental.pallas import tpu as pltpu
from jax.sharding import PartitionSpec as P


ITERS = 3
HALO = 8
LANES = 128
PAD = 8
AXES = ("gx", "gy", "gz")

time_step = 0.03
anchor_scale = 0.5
strain_gain = 2.0
CENTRE = 55.0 / 9.0

f32 = jnp.float32


def half_roll(x):
    return pltpu.roll(x, LANES // 2, 1)


def lane_of(shape):
    return lax.broadcasted_iota(jnp.int32, shape, 1)


def pack_rows_kernel(where_ref, traits, intensity, temp, label, patch, block, out, table):
    layers, rows, _ = temp.shape
    half = layers // 2
    theirs = 1 - where_ref[2]
    lane = lane_of((rows, LANES))
    in_half = (lane // (LANES // 2)) == theirs
    base = LANES // 2 - HALO * theirs
    kinds, count = traits.shape
    for k in range(kinds):
        for m in range(count):
            table[k * count + m] = jnp.full((8, LANES), traits[k, m], f32)
    for k in range(intensity.shape[0]):
        table[kinds * count + k] = jnp.full((8, LANES), intensity[k], f32)
    for a, ref in enumerate((temp, label, patch)):
        near = jnp.zeros((rows, LANES), f32)
        values = []
        for l in range(layers):
            value = ref[l].astype(f32)
            block[a, l] = value
            values.append(value)
            moved = pltpu.roll(value, (HALO * l - base) % LANES, 1)
            near = jnp.where((lane // HALO) == l, moved, near)
        for l in range(half):
            out[a, l] = jnp.where(in_half, values[l], half_roll(values[l + half]))
        out[a, half] = near


def pack_far_kernel(where_ref, block, got, out):
    _, layers, rows, _ = block.shape
    half = layers // 2
    gx = where_ref[0]
    pos = where_ref[2]
    lane = lane_of((rows, LANES))
    base = (LANES - HALO) * pos
    own = pl.multiple_of(gx * rows, rows)
    other = pl.multiple_of((1 - gx) * rows, rows)
    for a in range(3):
        mine = jnp.zeros((rows, LANES), f32)
        theirs = jnp.zeros((rows, LANES), f32)
        for l in range(layers):
            here = (lane // HALO) == l
            moved = pltpu.roll(block[a, l], (HALO * l - base) % LANES, 1)
            mine = jnp.where(here, moved, mine)
            extra = 0 if l < half else LANES // 2
            moved = pltpu.roll(got[a, l % half], (HALO * l - base + extra) % LANES, 1)
            theirs = jnp.where(here, moved, theirs)
        out[a, pl.ds(own, rows), :] = mine
        out[a, pl.ds(other, rows), :] = theirs


def picks(ref, index, l, row):
    def at(dz, dx):
        if index is None:
            return ref[l + 1 + dz, PAD + row + dx : PAD + row + dx + 8, :]
        return ref[index, l + 1 + dz, PAD + row + dx : PAD + row + dx + 8, :]

    out = {}
    for dx in (-1, 0, 1):
        up, mid, down = at(1, dx), at(0, dx), at(-1, dx)
        out["F", dx] = mid
        out["G", dx] = up + down
        out["H", dx] = up - down
    res = {}
    for k in "FGH":
        res[k] = out[k, 0]
        res["E" + k] = out[k, 1] + out[k, -1]
        res["D" + k] = out[k, 1] - out[k, -1]
    return res


def along_lanes(base, even, odd):
    total = base
    if odd is None:
        return total + pltpu.roll(even, LANES - 1, 1) + pltpu.roll(even, 1, 1)
    if even is None:
        return total + pltpu.roll(odd, LANES - 1, 1) - pltpu.roll(odd, 1, 1)
    return total + pltpu.roll(even + odd, LANES - 1, 1) + pltpu.roll(even - odd, 1, 1)


S9 = 5.0 / 36.0
S18 = 1.0 / 18.0
S6 = 1.0 / 6.0


def full_stencil(z, x, y):
    base0 = 0.25 * (z["EF"] + z["EG"]) + 0.75 * z["G"] + 0.125 * x["DH"]
    even0 = 0.25 * (z["F"] + z["G"]) + 0.125 * z["EF"] + S9 * z["EG"] + S18 * x["DH"]
    odd0 = 0.125 * y["H"] + S18 * y["EH"]
    base1 = 0.75 * x["EF"] + 0.25 * (x["G"] + x["EG"]) + 0.125 * z["DH"]
    even1 = 0.25 * (x["F"] + x["EF"]) + 0.125 * x["G"] + S9 * x["EG"] + S18 * z["DH"]
    odd1 = 0.125 * y["DF"] + S18 * y["DG"]
    base2 = 0.25 * (y["EF"] + y["G"]) + 0.125 * y["EG"]
    even2 = 0.75 * y["F"] + 0.25 * (y["EF"] + y["G"]) + S9 * y["EG"]
    odd2 = 0.125 * (x["DF"] + z["H"]) + S18 * (x["DG"] + z["EH"])
    return (
        along_lanes(base0, even0, odd0),
        along_lanes(base1, even1, odd1),
        along_lanes(base2, even2, odd2),
    )


def matrix_stencil(m):
    zz = along_lanes(
        0.25 * (m["EF"] + m["EG"]) + 0.75 * m["G"],
        0.25 * (m["F"] + m["G"]) + 0.125 * m["EF"] + S9 * m["EG"],
        None,
    )
    xx = along_lanes(
        0.75 * m["EF"] + 0.25 * (m["G"] + m["EG"]),
        0.25 * (m["F"] + m["EF"]) + 0.125 * m["G"] + S9 * m["EG"],
        None,
    )
    yy = along_lanes(
        0.25 * (m["EF"] + m["G"]) + 0.125 * m["EG"],
        0.75 * m["F"] + 0.25 * (m["EF"] + m["G"]) + S9 * m["EG"],
        None,
    )
    zx = along_lanes(0.125 * m["DH"], S18 * m["DH"], None)
    odd_zy = 0.125 * m["H"] + S18 * m["EH"]
    odd_xy = 0.125 * m["DF"] + S18 * m["DG"]
    zy = pltpu.roll(odd_zy, LANES - 1, 1) - pltpu.roll(odd_zy, 1, 1)
    xy = pltpu.roll(odd_xy, LANES - 1, 1) - pltpu.roll(odd_xy, 1, 1)
    return zz, xx, yy, zx, zy, xy


def gradient_stencil(f):
    gz = along_lanes(0.5 * f["H"] + 0.25 * f["EH"], 0.25 * f["H"] + S6 * f["EH"], None)
    gx = along_lanes(0.5 * f["DF"] + 0.25 * f["DG"], 0.25 * f["DF"] + S6 * f["DG"], None)
    odd = 0.5 * f["F"] + 0.25 * (f["G"] + f["EF"]) + S6 * f["EG"]
    gy = pltpu.roll(odd, LANES - 1, 1) - pltpu.roll(odd, 1, 1)
    return gz, gx, gy


def conduct(own, other):
    return 2.0 * own * other / jnp.maximum(own + other, 0.25)


def choose(label, values):
    out = jnp.zeros(label.shape, f32)
    for k, v in enumerate(values):
        out = jnp.where(label == float(k), v, out)
    return out


def shift_scale(table, count):
    total = table[2 * count]
    for k in range(1, count):
        total = total + table[2 * count + k]
    return total * ((anchor_scale + 2.0 * CENTRE) / count)


def pack_vectors(where_ref, v, outs, warm):
    count, _, layers, _, _ = v.shape
    rows = outs[0].shape[1]
    half = layers // 2
    quarter = half // 2
    gx, gz, pos = where_ref[0], where_ref[1], where_ref[2]
    in_half = (lane_of((8, LANES)) // (LANES // 2)) == pos
    for number, out in enumerate(outs):
        dx, dz = number % 2, number // 2
        row0 = pl.multiple_of((gx ^ dx) * rows, rows)
        layer0 = (gz ^ dz) * half

        def piece(l, _, out=out, row0=row0, layer0=layer0):
            for r in range(0, rows, 8):
                for k in range(count):
                    for c in range(3):
                        low = v[k, c, layer0 + l, pl.ds(row0 + r, 8), :]
                        high = v[k, c, layer0 + l + quarter, pl.ds(row0 + r, 8), :]
                        out[(3 * k + c) * quarter + l, r : r + 8, :] = jnp.where(
                            in_half, low, half_roll(high)
                        )
            return 0

        lax.fori_loop(0, quarter, piece, 0)
        if warm is not None and dz == 0:

            def warm_piece(l, _, out=out, row0=row0):
                for r in range(0, rows, 8):
                    low = warm[l, pl.ds(row0 + r, 8), :]
                    high = warm[l + half, pl.ds(row0 + r, 8), :]
                    out[3 * count * quarter + l, r : r + 8, :] = jnp.where(
                        in_half, low, half_roll(high)
                    )
                return 0

            lax.fori_loop(0, half, warm_piece, 0, unroll=2)


def power_step(mod, mats, inside, inv_scale, mine8, source, dest, v):
    u, w = source
    layers = mats.shape[1]
    tiles = range(0, mats.shape[2], 8)

    def step(l, accs):
        cross, square = accs
        for r in tiles:
            here = slice(PAD + r, PAD + r + 8)
            there = slice(r, r + 8)
            uz, ux, uy = (picks(u, c, l, r) for c in range(3))
            old = (uz["F"], ux["F"], uy["F"])
            cu = full_stencil(uz, ux, uy)
            wz, wx, wy = (picks(w, c, l, r) for c in range(3))
            weighted = (wz["F"], wx["F"], wy["F"])
            cw = full_stencil(wz, wx, wy)
            zz, xx, yy, zx, zy, xy = (mats[k, l, there, :] for k in range(6))
            mixed = (
                zz * old[0] + zx * old[1] + zy * old[2],
                zx * old[0] + xx * old[1] + xy * old[2],
                zy * old[0] + xy * old[1] + yy * old[2],
            )
            m = mod[l + 1, here, :]
            keep = inside[...]
            for c in range(3):
                inner = (anchor_scale + CENTRE) * weighted[c] - m * cu[c] - cw[c]
                new = (inner * inv_scale + mixed[c] - old[c]) * keep
                v[c, l, there, :] = new
                if dest is not None:
                    dest[0][c, l + 1, here, :] = new
                    dest[1][c, l + 1, here, :] = new * m
                own = jnp.where(mine8, new, 0.0)
                cross = cross + own * old[c]
                square = square + own * own
        return cross, square

    zero = jnp.zeros((8, LANES), f32)
    return lax.fori_loop(0, layers, step, (zero, zero))


def clear_edges(refs, zero_tile):
    for ref in refs:
        for index in ([()] if len(ref.shape) == 3 else [(c,) for c in range(ref.shape[0])]):
            ref[index + (0,)] = zero_tile
            ref[index + (ref.shape[-3] - 1,)] = zero_tile


def first_kernel(
    where_ref, table, block, got, far,
    mod, mats, inside, u_next, w_next, moments, mine, to_x, to_z, to_both,
    cond, temp_a, temp_b, cap, power, gz, gx, gy, gy_back, expand, strain, prod, u, w, v, warm,
    *, count,
):
    _, layers, rows, _ = block.shape
    full = far.shape[1]
    half = layers // 2
    me = where_ref[0]
    pos = where_ref[2]
    paired = where_ref[3] > 0
    tiles = range(0, full, 8)
    kinds = 4
    sources = table.shape[0] - kinds * count
    own = pl.multiple_of(me * rows, rows)
    other = pl.multiple_of((1 - me) * rows, rows)
    near_base = LANES // 2 - HALO * pos
    far_base = (LANES - HALO) * (1 - pos)
    near_lanes = (lane_of((rows, LANES)) // HALO) == (near_base // HALO)
    far_lanes = (lane_of((full, LANES)) // HALO) == (far_base // HALO)

    inv_scale = 1.0 / shift_scale(table, count)
    cond_t = [table[k] for k in range(count)]
    cap_t = [time_step / table[count + k] for k in range(count)]
    mod_t = [table[2 * count + k] for k in range(count)]
    exp_t = [table[3 * count + k] for k in range(count)]
    pow_t = [table[kinds * count + k] for k in range(sources)]

    zero_tile = jnp.zeros((full + 2 * PAD, LANES), f32)
    clear_edges((cond, temp_a, temp_b, mod, strain, prod, u, w, u_next, w_next), zero_tile)
    gz[0] = jnp.zeros((full, LANES), f32)
    edge = jnp.zeros((PAD, LANES), f32)

    def window(l, _):
        for ref in (cond, temp_a, temp_b, mod, strain, prod, gx):
            ref[l + 1, 0:PAD] = edge
            ref[l + 1, PAD + full : 2 * PAD + full] = edge
        for ref in (u, w, u_next, w_next):
            for c in range(3):
                ref[c, l + 1, 0:PAD] = edge
                ref[c, l + 1, PAD + full : 2 * PAD + full] = edge
        for a, dest in enumerate((temp_a, temp_b, cond)):
            packed = got[a, lax.rem(l, half)]
            theirs = jnp.where(l < half, packed, half_roll(packed))
            near = pltpu.roll(got[a, half], (near_base - HALO * l + 2 * LANES) % LANES, 1)
            theirs = jnp.where(near_lanes, near, theirs)
            dest[l + 1, pl.ds(PAD + own, rows), :] = block[a, l]
            dest[l + 1, pl.ds(PAD + other, rows), :] = theirs
            edge_cols = pltpu.roll(far[a], (far_base - HALO * l + 2 * LANES) % LANES, 1)
            if a == 1:
                edge_cols = jnp.where(paired, edge_cols, -1.0)
            old = dest[l + 1, PAD : PAD + full, :]
            dest[l + 1, PAD : PAD + full, :] = jnp.where(far_lanes, edge_cols, old)
        return 0

    lax.fori_loop(0, layers, window, 0, unroll=2)

    def looked_up(l, _):
        for r in tiles:
            here = slice(PAD + r, PAD + r + 8)
            there = slice(r, r + 8)
            lab = temp_b[l + 1, here, :]
            src = cond[l + 1, here, :]
            cond[l + 1, here, :] = choose(lab, cond_t)
            cap[l, there, :] = choose(lab, cap_t)
            mod[l + 1, here, :] = choose(lab, mod_t)
            expand[l, there, :] = choose(lab, exp_t)
            power[l, there, :] = choose(src, pow_t)
            if r == 0:
                inside[...] = jnp.where(lab >= 0.0, 1.0, 0.0)
        return 0

    lax.fori_loop(0, layers, looked_up, 0)

    def faces(l, _):
        for r in tiles:
            here = slice(PAD + r, PAD + r + 8)
            there = slice(r, r + 8)
            a = cond[l + 1, here, :]
            gz[l + 1, there, :] = conduct(a, cond[l + 2, here, :])
            gx[l + 1, here, :] = conduct(a, cond[l + 1, PAD + r + 1 : PAD + r + 9, :])
            gy[l, there, :] = conduct(a, pltpu.roll(a, LANES - 1, 1))
            gy_back[l, there, :] = conduct(a, pltpu.roll(a, 1, 1))
        return 0

    lax.fori_loop(0, layers, faces, 0, unroll=4)

    def heat(src, dst, last):
        def step(l, _):
            for r in tiles:
                here = slice(PAD + r, PAD + r + 8)
                there = slice(r, r + 8)
                t = src[l + 1, here, :]
                flux = gz[l + 1, there, :] * (src[l + 2, here, :] - t)
                flux += gz[l, there, :] * (src[l, here, :] - t)
                flux += gx[l + 1, here, :] * (src[l + 1, PAD + r + 1 : PAD + r + 9, :] - t)
                flux += gx[l + 1, PAD + r - 1 : PAD + r + 7, :] * (
                    src[l + 1, PAD + r - 1 : PAD + r + 7, :] - t
                )
                flux += gy[l, there, :] * (pltpu.roll(t, LANES - 1, 1) - t)
                flux += gy_back[l, there, :] * (pltpu.roll(t, 1, 1) - t)
                new = t + cap[l, there, :] * (flux + power[l, there, :])
                if last:
                    warm[l, there, :] = new
                    s = expand[l, there, :] * new
                    strain[l + 1, here, :] = s
                    prod[l + 1, here, :] = s * mod[l + 1, here, :]
                else:
                    dst[l + 1, here, :] = new
            return 0

        lax.fori_loop(0, layers, step, 0, unroll=4)

    heat(temp_a, temp_b, False)
    heat(temp_b, None, True)

    mine8 = (lane_of((8, LANES)) // (LANES // 2)) == pos

    def loads(l, acc):
        for r in tiles:
            here = slice(PAD + r, PAD + r + 8)
            there = slice(r, r + 8)
            s = picks(strain, None, l, r)
            m = picks(mod, None, l, r)
            q = picks(prod, None, l, r)
            gs, gm, gq = gradient_stencil(s), gradient_stencil(m), gradient_stencil(q)
            for k, entry in enumerate(matrix_stencil(m)):
                mats[k, l, there, :] = entry * inv_scale
            keep = inside[...]
            for c in range(3):
                new = (-0.5 * strain_gain) * (m["F"] * gs[c] + s["F"] * gm[c] + gq[c]) * keep
                u[c, l + 1, here, :] = new
                w[c, l + 1, here, :] = new * m["F"]
                v[0, c, l, there, :] = new
                acc = acc + jnp.where(mine8, new * new, 0.0)
        return acc

    moments[0] = lax.fori_loop(0, layers, loads, jnp.zeros((8, LANES), f32))
    cross, square = power_step(
        mod, mats, inside, inv_scale, mine8, (u, w), (u_next, w_next), v.at[1]
    )
    moments[1] = cross
    moments[2] = square
    pack_vectors(where_ref, v, (mine, to_x, to_z, to_both), warm)


def second_kernel(
    where_ref, table, mod, mats, inside, u, w, moments,
    mom_out, mine, to_x, to_z, to_both,
    u_next, w_next, v,
    *, count,
):
    layers = mats.shape[1]
    full = mats.shape[2]
    pos = where_ref[2]
    inv_scale = 1.0 / shift_scale(table, count)
    mine8 = (lane_of((8, LANES)) // (LANES // 2)) == pos
    clear_edges((u_next, w_next), jnp.zeros((full + 2 * PAD, LANES), f32))
    edge = jnp.zeros((PAD, LANES), f32)

    def clear(l, _):
        for ref in (u_next, w_next):
            for c in range(3):
                ref[c, l + 1, 0:PAD] = edge
                ref[c, l + 1, PAD + full : 2 * PAD + full] = edge
        return 0

    lax.fori_loop(0, layers, clear, 0)
    parts = [moments[k] for k in range(moments.shape[0])]
    parts += power_step(
        mod, mats, inside, inv_scale, mine8, (u, w), (u_next, w_next), v.at[0]
    )
    cross, _ = power_step(
        mod, mats, inside, inv_scale, mine8, (u_next, w_next), None, v.at[1]
    )
    parts.append(cross)
    lane1 = lane_of((1, LANES))
    row = jnp.zeros((1, LANES), f32)
    for k, part in enumerate(parts):
        row = jnp.where(lane1 == k, jnp.sum(part), row)
    for k in range(mom_out.shape[0]):
        mom_out[k] = row
    pack_vectors(where_ref, v, (mine, to_x, to_z, to_both), None)


def coefficients(mu, scale):
    def inner(a, b):
        total = None
        for i, x in enumerate(a):
            for j, y in enumerate(b):
                term = x * y * mu[i + j]
                total = term if total is None else total + term
        return total

    def added(a, b):
        out = []
        for k in range(max(len(a), len(b))):
            if k >= len(a):
                out.append(b[k])
            elif k >= len(b):
                out.append(a[k])
            else:
                out.append(a[k] + b[k])
        return out

    one = jnp.ones_like(mu[0])
    residual = [one]
    direction = [one]
    solution = []
    norm = mu[0]
    for number in range(ITERS):
        image = added(direction, [jnp.zeros_like(one)] + direction)
        alpha = norm / inner(direction, image)
        solution = added(solution, [alpha * d for d in direction])
        residual = added(residual, [-alpha * d for d in image])
        if number + 1 < ITERS:
            following = inner(residual, residual)
            ratio = following / norm
            direction = added(residual, [ratio * d for d in direction])
            norm = following
    return [s / scale for s in solution], residual


def place_kernel(where_ref, table, mom, *refs, count):
    early, late, outs = refs[:4], refs[4:8], refs[8:]
    warm_out, sol_out, res_out = outs
    layers, rows, _ = warm_out.shape
    half = layers // 2
    quarter = half // 2
    gz, pos = where_ref[1], where_ref[2]
    lane1 = lane_of((1, LANES))
    shape = (8, LANES)
    total = jnp.sum(mom[:, 0, :], axis=0, keepdims=True)
    mu = [
        jnp.full(shape, jnp.sum(jnp.where(lane1 == k, total, 0.0)), f32) for k in range(2 * ITERS)
    ]
    sol, res = coefficients(mu, shift_scale(table, count))
    half_of = lane_of(shape) // (LANES // 2)
    for block in range(2):
        first = half_of == (pos if block == 0 else 1 - pos)
        lanes = pl.ds(pl.multiple_of((gz ^ block) * LANES, LANES), LANES)
        a = (early[2 * block], late[2 * block])
        b = (early[2 * block + 1], late[2 * block + 1])
        for c in range(3):
            for l in range(quarter):
                for r in range(0, rows, 8):
                    there = slice(r, r + 8)
                    low, high = [], []
                    for k in range(ITERS + 1):
                        index = (3 * (k % 2) + c) * quarter + l
                        x = a[k // 2][index, there, :]
                        y = b[k // 2][index, there, :]
                        low.append(jnp.where(first, x, y))
                        high.append(jnp.where(first, y, x))
                    for at, values in ((l, low), (l + quarter, high)):
                        x = sol[0] * values[0]
                        y = res[0] * values[0]
                        for k in range(1, ITERS + 1):
                            if k < ITERS:
                                x = x + sol[k] * values[k]
                            y = y + res[k] * values[k]
                        if at != l:
                            x, y = half_roll(x), half_roll(y)
                        sol_out[c, at, there, lanes] = x
                        res_out[c, at, there, lanes] = y
        if block == 0:
            for l in range(half):
                for r in range(0, rows, 8):
                    there = slice(r, r + 8)
                    x = a[0][6 * quarter + l, there, :]
                    y = b[0][6 * quarter + l, there, :]
                    warm_out[l, there, :] = jnp.where(first, x, y)
                    warm_out[l + half, there, :] = half_roll(jnp.where(first, y, x))


LIMIT = 24 * 1024 * 1024


def params():
    return pltpu.CompilerParams(vmem_limit_bytes=LIMIT)


def vmem():
    return pl.BlockSpec(memory_space=pltpu.VMEM)


def smem():
    return pl.BlockSpec(memory_space=pltpu.SMEM)


def per_device_fast(temp, label, patch, traits, intensity):
    nx, ny, nz = (lax.axis_size(a) for a in AXES)
    layers, rows, width = temp.shape
    full = rows * nx
    half = layers // 2
    quarter = half // 2
    devices = nx * ny * nz
    gx, gy, gz = (lax.axis_index(a) for a in AXES)
    pos = gx ^ gz
    block = gy * nz + gz
    paired = jnp.where(pos == 0, block > 0, block < ny * nz - 1)
    where_am = jnp.stack([gx, gz, pos, paired.astype(jnp.int32)]).astype(jnp.int32)

    def number(x, b):
        return x * ny * nz + b

    def everywhere(dx, dz):
        return [
            (number(x, y * nz + z), number(x ^ dx, y * nz + (z ^ dz)))
            for x in range(nx) for y in range(ny) for z in range(nz)
        ]

    def side(x, b):
        return x ^ (b % nz)

    chain = []
    for b in range(1, ny * nz):
        left = [x for x in range(nx) if side(x, b - 1) == 1][0]
        right = [x for x in range(nx) if side(x, b) == 0][0]
        chain += [(number(left, b - 1), number(right, b)), (number(right, b), number(left, b - 1))]

    sds = lambda *s: jax.ShapeDtypeStruct(s, f32)
    held = lambda *s: pltpu.VMEM(s, f32)
    keep = lambda x: pltpu.with_memory_space_constraint(x, pltpu.VMEM)
    there = lambda x: pltpu.with_memory_space_constraint(x, pltpu.HBM)
    count = traits.shape[1]
    entries = traits.size + intensity.size
    own, send, table = pl.pallas_call(
        pack_rows_kernel,
        out_shape=(
            held(3, layers, rows, LANES), held(3, half + 1, rows, LANES), held(entries, 8, LANES)
        ),
        in_specs=[smem(), smem(), smem(), vmem(), vmem(), vmem()],
        out_specs=(vmem(),) * 3,
        compiler_params=params(),
        name="pack_rows",
    )(where_am, there(traits), there(intensity), there(temp), there(label), there(patch))
    own, table = keep(own), keep(table)
    got = keep(lax.ppermute(send, AXES, everywhere(1, 0)))
    send = pl.pallas_call(
        pack_far_kernel,
        out_shape=held(3, full, LANES),
        in_specs=[smem(), vmem(), vmem()],
        out_specs=vmem(),
        compiler_params=params(),
        name="pack_far",
    )(where_am, own, got)
    far = keep(lax.ppermute(send, AXES, chain))

    edged = (layers + 2, full + 2 * PAD, LANES)
    plain = (layers, full, LANES)
    padded = pltpu.VMEM(edged, f32)
    flat = pltpu.VMEM(plain, f32)
    vectors = pltpu.VMEM((3,) + edged, f32)
    pieces = (6 * quarter + half, 6 * quarter + half, 6 * quarter, 6 * quarter)
    first = pl.pallas_call(
        functools.partial(first_kernel, count=count),
        out_shape=(
            held(*edged), held(6, *plain), held(8, LANES), held(3, *edged), held(3, *edged),
            held(3, 8, LANES),
        ) + tuple(held(k, rows, LANES) for k in pieces),
        in_specs=[smem()] + [vmem()] * 4,
        out_specs=(vmem(),) * 10,
        scratch_shapes=[
            padded, padded, padded, flat, flat,
            pltpu.VMEM((layers + 1, full, LANES), f32), padded, flat, flat,
            flat, padded, padded, vectors, vectors,
            pltpu.VMEM((2, 3) + plain, f32), flat,
        ],
        compiler_params=params(),
        name="first",
    )(where_am, table, own, got, far)
    carried, early = first[:6], first[6:]

    def exchanged(mine, *pieces):
        moved = [mine]
        for (dx, dz), piece in zip(((1, 0), (0, 1), (1, 1)), pieces):
            moved.append(lax.ppermute(piece, AXES, everywhere(dx, dz)))
        return tuple(keep(x) for x in moved)

    early = exchanged(*early)
    second = pl.pallas_call(
        functools.partial(second_kernel, count=count),
        out_shape=(held(devices, 1, LANES),)
        + tuple(held(6 * quarter, rows, LANES) for _ in range(4)),
        in_specs=[smem()] + [vmem()] * 7,
        out_specs=(vmem(),) * 5,
        scratch_shapes=[vectors, vectors, pltpu.VMEM((2, 3) + plain, f32)],
        compiler_params=params(),
        name="second",
    )(where_am, table, *(keep(x) for x in carried))
    late = exchanged(*second[1:])
    mom = lax.all_to_all(second[0], AXES, 0, 0, tiled=True)
    mom = keep(mom)
    return pl.pallas_call(
        functools.partial(place_kernel, count=count),
        out_shape=(
            sds(layers, rows, width),
            sds(3, half, rows, nz * width),
            sds(3, half, rows, nz * width),
        ),
        in_specs=[smem()] + [vmem()] * 10,
        out_specs=(vmem(),) * 3,
        compiler_params=params(),
        name="place",
    )(where_am, table, mom, *early, *late)


def padded(value, sides, width):
    for axis, dim in sides:
        devices, length = (lax.axis_size(axis), value.shape[dim])
        up = [(i, (i + 1) % devices) for i in range(devices - 1)]
        down = [(j, i) for i, j in up]
        last = lax.slice_in_dim(value, length - width, length, axis=dim)
        initial = lax.slice_in_dim(value, 0, width, axis=dim)
        before = lax.ppermute(last, axis, up)
        after = lax.ppermute(initial, axis, down)
        value = jnp.concatenate([before, value, after], axis=dim)
    return value


def lookup(identity, table, count):
    summed = jnp.zeros(identity.shape, jnp.float32)
    for number in range(count):
        summed = summed + jnp.where(identity == number, table[number], jnp.float32(0.0))
    return summed


def heat_step(padded_temp, padded_cond, power, inverse_cap):
    centre = padded_temp[:, 1:-1, 1:-1]
    own = padded_cond[:, 1:-1, 1:-1]
    layers, rows, columns = centre.shape
    heat_flux = jnp.zeros_like(centre)
    for row_offset, column_offset in ((0, 1), (2, 1), (1, 0), (1, 2)):
        neighbour = padded_temp[
            :, row_offset : row_offset + rows, column_offset : column_offset + columns
        ]
        other = padded_cond[
            :, row_offset : row_offset + rows, column_offset : column_offset + columns
        ]
        heat_flux = heat_flux + conduct(own, other) * (neighbour - centre)
    vertical_temp = jnp.pad(centre, ((1, 1), (0, 0), (0, 0)))
    vertical_cond = jnp.pad(own, ((1, 1), (0, 0), (0, 0)))
    for layer_offset in (0, 2):
        other = vertical_cond[layer_offset : layer_offset + layers]
        neighbour = vertical_temp[layer_offset : layer_offset + layers]
        heat_flux = heat_flux + conduct(own, other) * (neighbour - centre)
    return centre + time_step * inverse_cap * (heat_flux + power)


def neighbour_offsets():
    listed = []
    for along_z in (-1, 0, 1):
        for along_x in (-1, 0, 1):
            for along_y in (-1, 0, 1):
                if along_z != 0 or along_x != 0 or along_y != 0:
                    listed.append((along_z, along_x, along_y))
    return listed


def apply_operator(field, padded_field, modulus, padded_modulus):
    layers, rows, columns = modulus.shape
    parts = [
        anchor_scale * modulus * field[0],
        anchor_scale * modulus * field[1],
        anchor_scale * modulus * field[2],
    ]
    for along_z, along_x, along_y in neighbour_offsets():
        length_sq = along_z * along_z + along_x * along_x + along_y * along_y
        window = (
            slice(1 + along_z, 1 + along_z + layers),
            slice(1 + along_x, 1 + along_x + rows),
            slice(1 + along_y, 1 + along_y + columns),
        )
        weight = 0.5 / length_sq * (modulus + padded_modulus[window])
        change = [field[index_c] - padded_field[index_c][window] for index_c in range(3)]
        projected = (along_z * change[0] + along_x * change[1] + along_y * change[2]) / length_sq
        for index_c, direction_part in enumerate((along_z, along_x, along_y)):
            parts[index_c] = parts[index_c] + weight * (
                0.5 * change[index_c] + direction_part * projected
            )
    return jnp.stack(parts)


def thermal_load(modulus, padded_modulus, strain, padded_strain):
    layers, rows, columns = modulus.shape
    parts = [jnp.zeros_like(modulus), jnp.zeros_like(modulus), jnp.zeros_like(modulus)]
    for along_z, along_x, along_y in neighbour_offsets():
        length_sq = along_z * along_z + along_x * along_x + along_y * along_y
        window = (
            slice(1 + along_z, 1 + along_z + layers),
            slice(1 + along_x, 1 + along_x + rows),
            slice(1 + along_y, 1 + along_y + columns),
        )
        weight = 0.5 / length_sq * (modulus + padded_modulus[window])
        pushing = weight * (0.5 * (strain + padded_strain[window]))
        for index_c, direction_part in enumerate((along_z, along_x, along_y)):
            if direction_part != 0:
                parts[index_c] = parts[index_c] - strain_gain * direction_part * pushing
    return jnp.stack(parts)


def two_products(residual, image):
    return lax.psum((jnp.sum(residual * residual), jnp.sum(residual * image)), ("gx", "gy", "gz"))


def per_device_plain(
    starting_kelvin, substance_label, voxel_source_patch, substance_traits, patch_source_intensity
):
    count = substance_traits.shape[1]
    diffusive_coefficient = lookup(substance_label, substance_traits[0], count)
    inverse_cap = 1.0 / lookup(substance_label, substance_traits[1], count)
    power = lookup(voxel_source_patch, patch_source_intensity, patch_source_intensity.shape[0])
    padded_array = padded(
        jnp.stack([starting_kelvin, diffusive_coefficient]), (("gx", 2), (("gy", "gz"), 3)), 1
    )
    padded_cond = padded_array[1]
    warmed_result = heat_step(padded_array[0], padded_cond, power, inverse_cap)
    number = 0
    extended = padded(warmed_result, (("gx", 1), (("gy", "gz"), 2)), 1)
    warmed_result = heat_step(extended, padded_cond, power, inverse_cap)
    modulus = lookup(substance_label, substance_traits[2], count)
    strain = lookup(substance_label, substance_traits[3], count) * warmed_result
    fields = jnp.stack([modulus, strain])
    vertical_cycle = ((0, 0), (1, 1), (0, 0), (0, 0))
    padded_fields = jnp.pad(padded(fields, (("gx", 2), (("gy", "gz"), 3)), 1), vertical_cycle)

    def extend(field):
        return jnp.pad(padded(field, (("gx", 2), (("gy", "gz"), 3)), 1), vertical_cycle)

    modulus = fields[0]
    padded_modulus = padded_fields[0]
    load = thermal_load(modulus, padded_modulus, fields[1], padded_fields[1])

    def operate(field):
        return apply_operator(field, extend(field), modulus, padded_modulus)

    solution = jnp.zeros_like(load)
    residual = load
    image = operate(residual)
    norm_now, product = two_products(residual, image)
    alpha = norm_now / product
    direction, along_image = (residual, image)
    for number in range(ITERS):
        solution = solution + alpha * direction
        residual = residual - alpha * along_image
        if number + 1 < ITERS:
            image = operate(residual)
            norm_next, product = two_products(residual, image)
            ratio = norm_next / norm_now
            alpha = norm_next / (product - ratio * norm_next / alpha)
            direction = residual + ratio * direction
            along_image = image + ratio * along_image
            norm_now = norm_next
    joined = lax.all_to_all(
        jnp.concatenate([solution, residual]), "gz", split_axis=1, concat_axis=3, tiled=True
    )
    solution = joined[:3]
    residual = joined[3:]
    return (warmed_result, solution, residual)


def solution(mesh):
    in_specs = (
        P(None, "gx", ("gy", "gz")),
        P(None, "gx", ("gy", "gz")),
        P(None, "gx", ("gy", "gz")),
        P(),
        P(),
    )
    out_specs = (P(None, "gx", ("gy", "gz")), P(None, "gz", "gx", "gy"), P(None, "gz", "gx", "gy"))

    def per_device(temp, label, patch, traits, intensity):
        layers, rows, width = temp.shape
        fits = (
            mesh.shape["gx"] == 2
            and mesh.shape["gz"] == 2
            and width == LANES
            and layers % 4 == 0
            and layers * HALO <= LANES
            and rows % 8 == 0
        )
        run = per_device_fast if fits else per_device_plain
        return run(temp, label, patch, traits, intensity)

    return jax.shard_map(
        per_device, mesh=mesh, in_specs=in_specs, out_specs=out_specs, check_vma=False
    )
```

```python
import functools

import jax
import jax.numpy as jnp
from jax import lax
from jax.experimental import pallas as pl
from jax.experimental.pallas import tpu as pltpu
from jax.sharding import PartitionSpec as P


ITERS = 3
HALO = 8
LANES = 128
PAD = 8
AXES = ("gx", "gy", "gz")

time_step = 0.03
anchor_scale = 0.5
strain_gain = 2.0
CENTRE = 55.0 / 9.0
K4 = 4.0 * (anchor_scale + CENTRE)

f32 = jnp.float32


def position():
    gx, gy, gz = (lax.axis_index(a) for a in AXES)
    ny, nz = lax.axis_size("gy"), lax.axis_size("gz")
    pos = gx ^ gz
    block = gy * nz + gz
    edge = jnp.where(pos == 0, 0, ny * nz - 1)
    return gx, gz, pos, block != edge


def lane_of(shape):
    return lax.broadcasted_iota(jnp.int32, shape, 1)


def pack_rows_kernel(
    traits, intensity, temp, label, patch, block, out, beside, across, table
):
    layers, rows, width = temp.shape
    groups = LANES // (2 * rows)
    deep = layers // groups
    pos = position()[2]
    kinds, count = traits.shape
    for k in range(kinds):
        for m in range(count):
            table[k * count + m] = jnp.full((8, LANES), traits[k, m], f32)
    for k in range(intensity.shape[0]):
        table[kinds * count + k] = jnp.full((8, LANES), intensity[k], f32)
    wide = width // 2 + HALO
    inner = pl.multiple_of((width - wide) * (1 - pos), 8)
    near = pl.multiple_of((width - HALO) * pos, 8)
    far = pl.multiple_of((width - HALO) * (1 - pos), 8)
    for a, ref in enumerate((temp, label, patch)):
        for p in range(deep // 2):
            parts = [ref[g * deep + 2 * p + j] for j in range(2) for g in range(groups)]
            block[a, p] = jnp.concatenate(parts, axis=0).astype(f32).T
            out[a, p] = block[a, p, pl.ds(inner, wide), :]
            beside[a, p] = block[a, p, pl.ds(near, HALO), :]
            across[a, p] = block[a, p, pl.ds(far, HALO), :]


def picks(ref, l, row):
    def at(dz, dx):
        return ref[l + 1 + dz, PAD + row + dx : PAD + row + dx + 8, :]

    out = {}
    for dx in (-1, 0, 1):
        up, mid, down = at(1, dx), at(0, dx), at(-1, dx)
        out["F", dx] = mid
        out["G", dx] = up + down
        out["H", dx] = up - down
    res = {}
    for k in "FGH":
        res[k] = out[k, 0]
        res["E" + k] = out[k, 1] + out[k, -1]
        res["D" + k] = out[k, 1] - out[k, -1]
    return res


def next_row(x, full):
    kept = lane_of(x.shape) % full != full - 1
    return jnp.where(kept, pltpu.roll(x, LANES - 1, 1), 0.0)


def last_row(x, full):
    kept = lane_of(x.shape) % full != 0
    return jnp.where(kept, pltpu.roll(x, 1, 1), 0.0)


def pair_sum(x, full):
    return next_row(x, full) + last_row(x, full)


def pair_difference(x, full):
    return next_row(x, full) - last_row(x, full)


def along_lanes(base, even, odd, full):
    return base + next_row(even + odd, full) + last_row(even - odd, full)


def wrap_layers(refs, full):
    for ref in refs:
        deep, height = ref.shape[-3] - 2, ref.shape[-2]
        for index in ([()] if len(ref.shape) == 3 else [(c,) for c in range(ref.shape[0])]):
            for r in range(PAD, height - PAD, 8):
                here = (slice(r, r + 8), slice(None))
                group = lane_of((8, LANES)) // full
                below = pltpu.roll(ref[index + (deep,) + here], full, 1)
                ref[index + (0,) + here] = jnp.where(group == 0, 0.0, below)
                above = pltpu.roll(ref[index + (1,) + here], LANES - full, 1)
                ref[index + (deep + 1,) + here] = jnp.where(
                    group == LANES // full - 1, 0.0, above
                )


N5 = 5.0 / 9.0
N2 = 2.0 / 9.0
N3 = 1.0 / 3.0


def full_stencil(z, x, y, full):
    base0 = z["EF"] + z["EG"] + 3.0 * z["G"] + 0.5 * x["DH"]
    even0 = z["F"] + z["G"] + 0.5 * z["EF"] + N5 * z["EG"] + N2 * x["DH"]
    odd0 = 0.5 * y["H"] + N2 * y["EH"]
    base1 = 3.0 * x["EF"] + x["G"] + x["EG"] + 0.5 * z["DH"]
    even1 = x["F"] + x["EF"] + 0.5 * x["G"] + N5 * x["EG"] + N2 * z["DH"]
    odd1 = 0.5 * y["DF"] + N2 * y["DG"]
    shared = y["EF"] + y["G"]
    base2 = shared + 0.5 * y["EG"]
    even2 = shared + 3.0 * y["F"] + N5 * y["EG"]
    odd2 = 0.5 * (x["DF"] + z["H"]) + N2 * (x["DG"] + z["EH"])
    return (
        along_lanes(base0, even0, odd0, full),
        along_lanes(base1, even1, odd1, full),
        along_lanes(base2, even2, odd2, full),
    )


def matrix_stencil(m, full):
    both = m["EF"] + m["EG"]
    shared = m["EF"] + m["G"]
    tail = N5 * m["EG"]
    zz = both + 3.0 * m["G"] + pair_sum(m["F"] + m["G"] + 0.5 * m["EF"] + tail, full)
    xx = 3.0 * m["EF"] + m["G"] + m["EG"] + pair_sum(m["F"] + m["EF"] + 0.5 * m["G"] + tail, full)
    yy = shared + 0.5 * m["EG"] + pair_sum(shared + 3.0 * m["F"] + tail, full)
    zx = 0.5 * m["DH"] + pair_sum(N2 * m["DH"], full)
    zy = pair_difference(0.5 * m["H"] + N2 * m["EH"], full)
    xy = pair_difference(0.5 * m["DF"] + N2 * m["DG"], full)
    return zz, xx, yy, zx, zy, xy


def gradient_stencil(f, full):
    gz = f["H"] + 0.5 * f["EH"] + pair_sum(0.5 * f["H"] + N3 * f["EH"], full)
    gx = f["DF"] + 0.5 * f["DG"] + pair_sum(0.5 * f["DF"] + N3 * f["DG"], full)
    gy = pair_difference(f["F"] + 0.5 * (f["G"] + f["EF"]) + N3 * f["EG"], full)
    return gz, gx, gy


def conduct(own, other):
    return 2.0 * own * other / jnp.maximum(own + other, 0.25)


def choose(label, values):
    out = jnp.zeros(label.shape, f32)
    for k, v in enumerate(values):
        out = jnp.where(label == float(k), v, out)
    return out


def shift_scale(table, count):
    total = table[2 * count]
    for k in range(1, count):
        total = total + table[2 * count + k]
    return total * ((anchor_scale + 2.0 * CENTRE) / count)


def packed_lanes(values, full, row_half, layer_half):
    lane = lane_of((8, LANES))
    rows = full // 2
    out = None
    for i, value in enumerate(values):
        target = (i // 2) * (LANES // 2) + (i % 2) * rows
        shift = target - layer_half * (LANES // 2) - row_half * rows + 2 * LANES
        moved = pltpu.roll(value, shift % LANES, 1)
        mine = ((lane // (LANES // 2)) == i // 2) & ((lane // rows) % 2 == i % 2)
        out = moved if out is None else jnp.where(mine, moved, out)
    return out


def pack_vectors(v, outs, warm, full):
    fields, deep, own, _ = v.shape
    gx, gz, _, _ = position()

    def piece(f, _):
        for number, out in enumerate(outs):
            row_half, layer_half = gx ^ (number % 2), gz ^ (number // 2)
            for r in range(0, own, 8):
                values = [v[f, i, r : r + 8, :] for i in range(deep)]
                out[f, r : r + 8, :] = packed_lanes(values, full, row_half, layer_half)
        return 0

    lax.fori_loop(0, fields, piece, 0)
    if warm is not None:
        for number in range(2):
            for layer_half in range(2):
                for r in range(0, own, 8):
                    values = [warm[i, r : r + 8, :] for i in range(deep)]
                    outs[number][fields + layer_half, r : r + 8, :] = packed_lanes(
                        values, full, gx ^ number, layer_half
                    )


def power_step(weight, mats, inside, source, dest, v, first_field, square_too, full):
    u, w = source
    deep, width = mats.shape[1], mats.shape[2]
    own = range(HALO, width - HALO, 8)
    tiles = own if dest is None else range(0, width, 8)

    def step(l, accs):
        accs = list(accs)
        for r in tiles:
            here = slice(PAD + r, PAD + r + 8)
            there = slice(r, r + 8)
            found, stencils = [], []
            for ref in (u, w):
                f = [picks(ref.at[c], l, r) for c in range(3)]
                found.append([x["F"] for x in f])
                stencils.append(full_stencil(*f, full))
            old, weighted = found
            cu, cw = stencils
            zz, xx, yy, zx, zy, xy = (mats[k, l, there, :] for k in range(6))
            mixed = (
                zz * old[0] + zx * old[1] + zy * old[2],
                zx * old[0] + xx * old[1] + xy * old[2],
                zy * old[0] + xy * old[1] + yy * old[2],
            )
            m = weight[l, there, :]
            keep = inside[there, :]
            for c in range(3):
                new = (K4 * weighted[c] + mixed[c] - m * cu[c] - cw[c]) * keep
                if dest is not None:
                    dest[0][c, l + 1, here, :] = new
                    dest[1][c, l + 1, here, :] = new * m
                if r in own:
                    v[first_field + c, l, r - HALO : r - HALO + 8, :] = new
                    accs[0] = accs[0] + new * old[c]
                    if square_too:
                        accs[1] = accs[1] + new * new
        return tuple(accs)

    zero = jnp.zeros((8, LANES), f32)
    accs = lax.fori_loop(0, deep, step, (zero,) * (2 if square_too else 1))
    if dest is not None:
        wrap_layers(dest, full)
    return accs


def clear_edges(refs):
    edge = jnp.zeros((PAD, LANES), f32)
    for ref in refs:
        height = ref.shape[-2]
        for index in ([()] if len(ref.shape) == 3 else [(c,) for c in range(ref.shape[0])]):
            for l in range(ref.shape[-3]):
                ref[index + (l, slice(0, PAD))] = edge
                ref[index + (l, slice(height - PAD, height))] = edge


def first_kernel(
    table, block, got, beside, across,
    weight, mats, inside, u_next, w_next, moments, mine, to_x, to_z, to_both,
    cond, temp_a, temp_b, cap, power, gz, gx, gy, gy_back, expand, strain, prod, u, w, v, warm,
    mod, source, win,
    *, count, full,
):
    pairs, wide = got.shape[1], got.shape[2]
    deep, width = mats.shape[1], mats.shape[2]
    rows = full // 2
    groups = LANES // full
    me, _, pos, paired = position()
    tiles = range(0, width, 8)
    kinds = 4
    sources = table.shape[0] - kinds * count

    inv_scale = 1.0 / shift_scale(table, count)
    cond_t = [table[k] for k in range(count)]
    cap_t = [time_step / table[count + k] for k in range(count)]
    mod_t = [table[2 * count + k] for k in range(count)]
    exp_t = [table[3 * count + k] for k in range(count)]
    pow_t = [table[kinds * count + k] for k in range(sources)]

    clear_edges((cond, temp_a, temp_b, mod, strain, prod, u, w, u_next, w_next))
    for l in range(deep):
        gx[l, 0:PAD] = jnp.zeros((PAD, LANES), f32)

    body = pl.multiple_of(HALO * (1 - pos), 8)
    strip = pl.multiple_of((width - HALO) * pos, 8)
    inner = pl.multiple_of((block.shape[2] - wide) * pos, 8)
    for a in range(3):
        for p in range(pairs):
            source[me, a * pairs + p, pl.ds(body, wide), :] = block[a, p, pl.ds(inner, wide), :]
            source[1 - me, a * pairs + p, pl.ds(body, wide), :] = got[a, p]
            for half, ref in ((me, beside), (1 - me, across)):
                value = ref[a, p]
                if a == 1:
                    value = jnp.where(paired, value, -1.0)
                source[half, a * pairs + p, pl.ds(strip, HALO), :] = value

    def window(k, _):
        lane = lane_of((8, LANES))
        for r in tiles:
            for j in range(2):
                value = None
                for half in range(2):
                    read = source[half, k, r : r + 8, :]
                    for g in range(groups):
                        shift = (g * full + half * rows - j * (LANES // 2) - g * rows) % LANES
                        moved = pltpu.roll(read, shift, 1) if shift else read
                        if value is None:
                            value = moved
                        else:
                            value = jnp.where(lane // rows == 2 * g + half, moved, value)
                win[2 * k + j, r : r + 8, :] = value
        return 0

    lax.fori_loop(0, 3 * pairs, window, 0)

    def looked_up(l, _):
        for r in tiles:
            here = slice(PAD + r, PAD + r + 8)
            there = slice(r, r + 8)
            temp_a[l + 1, here, :] = win[l, there, :]
            lab = win[deep + l, there, :]
            src = win[2 * deep + l, there, :]
            cond[l + 1, here, :] = choose(lab, cond_t)
            cap[l, there, :] = choose(lab, cap_t)
            mod[l + 1, here, :] = choose(lab, mod_t)
            expand[l, there, :] = choose(lab, exp_t)
            power[l, there, :] = choose(src, pow_t)
            inside[there, :] = jnp.where(lab >= 0.0, 1.0, 0.0)
        return 0

    lax.fori_loop(0, deep, looked_up, 0)
    wrap_layers((temp_a, cond, mod), full)

    for r in tiles:
        here = slice(PAD + r, PAD + r + 8)
        gz[0, r : r + 8, :] = conduct(cond[0, here, :], cond[1, here, :])

    def faces(l, _):
        for r in tiles:
            here = slice(PAD + r, PAD + r + 8)
            there = slice(r, r + 8)
            a = cond[l + 1, here, :]
            gz[l + 1, there, :] = conduct(a, cond[l + 2, here, :])
            gx[l, here, :] = conduct(a, cond[l + 1, PAD + r + 1 : PAD + r + 9, :])
            gy[l, there, :] = conduct(a, next_row(a, full))
            gy_back[l, there, :] = conduct(a, last_row(a, full))
        return 0

    lax.fori_loop(0, deep, faces, 0)

    def heat(src, dst, last):
        def step(l, _):
            for r in tiles:
                here = slice(PAD + r, PAD + r + 8)
                there = slice(r, r + 8)
                t = src[l + 1, here, :]
                flux = gz[l + 1, there, :] * (src[l + 2, here, :] - t)
                flux += gz[l, there, :] * (src[l, here, :] - t)
                flux += gx[l, here, :] * (src[l + 1, PAD + r + 1 : PAD + r + 9, :] - t)
                flux += gx[l, PAD + r - 1 : PAD + r + 7, :] * (
                    src[l + 1, PAD + r - 1 : PAD + r + 7, :] - t
                )
                flux += gy[l, there, :] * (pltpu.roll(t, LANES - 1, 1) - t)
                flux += gy_back[l, there, :] * (pltpu.roll(t, 1, 1) - t)
                new = t + cap[l, there, :] * (flux + power[l, there, :])
                if last:
                    if HALO <= r < width - HALO:
                        warm[l, r - HALO : r - HALO + 8, :] = new
                    s = expand[l, there, :] * new
                    strain[l + 1, here, :] = s
                    prod[l + 1, here, :] = s * mod[l + 1, here, :]
                else:
                    dst[l + 1, here, :] = new
            return 0

        lax.fori_loop(0, deep, step, 0, unroll=2)

    heat(temp_a, temp_b, False)
    wrap_layers((temp_b,), full)
    heat(temp_b, None, True)
    wrap_layers((strain, prod), full)

    quarter_scale = 0.25 * inv_scale

    def loads(l, acc):
        for r in tiles:
            here = slice(PAD + r, PAD + r + 8)
            there = slice(r, r + 8)
            s = picks(strain, l, r)
            m = picks(mod, l, r)
            q = picks(prod, l, r)
            gs, gm, gq = (gradient_stencil(f, full) for f in (s, m, q))
            for k, entry in enumerate(matrix_stencil(m, full)):
                entry = entry * quarter_scale
                mats[k, l, there, :] = entry - 1.0 if k < 3 else entry
            scaled = m["F"] * quarter_scale
            weight[l, there, :] = scaled
            keep = inside[there, :] * (-0.25 * strain_gain)
            for c in range(3):
                new = (m["F"] * gs[c] + s["F"] * gm[c] + gq[c]) * keep
                u[c, l + 1, here, :] = new
                w[c, l + 1, here, :] = new * scaled
                if HALO <= r < width - HALO:
                    v[c, l, r - HALO : r - HALO + 8, :] = new
                    acc = acc + new * new
        return acc

    moments[0] = lax.fori_loop(0, deep, loads, jnp.zeros((8, LANES), f32))
    wrap_layers((u, w), full)
    cross, square = power_step(
        weight, mats, inside, (u, w), (u_next, w_next), v, 3, True, full
    )
    moments[1] = cross
    moments[2] = square
    pack_vectors(v, (mine, to_x, to_z, to_both), warm, full)


def second_kernel(
    weight, mats, inside, u, w, moments,
    mom_out, mine, to_x, to_z, to_both,
    u_next, w_next, v,
    *, full,
):
    clear_edges((u_next, w_next))
    parts = [moments[k] for k in range(moments.shape[0])]
    parts += power_step(weight, mats, inside, (u, w), (u_next, w_next), v, 0, True, full)
    parts += power_step(weight, mats, inside, (u_next, w_next), None, v, 3, False, full)
    lane1 = lane_of((1, LANES))
    row = jnp.zeros((1, LANES), f32)
    for k, part in enumerate(parts):
        lanes = jnp.sum(part, axis=0, keepdims=True)
        row = jnp.where(lane1 == k, jnp.sum(lanes, axis=1, keepdims=True), row)
    for k in range(mom_out.shape[0]):
        mom_out[k] = row
    pack_vectors(v, (mine, to_x, to_z, to_both), None, full)


def coefficients(mu, scale):
    def inner(a, b):
        total = None
        for i, x in enumerate(a):
            for j, y in enumerate(b):
                term = x * y * mu[i + j]
                total = term if total is None else total + term
        return total

    def added(a, b):
        out = []
        for k in range(max(len(a), len(b))):
            if k >= len(a):
                out.append(b[k])
            elif k >= len(b):
                out.append(a[k])
            else:
                out.append(a[k] + b[k])
        return out

    one = jnp.ones_like(mu[0])
    residual = [one]
    direction = [one]
    solution = []
    norm = mu[0]
    for number in range(ITERS):
        image = added(direction, [jnp.zeros_like(one)] + direction)
        alpha = norm / inner(direction, image)
        solution = added(solution, [alpha * d for d in direction])
        residual = added(residual, [-alpha * d for d in image])
        if number + 1 < ITERS:
            following = inner(residual, residual)
            ratio = following / norm
            direction = added(residual, [ratio * d for d in direction])
            norm = following
    return [s / scale for s in solution], residual


def place_kernel(table, mom, *refs, count, full):
    early, late, outs, board = refs[:4], refs[4:8], refs[8:11], refs[11]
    warm_out, sol_out, res_out = outs
    layers, rows, _ = warm_out.shape
    deep = layers // (LANES // full)
    own = early[2].shape[1]
    _, gz, pos, _ = position()
    shape = (8, LANES)
    total = jnp.broadcast_to(jnp.sum(mom[:, 0, :], axis=0, keepdims=True), shape)
    mu = []
    for k in range(2 * ITERS):
        picked = jnp.where(lane_of(shape) == k, total, 0.0)
        mu.append(jnp.broadcast_to(jnp.sum(picked, axis=1, keepdims=True), shape))
    sol, res = coefficients(mu, shift_scale(table, count))

    def spread(slot, out, lanes, layer0):
        turned = board[slot].T
        for i in range(deep):
            for g in range(2):
                at = (i // 2) * (LANES // 2) + g * full + (i % 2) * rows
                out[layer0 + g * deep + i, :, lanes] = turned[at : at + rows]

    for half in range(2):
        for number in range(2):
            at = pl.multiple_of((pos ^ number) * own, own)
            board[half, pl.ds(at, own), :] = early[number][6 + half]
        spread(half, warm_out, slice(None), half * (layers // 2))
    slot = 2
    for block in range(2):
        lanes = pl.ds(pl.multiple_of((gz ^ block) * LANES, LANES), LANES)
        for c in range(3):
            for number in range(2):
                a, b = early[2 * block + number], late[2 * block + number]
                at = pl.multiple_of((pos ^ block ^ number) * own, own)
                for r in range(0, own, 8):
                    there = slice(r, r + 8)
                    values = (a[c, there, :], a[3 + c, there, :], b[c, there, :], b[3 + c, there, :])
                    x = sol[0] * values[0]
                    y = res[0] * values[0]
                    for k in range(1, ITERS + 1):
                        if k < ITERS:
                            x = x + sol[k] * values[k]
                        y = y + res[k] * values[k]
                    board[slot, pl.ds(at + r, 8), :] = x
                    board[slot + 1, pl.ds(at + r, 8), :] = y
            spread(slot, sol_out.at[(0, 2, 1)[c]], lanes, 0)
            spread(slot + 1, res_out.at[(0, 2, 1)[c]], lanes, 0)
            slot += 2


LIMIT = 28 * 1024 * 1024


def params():
    return pltpu.CompilerParams(vmem_limit_bytes=LIMIT)


def vmem():
    return pl.BlockSpec(memory_space=pltpu.VMEM)


def smem():
    return pl.BlockSpec(memory_space=pltpu.SMEM)


def per_device_fast(temp, label, patch, traits, intensity):
    nx, ny, nz = (lax.axis_size(a) for a in AXES)
    layers, rows, width = temp.shape
    full = rows * nx
    half = layers // 2
    devices = nx * ny * nz

    def number(x, b):
        return x * ny * nz + b

    def everywhere(dx, dz):
        return [
            (number(x, y * nz + z), number(x ^ dx, y * nz + (z ^ dz)))
            for x in range(nx) for y in range(ny) for z in range(nz)
        ]

    def side(x, b):
        return x ^ (b % nz)

    chain = []
    for b in range(1, ny * nz):
        left = [x for x in range(nx) if side(x, b - 1) == 1][0]
        right = [x for x in range(nx) if side(x, b) == 0][0]
        chain += [(number(left, b - 1), number(right, b)), (number(right, b), number(left, b - 1))]

    cross = []
    for x in range(nx):
        for b in range(ny * nz):
            toward = b - 1 if side(x, b) == 0 else b + 1
            if 0 <= toward < ny * nz:
                cross.append((number(x ^ 1, toward), number(x, b)))

    sds = lambda *s: jax.ShapeDtypeStruct(s, f32)
    held = lambda *s: pltpu.VMEM(s, f32)
    keep = lambda x: pltpu.with_memory_space_constraint(x, pltpu.VMEM)
    there = lambda x: pltpu.with_memory_space_constraint(x, pltpu.HBM)
    count = traits.shape[1]
    entries = traits.size + intensity.size
    groups = LANES // full
    deep = layers // groups
    mid = width // 2
    wide = mid + HALO
    own, to_partner, to_beside, to_across, table = pl.pallas_call(
        pack_rows_kernel,
        out_shape=(
            held(3, deep // 2, width, LANES), held(3, deep // 2, wide, LANES),
            held(3, deep // 2, HALO, LANES), held(3, deep // 2, HALO, LANES),
            held(entries, 8, LANES),
        ),
        in_specs=[smem(), smem(), vmem(), vmem(), vmem()],
        out_specs=(vmem(),) * 5,
        compiler_params=params(),
        name="pack_rows",
    )(there(traits), there(intensity), there(temp), there(label), there(patch))
    own, table = keep(own), keep(table)
    got = lax.ppermute(to_partner, AXES, everywhere(1, 0))
    across = lax.ppermute(to_across, AXES, cross)
    beside = lax.ppermute(to_beside, AXES, chain)
    got, across, beside = keep(got), keep(across), keep(beside)

    span = mid + 2 * HALO
    edged = (deep + 2, span + 2 * PAD, LANES)
    plain = (deep, span, LANES)
    padded = pltpu.VMEM(edged, f32)
    flat = pltpu.VMEM(plain, f32)
    vectors = pltpu.VMEM((3,) + edged, f32)
    packed = pltpu.VMEM((6, deep, mid, LANES), f32)
    first = pl.pallas_call(
        functools.partial(first_kernel, count=count, full=full),
        out_shape=(
            held(*plain), held(6, *plain), held(span, LANES), held(3, *edged), held(3, *edged),
            held(3, 8, LANES),
        ) + tuple(held(k, mid, LANES) for k in (8, 8, 6, 6)),
        in_specs=[vmem()] * 5,
        out_specs=(vmem(),) * 10,
        scratch_shapes=[
            padded, padded, padded, flat, flat,
            pltpu.VMEM((deep + 1, span, LANES), f32),
            pltpu.VMEM((deep, span + 2 * PAD, LANES), f32), flat, flat,
            flat, padded, padded, vectors, vectors,
            packed, pltpu.VMEM((deep, mid, LANES), f32), padded,
            pltpu.VMEM((2, 3 * (deep // 2), span, LANES), f32),
            pltpu.VMEM((3 * deep, span, LANES), f32),
        ],
        compiler_params=params(),
        name="first",
    )(table, own, got, beside, across)
    carried, early = first[:6], first[6:]

    def exchanged(mine, *pieces):
        moved = [mine]
        for (dx, dz), piece in zip(((1, 0), (0, 1), (1, 1)), pieces):
            moved.append(lax.ppermute(piece, AXES, everywhere(dx, dz)))
        return tuple(keep(x) for x in moved)

    early = exchanged(*early)
    second = pl.pallas_call(
        functools.partial(second_kernel, full=full),
        out_shape=(held(devices, 1, LANES),)
        + tuple(held(6, mid, LANES) for _ in range(4)),
        in_specs=[vmem()] * 6,
        out_specs=(vmem(),) * 5,
        scratch_shapes=[vectors, vectors, packed],
        compiler_params=params(),
        name="second",
    )(*(keep(x) for x in carried))
    late = exchanged(*second[1:])
    mom = lax.all_to_all(second[0], AXES, 0, 0, tiled=True)
    mom = keep(mom)
    return pl.pallas_call(
        functools.partial(place_kernel, count=count, full=full),
        out_shape=(
            sds(layers, rows, width),
            sds(3, half, rows, nz * width),
            sds(3, half, rows, nz * width),
        ),
        in_specs=[vmem()] * 10,
        out_specs=(vmem(),) * 3,
        scratch_shapes=[pltpu.VMEM((14, width, LANES), f32)],
        compiler_params=params(),
        name="place",
    )(table, mom, *early, *late)


def padded(value, sides, width):
    for axis, dim in sides:
        devices, length = (lax.axis_size(axis), value.shape[dim])
        up = [(i, (i + 1) % devices) for i in range(devices - 1)]
        down = [(j, i) for i, j in up]
        last = lax.slice_in_dim(value, length - width, length, axis=dim)
        initial = lax.slice_in_dim(value, 0, width, axis=dim)
        before = lax.ppermute(last, axis, up)
        after = lax.ppermute(initial, axis, down)
        value = jnp.concatenate([before, value, after], axis=dim)
    return value


def lookup(identity, table, count):
    summed = jnp.zeros(identity.shape, jnp.float32)
    for number in range(count):
        summed = summed + jnp.where(identity == number, table[number], jnp.float32(0.0))
    return summed


def heat_step(padded_temp, padded_cond, power, inverse_cap):
    centre = padded_temp[:, 1:-1, 1:-1]
    own = padded_cond[:, 1:-1, 1:-1]
    layers, rows, columns = centre.shape
    heat_flux = jnp.zeros_like(centre)
    for row_offset, column_offset in ((0, 1), (2, 1), (1, 0), (1, 2)):
        neighbour = padded_temp[
            :, row_offset : row_offset + rows, column_offset : column_offset + columns
        ]
        other = padded_cond[
            :, row_offset : row_offset + rows, column_offset : column_offset + columns
        ]
        heat_flux = heat_flux + conduct(own, other) * (neighbour - centre)
    vertical_temp = jnp.pad(centre, ((1, 1), (0, 0), (0, 0)))
    vertical_cond = jnp.pad(own, ((1, 1), (0, 0), (0, 0)))
    for layer_offset in (0, 2):
        other = vertical_cond[layer_offset : layer_offset + layers]
        neighbour = vertical_temp[layer_offset : layer_offset + layers]
        heat_flux = heat_flux + conduct(own, other) * (neighbour - centre)
    return centre + time_step * inverse_cap * (heat_flux + power)


def neighbour_offsets():
    listed = []
    for along_z in (-1, 0, 1):
        for along_x in (-1, 0, 1):
            for along_y in (-1, 0, 1):
                if along_z != 0 or along_x != 0 or along_y != 0:
                    listed.append((along_z, along_x, along_y))
    return listed


def apply_operator(field, padded_field, modulus, padded_modulus):
    layers, rows, columns = modulus.shape
    parts = [
        anchor_scale * modulus * field[0],
        anchor_scale * modulus * field[1],
        anchor_scale * modulus * field[2],
    ]
    for along_z, along_x, along_y in neighbour_offsets():
        length_sq = along_z * along_z + along_x * along_x + along_y * along_y
        window = (
            slice(1 + along_z, 1 + along_z + layers),
            slice(1 + along_x, 1 + along_x + rows),
            slice(1 + along_y, 1 + along_y + columns),
        )
        weight = 0.5 / length_sq * (modulus + padded_modulus[window])
        change = [field[index_c] - padded_field[index_c][window] for index_c in range(3)]
        projected = (along_z * change[0] + along_x * change[1] + along_y * change[2]) / length_sq
        for index_c, direction_part in enumerate((along_z, along_x, along_y)):
            parts[index_c] = parts[index_c] + weight * (
                0.5 * change[index_c] + direction_part * projected
            )
    return jnp.stack(parts)


def thermal_load(modulus, padded_modulus, strain, padded_strain):
    layers, rows, columns = modulus.shape
    parts = [jnp.zeros_like(modulus), jnp.zeros_like(modulus), jnp.zeros_like(modulus)]
    for along_z, along_x, along_y in neighbour_offsets():
        length_sq = along_z * along_z + along_x * along_x + along_y * along_y
        window = (
            slice(1 + along_z, 1 + along_z + layers),
            slice(1 + along_x, 1 + along_x + rows),
            slice(1 + along_y, 1 + along_y + columns),
        )
        weight = 0.5 / length_sq * (modulus + padded_modulus[window])
        pushing = weight * (0.5 * (strain + padded_strain[window]))
        for index_c, direction_part in enumerate((along_z, along_x, along_y)):
            if direction_part != 0:
                parts[index_c] = parts[index_c] - strain_gain * direction_part * pushing
    return jnp.stack(parts)


def two_products(residual, image):
    return lax.psum((jnp.sum(residual * residual), jnp.sum(residual * image)), ("gx", "gy", "gz"))


def per_device_plain(
    starting_kelvin, substance_label, voxel_source_patch, substance_traits, patch_source_intensity
):
    count = substance_traits.shape[1]
    diffusive_coefficient = lookup(substance_label, substance_traits[0], count)
    inverse_cap = 1.0 / lookup(substance_label, substance_traits[1], count)
    power = lookup(voxel_source_patch, patch_source_intensity, patch_source_intensity.shape[0])
    padded_array = padded(
        jnp.stack([starting_kelvin, diffusive_coefficient]), (("gx", 2), (("gy", "gz"), 3)), 1
    )
    padded_cond = padded_array[1]
    warmed_result = heat_step(padded_array[0], padded_cond, power, inverse_cap)
    number = 0
    extended = padded(warmed_result, (("gx", 1), (("gy", "gz"), 2)), 1)
    warmed_result = heat_step(extended, padded_cond, power, inverse_cap)
    modulus = lookup(substance_label, substance_traits[2], count)
    strain = lookup(substance_label, substance_traits[3], count) * warmed_result
    fields = jnp.stack([modulus, strain])
    vertical_cycle = ((0, 0), (1, 1), (0, 0), (0, 0))
    padded_fields = jnp.pad(padded(fields, (("gx", 2), (("gy", "gz"), 3)), 1), vertical_cycle)

    def extend(field):
        return jnp.pad(padded(field, (("gx", 2), (("gy", "gz"), 3)), 1), vertical_cycle)

    modulus = fields[0]
    padded_modulus = padded_fields[0]
    load = thermal_load(modulus, padded_modulus, fields[1], padded_fields[1])

    def operate(field):
        return apply_operator(field, extend(field), modulus, padded_modulus)

    solution = jnp.zeros_like(load)
    residual = load
    image = operate(residual)
    norm_now, product = two_products(residual, image)
    alpha = norm_now / product
    direction, along_image = (residual, image)
    for number in range(ITERS):
        solution = solution + alpha * direction
        residual = residual - alpha * along_image
        if number + 1 < ITERS:
            image = operate(residual)
            norm_next, product = two_products(residual, image)
            ratio = norm_next / norm_now
            alpha = norm_next / (product - ratio * norm_next / alpha)
            direction = residual + ratio * direction
            along_image = image + ratio * along_image
            norm_now = norm_next
    joined = lax.all_to_all(
        jnp.concatenate([solution, residual]), "gz", split_axis=1, concat_axis=3, tiled=True
    )
    solution = joined[:3]
    residual = joined[3:]
    return (warmed_result, solution, residual)


def solution(mesh):
    in_specs = (
        P(None, "gx", ("gy", "gz")),
        P(None, "gx", ("gy", "gz")),
        P(None, "gx", ("gy", "gz")),
        P(),
        P(),
    )
    out_specs = (P(None, "gx", ("gy", "gz")), P(None, "gz", "gx", "gy"), P(None, "gz", "gx", "gy"))

    def per_device(temp, label, patch, traits, intensity):
        layers, rows, width = temp.shape
        fits = (
            mesh.shape["gx"] == 2
            and mesh.shape["gz"] == 2
            and width == LANES
            and rows % 8 == 0
            and LANES == 4 * 2 * rows
            and layers == 4 * 4
        )
        run = per_device_fast if fits else per_device_plain
        return run(temp, label, patch, traits, intensity)

    return jax.shard_map(
        per_device, mesh=mesh, in_specs=in_specs, out_specs=out_specs, check_vma=False
    )
```

```python
import functools

import jax
import jax.numpy as jnp
from jax import lax
from jax.experimental import pallas as pl
from jax.experimental.pallas import tpu as pltpu
from jax.sharding import PartitionSpec as P


ITERS = 3
HALO = 8
LANES = 128
PAD = 8
AXES = ("gx", "gy", "gz")

time_step = 0.03
anchor_scale = 0.5
strain_gain = 2.0
CENTRE = 55.0 / 9.0
K4 = 4.0 * (anchor_scale + CENTRE)

f32 = jnp.float32


def position():
    gx, gy, gz = (lax.axis_index(a) for a in AXES)
    ny, nz = lax.axis_size("gy"), lax.axis_size("gz")
    pos = gx ^ gz
    block = gy * nz + gz
    edge = jnp.where(pos == 0, 0, ny * nz - 1)
    return gx, gz, pos, block != edge


def lane_of(shape):
    return lax.broadcasted_iota(jnp.int32, shape, 1)


def pack_rows_kernel(
    traits, intensity, temp, label, patch, block, out, beside, across, table
):
    layers, rows, width = temp.shape
    groups = LANES // (2 * rows)
    deep = layers // groups
    pos = position()[2]
    kinds, count = traits.shape
    for k in range(kinds):
        for m in range(count):
            table[k * count + m] = jnp.full((8, LANES), traits[k, m], f32)
    for k in range(intensity.shape[0]):
        table[kinds * count + k] = jnp.full((8, LANES), intensity[k], f32)
    wide = width // 2 + HALO
    inner = pl.multiple_of((width - wide) * (1 - pos), 8)
    near = pl.multiple_of((width - HALO) * pos, 8)
    far = pl.multiple_of((width - HALO) * (1 - pos), 8)
    for a, ref in enumerate((temp, label, patch)):
        for p in range(deep // 2):
            parts = [ref[g * deep + 2 * p + j] for g in range(groups) for j in range(2)]
            block[a, p] = jnp.concatenate(parts, axis=0).astype(f32).T
            out[a, p] = block[a, p, pl.ds(inner, wide), :]
            beside[a, p] = block[a, p, pl.ds(near, HALO), :]
            across[a, p] = block[a, p, pl.ds(far, HALO), :]


def picks(ref, l, row):
    def at(dz, dx):
        return ref[l + 1 + dz, PAD + row + dx : PAD + row + dx + 8, :]

    out = {}
    for dx in (-1, 0, 1):
        up, mid, down = at(1, dx), at(0, dx), at(-1, dx)
        out["F", dx] = mid
        out["G", dx] = up + down
        out["H", dx] = up - down
    res = {}
    for k in "FGH":
        res[k] = out[k, 0]
        res["E" + k] = out[k, 1] + out[k, -1]
        res["D" + k] = out[k, 1] - out[k, -1]
    return res


def next_row(x, full):
    kept = lane_of(x.shape) % full != full - 1
    return jnp.where(kept, pltpu.roll(x, LANES - 1, 1), 0.0)


def last_row(x, full):
    kept = lane_of(x.shape) % full != 0
    return jnp.where(kept, pltpu.roll(x, 1, 1), 0.0)


def pair_sum(x, full):
    return next_row(x, full) + last_row(x, full)


def pair_difference(x, full):
    return next_row(x, full) - last_row(x, full)


def along_lanes(base, even, odd, full):
    return base + next_row(even + odd, full) + last_row(even - odd, full)


def wrap_layers(refs, full):
    for ref in refs:
        deep, height = ref.shape[-3] - 2, ref.shape[-2]
        for index in ([()] if len(ref.shape) == 3 else [(c,) for c in range(ref.shape[0])]):
            for r in range(PAD, height - PAD, 8):
                here = (slice(r, r + 8), slice(None))
                group = lane_of((8, LANES)) // full
                below = pltpu.roll(ref[index + (deep,) + here], full, 1)
                ref[index + (0,) + here] = jnp.where(group == 0, 0.0, below)
                above = pltpu.roll(ref[index + (1,) + here], LANES - full, 1)
                ref[index + (deep + 1,) + here] = jnp.where(
                    group == LANES // full - 1, 0.0, above
                )


N5 = 5.0 / 9.0
N2 = 2.0 / 9.0
N3 = 1.0 / 3.0


def full_stencil(z, x, y, full):
    base0 = z["EF"] + z["EG"] + 3.0 * z["G"] + 0.5 * x["DH"]
    even0 = z["F"] + z["G"] + 0.5 * z["EF"] + N5 * z["EG"] + N2 * x["DH"]
    odd0 = 0.5 * y["H"] + N2 * y["EH"]
    base1 = 3.0 * x["EF"] + x["G"] + x["EG"] + 0.5 * z["DH"]
    even1 = x["F"] + x["EF"] + 0.5 * x["G"] + N5 * x["EG"] + N2 * z["DH"]
    odd1 = 0.5 * y["DF"] + N2 * y["DG"]
    shared = y["EF"] + y["G"]
    base2 = shared + 0.5 * y["EG"]
    even2 = shared + 3.0 * y["F"] + N5 * y["EG"]
    odd2 = 0.5 * (x["DF"] + z["H"]) + N2 * (x["DG"] + z["EH"])
    return (
        along_lanes(base0, even0, odd0, full),
        along_lanes(base1, even1, odd1, full),
        along_lanes(base2, even2, odd2, full),
    )


def matrix_stencil(m, full):
    both = m["EF"] + m["EG"]
    shared = m["EF"] + m["G"]
    tail = N5 * m["EG"]
    zz = both + 3.0 * m["G"] + pair_sum(m["F"] + m["G"] + 0.5 * m["EF"] + tail, full)
    xx = 3.0 * m["EF"] + m["G"] + m["EG"] + pair_sum(m["F"] + m["EF"] + 0.5 * m["G"] + tail, full)
    yy = shared + 0.5 * m["EG"] + pair_sum(shared + 3.0 * m["F"] + tail, full)
    zx = 0.5 * m["DH"] + pair_sum(N2 * m["DH"], full)
    zy = pair_difference(0.5 * m["H"] + N2 * m["EH"], full)
    xy = pair_difference(0.5 * m["DF"] + N2 * m["DG"], full)
    return zz, xx, yy, zx, zy, xy


def gradient_stencil(f, full):
    gz = f["H"] + 0.5 * f["EH"] + pair_sum(0.5 * f["H"] + N3 * f["EH"], full)
    gx = f["DF"] + 0.5 * f["DG"] + pair_sum(0.5 * f["DF"] + N3 * f["DG"], full)
    gy = pair_difference(f["F"] + 0.5 * (f["G"] + f["EF"]) + N3 * f["EG"], full)
    return gz, gx, gy


def conduct(own, other):
    return 2.0 * own * other / jnp.maximum(own + other, 0.25)


def choose(label, values):
    out = jnp.zeros(label.shape, f32)
    for k, v in enumerate(values):
        out = jnp.where(label == float(k), v, out)
    return out


def shift_scale(table, count):
    total = table[2 * count]
    for k in range(1, count):
        total = total + table[2 * count + k]
    return total * ((anchor_scale + 2.0 * CENTRE) / count)


def exchanged_lanes(x, y, distance, swap):
    low = (lane_of(x.shape) // distance) % 2 == 0
    y_up = pltpu.roll(y, distance, 1)
    x_down = pltpu.roll(x, LANES - distance, 1)
    first = jnp.where(low, x, y_up)
    second = jnp.where(low, x_down, y)
    return jnp.where(swap, second, first), jnp.where(swap, first, second)


def owner_lanes(values, rows, swap_rows, swap_layers):
    wide = LANES // 2
    a = exchanged_lanes(values[0], values[2], wide, swap_layers)
    b = exchanged_lanes(values[1], values[3], wide, swap_layers)
    return [exchanged_lanes(x, y, rows, swap_rows) for x, y in zip(a, b)]


def pack_vectors(v, outs, warm, full):
    fields, deep, own, _ = v.shape
    rows = full // 2
    gx, gz, _, _ = position()
    shape = (8, LANES)
    swap_rows = jnp.broadcast_to(gx, shape) == 1
    swap_layers = jnp.broadcast_to(gz, shape) == 1

    def piece(f, _):
        for r in range(0, own, 8):
            made = owner_lanes(
                [v[f, i, r : r + 8, :] for i in range(deep)], rows, swap_rows, swap_layers
            )
            for number, out in enumerate(outs):
                out[f, r : r + 8, :] = made[number // 2][number % 2]
        return 0

    lax.fori_loop(0, fields, piece, 0, unroll=2)
    if warm is not None:
        never = jnp.zeros(shape, jnp.bool_)
        for r in range(0, own, 8):
            made = owner_lanes(
                [warm[i, r : r + 8, :] for i in range(deep)], rows, swap_rows, never
            )
            for number in range(2):
                for layer_half in range(2):
                    outs[number][fields + layer_half, r : r + 8, :] = made[layer_half][number]


def power_step(weight, mats, inside, source, dest, v, first_field, square_too, full):
    u, w = source
    deep, width = mats.shape[1], mats.shape[2]
    own = range(HALO, width - HALO, 8)
    tiles = own if dest is None else range(0, width, 8)

    def step(l, accs):
        accs = list(accs)
        for r in tiles:
            here = slice(PAD + r, PAD + r + 8)
            there = slice(r, r + 8)
            found, stencils = [], []
            for ref in (u, w):
                f = [picks(ref.at[c], l, r) for c in range(3)]
                found.append([x["F"] for x in f])
                stencils.append(full_stencil(*f, full))
            old, weighted = found
            cu, cw = stencils
            zz, xx, yy, zx, zy, xy = (mats[k, l, there, :] for k in range(6))
            mixed = (
                zz * old[0] + zx * old[1] + zy * old[2],
                zx * old[0] + xx * old[1] + xy * old[2],
                zy * old[0] + xy * old[1] + yy * old[2],
            )
            m = weight[l, there, :]
            keep = inside[there, :]
            for c in range(3):
                new = (K4 * weighted[c] + mixed[c] - m * cu[c] - cw[c]) * keep
                if dest is not None:
                    dest[0][c, l + 1, here, :] = new
                    dest[1][c, l + 1, here, :] = new * m
                if r in own:
                    v[first_field + c, l, r - HALO : r - HALO + 8, :] = new
                    accs[0] = accs[0] + new * old[c]
                    if square_too:
                        accs[1] = accs[1] + new * new
        return tuple(accs)

    zero = jnp.zeros((8, LANES), f32)
    accs = lax.fori_loop(0, deep, step, (zero,) * (2 if square_too else 1))
    if dest is not None:
        wrap_layers(dest, full)
    return accs


def clear_edges(refs):
    edge = jnp.zeros((PAD, LANES), f32)
    for ref in refs:
        height = ref.shape[-2]
        for index in ([()] if len(ref.shape) == 3 else [(c,) for c in range(ref.shape[0])]):
            for l in range(ref.shape[-3]):
                ref[index + (l, slice(0, PAD))] = edge
                ref[index + (l, slice(height - PAD, height))] = edge


def first_kernel(
    table, block, got, beside, across,
    weight, mats, inside, u_next, w_next, moments, mine, to_x, to_z, to_both,
    cond, temp_a, temp_b, cap, power, gz, gx, gy, gy_back, expand, strain, prod, u, w, v, warm,
    mod, source, win,
    *, count, full,
):
    pairs, wide = got.shape[1], got.shape[2]
    deep, width = mats.shape[1], mats.shape[2]
    rows = full // 2
    me, _, pos, paired = position()
    tiles = range(0, width, 8)
    kinds = 4
    sources = table.shape[0] - kinds * count

    inv_scale = 1.0 / shift_scale(table, count)
    cond_t = [table[k] for k in range(count)]
    cap_t = [time_step / table[count + k] for k in range(count)]
    mod_t = [table[2 * count + k] for k in range(count)]
    exp_t = [table[3 * count + k] for k in range(count)]
    pow_t = [table[kinds * count + k] for k in range(sources)]

    clear_edges((cond, temp_a, temp_b, mod, strain, prod, u, w, u_next, w_next))
    for l in range(deep):
        gx[l, 0:PAD] = jnp.zeros((PAD, LANES), f32)

    body = pl.multiple_of(HALO * (1 - pos), 8)
    strip = pl.multiple_of((width - HALO) * pos, 8)
    inner = pl.multiple_of((block.shape[2] - wide) * pos, 8)
    for a in range(3):
        for p in range(pairs):
            source[me, a * pairs + p, pl.ds(body, wide), :] = block[a, p, pl.ds(inner, wide), :]
            source[1 - me, a * pairs + p, pl.ds(body, wide), :] = got[a, p]
            for half, ref in ((me, beside), (1 - me, across)):
                value = ref[a, p]
                if a == 1:
                    value = jnp.where(paired, value, -1.0)
                source[half, a * pairs + p, pl.ds(strip, HALO), :] = value

    def window(k, _):
        low = (lane_of((8, LANES)) // rows) % 2 == 0
        for r in tiles:
            x, y = source[0, k, r : r + 8, :], source[1, k, r : r + 8, :]
            win[2 * k, r : r + 8, :] = jnp.where(low, x, pltpu.roll(y, rows, 1))
            win[2 * k + 1, r : r + 8, :] = jnp.where(low, pltpu.roll(x, LANES - rows, 1), y)
        return 0

    lax.fori_loop(0, 3 * pairs, window, 0, unroll=2)

    def looked_up(l, _):
        for r in tiles:
            here = slice(PAD + r, PAD + r + 8)
            there = slice(r, r + 8)
            temp_a[l + 1, here, :] = win[l, there, :]
            lab = win[deep + l, there, :]
            src = win[2 * deep + l, there, :]
            cond[l + 1, here, :] = choose(lab, cond_t)
            cap[l, there, :] = choose(lab, cap_t)
            mod[l + 1, here, :] = choose(lab, mod_t)
            expand[l, there, :] = choose(lab, exp_t)
            power[l, there, :] = choose(src, pow_t)
            inside[there, :] = jnp.where(lab >= 0.0, 1.0, 0.0)
        return 0

    lax.fori_loop(0, deep, looked_up, 0)
    wrap_layers((temp_a, cond, mod), full)

    for r in tiles:
        here = slice(PAD + r, PAD + r + 8)
        gz[0, r : r + 8, :] = conduct(cond[0, here, :], cond[1, here, :])

    def faces(l, _):
        for r in tiles:
            here = slice(PAD + r, PAD + r + 8)
            there = slice(r, r + 8)
            a = cond[l + 1, here, :]
            gz[l + 1, there, :] = conduct(a, cond[l + 2, here, :])
            gx[l, here, :] = conduct(a, cond[l + 1, PAD + r + 1 : PAD + r + 9, :])
            gy[l, there, :] = conduct(a, next_row(a, full))
            gy_back[l, there, :] = conduct(a, last_row(a, full))
        return 0

    lax.fori_loop(0, deep, faces, 0)

    def heat(src, dst, last):
        def step(l, _):
            for r in tiles:
                here = slice(PAD + r, PAD + r + 8)
                there = slice(r, r + 8)
                t = src[l + 1, here, :]
                flux = gz[l + 1, there, :] * (src[l + 2, here, :] - t)
                flux += gz[l, there, :] * (src[l, here, :] - t)
                flux += gx[l, here, :] * (src[l + 1, PAD + r + 1 : PAD + r + 9, :] - t)
                flux += gx[l, PAD + r - 1 : PAD + r + 7, :] * (
                    src[l + 1, PAD + r - 1 : PAD + r + 7, :] - t
                )
                flux += gy[l, there, :] * (pltpu.roll(t, LANES - 1, 1) - t)
                flux += gy_back[l, there, :] * (pltpu.roll(t, 1, 1) - t)
                new = t + cap[l, there, :] * (flux + power[l, there, :])
                if last:
                    if HALO <= r < width - HALO:
                        warm[l, r - HALO : r - HALO + 8, :] = new
                    s = expand[l, there, :] * new
                    strain[l + 1, here, :] = s
                    prod[l + 1, here, :] = s * mod[l + 1, here, :]
                else:
                    dst[l + 1, here, :] = new
            return 0

        lax.fori_loop(0, deep, step, 0, unroll=2)

    heat(temp_a, temp_b, False)
    wrap_layers((temp_b,), full)
    heat(temp_b, None, True)
    wrap_layers((strain, prod), full)

    quarter_scale = 0.25 * inv_scale

    def loads(l, acc):
        for r in tiles:
            here = slice(PAD + r, PAD + r + 8)
            there = slice(r, r + 8)
            s = picks(strain, l, r)
            m = picks(mod, l, r)
            q = picks(prod, l, r)
            gs, gm, gq = (gradient_stencil(f, full) for f in (s, m, q))
            for k, entry in enumerate(matrix_stencil(m, full)):
                entry = entry * quarter_scale
                mats[k, l, there, :] = entry - 1.0 if k < 3 else entry
            scaled = m["F"] * quarter_scale
            weight[l, there, :] = scaled
            keep = inside[there, :] * (-0.25 * strain_gain)
            for c in range(3):
                new = (m["F"] * gs[c] + s["F"] * gm[c] + gq[c]) * keep
                u[c, l + 1, here, :] = new
                w[c, l + 1, here, :] = new * scaled
                if HALO <= r < width - HALO:
                    v[c, l, r - HALO : r - HALO + 8, :] = new
                    acc = acc + new * new
        return acc

    moments[0] = lax.fori_loop(0, deep, loads, jnp.zeros((8, LANES), f32))
    wrap_layers((u, w), full)
    cross, square = power_step(
        weight, mats, inside, (u, w), (u_next, w_next), v, 3, True, full
    )
    moments[1] = cross
    moments[2] = square
    pack_vectors(v, (mine, to_x, to_z, to_both), warm, full)


def second_kernel(
    weight, mats, inside, u, w, moments,
    mom_out, mine, to_x, to_z, to_both,
    u_next, w_next, v,
    *, full,
):
    clear_edges((u_next, w_next))
    parts = [moments[k] for k in range(moments.shape[0])]
    parts += power_step(weight, mats, inside, (u, w), (u_next, w_next), v, 0, True, full)
    parts += power_step(weight, mats, inside, (u_next, w_next), None, v, 3, False, full)
    lane1 = lane_of((1, LANES))
    row = jnp.zeros((1, LANES), f32)
    for k, part in enumerate(parts):
        lanes = jnp.sum(part, axis=0, keepdims=True)
        row = jnp.where(lane1 == k, jnp.sum(lanes, axis=1, keepdims=True), row)
    for k in range(mom_out.shape[0]):
        mom_out[k] = row
    pack_vectors(v, (mine, to_x, to_z, to_both), None, full)


def coefficients(mu, scale):
    def inner(a, b):
        total = None
        for i, x in enumerate(a):
            for j, y in enumerate(b):
                term = x * y * mu[i + j]
                total = term if total is None else total + term
        return total

    def added(a, b):
        out = []
        for k in range(max(len(a), len(b))):
            if k >= len(a):
                out.append(b[k])
            elif k >= len(b):
                out.append(a[k])
            else:
                out.append(a[k] + b[k])
        return out

    one = jnp.ones_like(mu[0])
    residual = [one]
    direction = [one]
    solution = []
    norm = mu[0]
    for number in range(ITERS):
        image = added(direction, [jnp.zeros_like(one)] + direction)
        alpha = norm / inner(direction, image)
        solution = added(solution, [alpha * d for d in direction])
        residual = added(residual, [-alpha * d for d in image])
        if number + 1 < ITERS:
            following = inner(residual, residual)
            ratio = following / norm
            direction = added(residual, [ratio * d for d in direction])
            norm = following
    return [s / scale for s in solution], residual


def place_kernel(table, mom, *refs, count, full):
    early, late, outs, board = refs[:4], refs[4:8], refs[8:11], refs[11]
    warm_out, sol_out, res_out = outs
    layers, rows, _ = warm_out.shape
    deep = layers // (LANES // full)
    own = early[2].shape[1]
    _, gz, pos, _ = position()
    shape = (8, LANES)
    total = jnp.broadcast_to(jnp.sum(mom[:, 0, :], axis=0, keepdims=True), shape)
    mu = []
    for k in range(2 * ITERS):
        picked = jnp.where(lane_of(shape) == k, total, 0.0)
        mu.append(jnp.broadcast_to(jnp.sum(picked, axis=1, keepdims=True), shape))
    sol, res = coefficients(mu, shift_scale(table, count))

    def spread(slot, out, lanes, layer0):
        turned = board[slot].T
        for i in range(deep):
            for g in range(2):
                at = (i // 2) * (LANES // 2) + g * full + (i % 2) * rows
                out[layer0 + g * deep + i, :, lanes] = turned[at : at + rows]

    for half in range(2):
        for number in range(2):
            at = pl.multiple_of((pos ^ number) * own, own)
            board[half, pl.ds(at, own), :] = early[number][6 + half]
        spread(half, warm_out, slice(None), half * (layers // 2))
    slot = 2
    for block in range(2):
        lanes = pl.ds(pl.multiple_of((gz ^ block) * LANES, LANES), LANES)
        for c in range(3):
            for number in range(2):
                a, b = early[2 * block + number], late[2 * block + number]
                at = pl.multiple_of((pos ^ block ^ number) * own, own)
                for r in range(0, own, 8):
                    there = slice(r, r + 8)
                    values = (a[c, there, :], a[3 + c, there, :], b[c, there, :], b[3 + c, there, :])
                    x = sol[0] * values[0]
                    y = res[0] * values[0]
                    for k in range(1, ITERS + 1):
                        if k < ITERS:
                            x = x + sol[k] * values[k]
                        y = y + res[k] * values[k]
                    board[slot, pl.ds(at + r, 8), :] = x
                    board[slot + 1, pl.ds(at + r, 8), :] = y
            spread(slot, sol_out.at[(0, 2, 1)[c]], lanes, 0)
            spread(slot + 1, res_out.at[(0, 2, 1)[c]], lanes, 0)
            slot += 2


LIMIT = 28 * 1024 * 1024


def params():
    return pltpu.CompilerParams(vmem_limit_bytes=LIMIT)


def vmem():
    return pl.BlockSpec(memory_space=pltpu.VMEM)


def smem():
    return pl.BlockSpec(memory_space=pltpu.SMEM)


def per_device_fast(temp, label, patch, traits, intensity):
    nx, ny, nz = (lax.axis_size(a) for a in AXES)
    layers, rows, width = temp.shape
    full = rows * nx
    half = layers // 2
    devices = nx * ny * nz

    def number(x, b):
        return x * ny * nz + b

    def everywhere(dx, dz):
        return [
            (number(x, y * nz + z), number(x ^ dx, y * nz + (z ^ dz)))
            for x in range(nx) for y in range(ny) for z in range(nz)
        ]

    def side(x, b):
        return x ^ (b % nz)

    chain = []
    for b in range(1, ny * nz):
        left = [x for x in range(nx) if side(x, b - 1) == 1][0]
        right = [x for x in range(nx) if side(x, b) == 0][0]
        chain += [(number(left, b - 1), number(right, b)), (number(right, b), number(left, b - 1))]

    cross = []
    for x in range(nx):
        for b in range(ny * nz):
            toward = b - 1 if side(x, b) == 0 else b + 1
            if 0 <= toward < ny * nz:
                cross.append((number(x ^ 1, toward), number(x, b)))

    sds = lambda *s: jax.ShapeDtypeStruct(s, f32)
    held = lambda *s: pltpu.VMEM(s, f32)
    keep = lambda x: pltpu.with_memory_space_constraint(x, pltpu.VMEM)
    there = lambda x: pltpu.with_memory_space_constraint(x, pltpu.HBM)
    count = traits.shape[1]
    entries = traits.size + intensity.size
    groups = LANES // full
    deep = layers // groups
    mid = width // 2
    wide = mid + HALO
    own, to_partner, to_beside, to_across, table = pl.pallas_call(
        pack_rows_kernel,
        out_shape=(
            held(3, deep // 2, width, LANES), held(3, deep // 2, wide, LANES),
            held(3, deep // 2, HALO, LANES), held(3, deep // 2, HALO, LANES),
            held(entries, 8, LANES),
        ),
        in_specs=[smem(), smem(), vmem(), vmem(), vmem()],
        out_specs=(vmem(),) * 5,
        compiler_params=params(),
        name="pack_rows",
    )(there(traits), there(intensity), there(temp), there(label), there(patch))
    own, table = keep(own), keep(table)
    got = lax.ppermute(to_partner, AXES, everywhere(1, 0))
    across = lax.ppermute(to_across, AXES, cross)
    beside = lax.ppermute(to_beside, AXES, chain)
    got, across, beside = keep(got), keep(across), keep(beside)

    span = mid + 2 * HALO
    edged = (deep + 2, span + 2 * PAD, LANES)
    plain = (deep, span, LANES)
    padded = pltpu.VMEM(edged, f32)
    flat = pltpu.VMEM(plain, f32)
    vectors = pltpu.VMEM((3,) + edged, f32)
    packed = pltpu.VMEM((6, deep, mid, LANES), f32)
    first = pl.pallas_call(
        functools.partial(first_kernel, count=count, full=full),
        out_shape=(
            held(*plain), held(6, *plain), held(span, LANES), held(3, *edged), held(3, *edged),
            held(3, 8, LANES),
        ) + tuple(held(k, mid, LANES) for k in (8, 8, 6, 6)),
        in_specs=[vmem()] * 5,
        out_specs=(vmem(),) * 10,
        scratch_shapes=[
            padded, padded, padded, flat, flat,
            pltpu.VMEM((deep + 1, span, LANES), f32),
            pltpu.VMEM((deep, span + 2 * PAD, LANES), f32), flat, flat,
            flat, padded, padded, vectors, vectors,
            packed, pltpu.VMEM((deep, mid, LANES), f32), padded,
            pltpu.VMEM((2, 3 * (deep // 2), span, LANES), f32),
            pltpu.VMEM((3 * deep, span, LANES), f32),
        ],
        compiler_params=params(),
        name="first",
    )(table, own, got, beside, across)
    carried, early = first[:6], first[6:]

    def exchanged(mine, *pieces):
        moved = [mine]
        for (dx, dz), piece in zip(((1, 0), (0, 1), (1, 1)), pieces):
            moved.append(lax.ppermute(piece, AXES, everywhere(dx, dz)))
        return tuple(keep(x) for x in moved)

    early = exchanged(*early)
    second = pl.pallas_call(
        functools.partial(second_kernel, full=full),
        out_shape=(held(devices, 1, LANES),)
        + tuple(held(6, mid, LANES) for _ in range(4)),
        in_specs=[vmem()] * 6,
        out_specs=(vmem(),) * 5,
        scratch_shapes=[vectors, vectors, packed],
        compiler_params=params(),
        name="second",
    )(*(keep(x) for x in carried))
    late = exchanged(*second[1:])
    mom = lax.all_to_all(second[0], AXES, 0, 0, tiled=True)
    mom = keep(mom)
    return pl.pallas_call(
        functools.partial(place_kernel, count=count, full=full),
        out_shape=(
            sds(layers, rows, width),
            sds(3, half, rows, nz * width),
            sds(3, half, rows, nz * width),
        ),
        in_specs=[vmem()] * 10,
        out_specs=(vmem(),) * 3,
        scratch_shapes=[pltpu.VMEM((14, width, LANES), f32)],
        compiler_params=params(),
        name="place",
    )(table, mom, *early, *late)


def padded(value, sides, width):
    for axis, dim in sides:
        devices, length = (lax.axis_size(axis), value.shape[dim])
        up = [(i, (i + 1) % devices) for i in range(devices - 1)]
        down = [(j, i) for i, j in up]
        last = lax.slice_in_dim(value, length - width, length, axis=dim)
        initial = lax.slice_in_dim(value, 0, width, axis=dim)
        before = lax.ppermute(last, axis, up)
        after = lax.ppermute(initial, axis, down)
        value = jnp.concatenate([before, value, after], axis=dim)
    return value


def lookup(identity, table, count):
    summed = jnp.zeros(identity.shape, jnp.float32)
    for number in range(count):
        summed = summed + jnp.where(identity == number, table[number], jnp.float32(0.0))
    return summed


def heat_step(padded_temp, padded_cond, power, inverse_cap):
    centre = padded_temp[:, 1:-1, 1:-1]
    own = padded_cond[:, 1:-1, 1:-1]
    layers, rows, columns = centre.shape
    heat_flux = jnp.zeros_like(centre)
    for row_offset, column_offset in ((0, 1), (2, 1), (1, 0), (1, 2)):
        neighbour = padded_temp[
            :, row_offset : row_offset + rows, column_offset : column_offset + columns
        ]
        other = padded_cond[
            :, row_offset : row_offset + rows, column_offset : column_offset + columns
        ]
        heat_flux = heat_flux + conduct(own, other) * (neighbour - centre)
    vertical_temp = jnp.pad(centre, ((1, 1), (0, 0), (0, 0)))
    vertical_cond = jnp.pad(own, ((1, 1), (0, 0), (0, 0)))
    for layer_offset in (0, 2):
        other = vertical_cond[layer_offset : layer_offset + layers]
        neighbour = vertical_temp[layer_offset : layer_offset + layers]
        heat_flux = heat_flux + conduct(own, other) * (neighbour - centre)
    return centre + time_step * inverse_cap * (heat_flux + power)


def neighbour_offsets():
    listed = []
    for along_z in (-1, 0, 1):
        for along_x in (-1, 0, 1):
            for along_y in (-1, 0, 1):
                if along_z != 0 or along_x != 0 or along_y != 0:
                    listed.append((along_z, along_x, along_y))
    return listed


def apply_operator(field, padded_field, modulus, padded_modulus):
    layers, rows, columns = modulus.shape
    parts = [
        anchor_scale * modulus * field[0],
        anchor_scale * modulus * field[1],
        anchor_scale * modulus * field[2],
    ]
    for along_z, along_x, along_y in neighbour_offsets():
        length_sq = along_z * along_z + along_x * along_x + along_y * along_y
        window = (
            slice(1 + along_z, 1 + along_z + layers),
            slice(1 + along_x, 1 + along_x + rows),
            slice(1 + along_y, 1 + along_y + columns),
        )
        weight = 0.5 / length_sq * (modulus + padded_modulus[window])
        change = [field[index_c] - padded_field[index_c][window] for index_c in range(3)]
        projected = (along_z * change[0] + along_x * change[1] + along_y * change[2]) / length_sq
        for index_c, direction_part in enumerate((along_z, along_x, along_y)):
            parts[index_c] = parts[index_c] + weight * (
                0.5 * change[index_c] + direction_part * projected
            )
    return jnp.stack(parts)


def thermal_load(modulus, padded_modulus, strain, padded_strain):
    layers, rows, columns = modulus.shape
    parts = [jnp.zeros_like(modulus), jnp.zeros_like(modulus), jnp.zeros_like(modulus)]
    for along_z, along_x, along_y in neighbour_offsets():
        length_sq = along_z * along_z + along_x * along_x + along_y * along_y
        window = (
            slice(1 + along_z, 1 + along_z + layers),
            slice(1 + along_x, 1 + along_x + rows),
            slice(1 + along_y, 1 + along_y + columns),
        )
        weight = 0.5 / length_sq * (modulus + padded_modulus[window])
        pushing = weight * (0.5 * (strain + padded_strain[window]))
        for index_c, direction_part in enumerate((along_z, along_x, along_y)):
            if direction_part != 0:
                parts[index_c] = parts[index_c] - strain_gain * direction_part * pushing
    return jnp.stack(parts)


def two_products(residual, image):
    return lax.psum((jnp.sum(residual * residual), jnp.sum(residual * image)), ("gx", "gy", "gz"))


def per_device_plain(
    starting_kelvin, substance_label, voxel_source_patch, substance_traits, patch_source_intensity
):
    count = substance_traits.shape[1]
    diffusive_coefficient = lookup(substance_label, substance_traits[0], count)
    inverse_cap = 1.0 / lookup(substance_label, substance_traits[1], count)
    power = lookup(voxel_source_patch, patch_source_intensity, patch_source_intensity.shape[0])
    padded_array = padded(
        jnp.stack([starting_kelvin, diffusive_coefficient]), (("gx", 2), (("gy", "gz"), 3)), 1
    )
    padded_cond = padded_array[1]
    warmed_result = heat_step(padded_array[0], padded_cond, power, inverse_cap)
    number = 0
    extended = padded(warmed_result, (("gx", 1), (("gy", "gz"), 2)), 1)
    warmed_result = heat_step(extended, padded_cond, power, inverse_cap)
    modulus = lookup(substance_label, substance_traits[2], count)
    strain = lookup(substance_label, substance_traits[3], count) * warmed_result
    fields = jnp.stack([modulus, strain])
    vertical_cycle = ((0, 0), (1, 1), (0, 0), (0, 0))
    padded_fields = jnp.pad(padded(fields, (("gx", 2), (("gy", "gz"), 3)), 1), vertical_cycle)

    def extend(field):
        return jnp.pad(padded(field, (("gx", 2), (("gy", "gz"), 3)), 1), vertical_cycle)

    modulus = fields[0]
    padded_modulus = padded_fields[0]
    load = thermal_load(modulus, padded_modulus, fields[1], padded_fields[1])

    def operate(field):
        return apply_operator(field, extend(field), modulus, padded_modulus)

    solution = jnp.zeros_like(load)
    residual = load
    image = operate(residual)
    norm_now, product = two_products(residual, image)
    alpha = norm_now / product
    direction, along_image = (residual, image)
    for number in range(ITERS):
        solution = solution + alpha * direction
        residual = residual - alpha * along_image
        if number + 1 < ITERS:
            image = operate(residual)
            norm_next, product = two_products(residual, image)
            ratio = norm_next / norm_now
            alpha = norm_next / (product - ratio * norm_next / alpha)
            direction = residual + ratio * direction
            along_image = image + ratio * along_image
            norm_now = norm_next
    joined = lax.all_to_all(
        jnp.concatenate([solution, residual]), "gz", split_axis=1, concat_axis=3, tiled=True
    )
    solution = joined[:3]
    residual = joined[3:]
    return (warmed_result, solution, residual)


def solution(mesh):
    in_specs = (
        P(None, "gx", ("gy", "gz")),
        P(None, "gx", ("gy", "gz")),
        P(None, "gx", ("gy", "gz")),
        P(),
        P(),
    )
    out_specs = (P(None, "gx", ("gy", "gz")), P(None, "gz", "gx", "gy"), P(None, "gz", "gx", "gy"))

    def per_device(temp, label, patch, traits, intensity):
        layers, rows, width = temp.shape
        fits = (
            mesh.shape["gx"] == 2
            and mesh.shape["gz"] == 2
            and width == LANES
            and rows % 8 == 0
            and LANES == 4 * 2 * rows
            and layers == 4 * 4
        )
        run = per_device_fast if fits else per_device_plain
        return run(temp, label, patch, traits, intensity)

    return jax.shard_map(
        per_device, mesh=mesh, in_specs=in_specs, out_specs=out_specs, check_vma=False
    )
```

```python
import functools

import jax
import jax.numpy as jnp
from jax import lax
from jax.experimental import pallas as pl
from jax.experimental.pallas import tpu as pltpu
from jax.sharding import PartitionSpec as P


ITERS = 3
HALO = 8
LANES = 128
PAD = 8
AXES = ("gx", "gy", "gz")

time_step = 0.03
anchor_scale = 0.5
strain_gain = 2.0
CENTRE = 55.0 / 9.0
K4 = 4.0 * (anchor_scale + CENTRE)

f32 = jnp.float32


def position():
    gx, gy, gz = (lax.axis_index(a) for a in AXES)
    ny, nz = lax.axis_size("gy"), lax.axis_size("gz")
    pos = gx ^ gz
    block = gy * nz + gz
    edge = jnp.where(pos == 0, 0, ny * nz - 1)
    return gx, gz, pos, block != edge


def lane_of(shape):
    return lax.broadcasted_iota(jnp.int32, shape, 1)


def pack_rows_kernel(
    traits, intensity, temp, label, patch, block, out, beside, across, table
):
    layers, rows, width = temp.shape
    groups = LANES // (2 * rows)
    deep = layers // groups
    pos = position()[2]
    kinds, count = traits.shape
    for k in range(kinds):
        for m in range(count):
            table[k * count + m] = jnp.full((8, LANES), traits[k, m], f32)
    for k in range(intensity.shape[0]):
        table[kinds * count + k] = jnp.full((8, LANES), intensity[k], f32)
    wide = width // 2 + HALO
    inner = pl.multiple_of((width - wide) * (1 - pos), 8)
    near = pl.multiple_of((width - HALO) * pos, 8)
    far = pl.multiple_of((width - HALO) * (1 - pos), 8)
    for a, ref in enumerate((temp, label, patch)):
        for p in range(deep // 2):
            parts = [ref[g * deep + 2 * p + j] for g in range(groups) for j in range(2)]
            block[a, p] = jnp.concatenate(parts, axis=0).astype(f32).T
            out[a, p] = block[a, p, pl.ds(inner, wide), :]
            beside[a, p] = block[a, p, pl.ds(near, HALO), :]
            across[a, p] = block[a, p, pl.ds(far, HALO), :]


def picks(ref, l, row):
    def at(dz, dx):
        return ref[l + 1 + dz, PAD + row + dx : PAD + row + dx + 8, :]

    out = {}
    for dx in (-1, 0, 1):
        up, mid, down = at(1, dx), at(0, dx), at(-1, dx)
        out["F", dx] = mid
        out["G", dx] = up + down
        out["H", dx] = up - down
    res = {}
    for k in "FGH":
        res[k] = out[k, 0]
        res["E" + k] = out[k, 1] + out[k, -1]
        res["D" + k] = out[k, 1] - out[k, -1]
    return res


def next_row(x, full):
    kept = lane_of(x.shape) % full != full - 1
    return jnp.where(kept, pltpu.roll(x, LANES - 1, 1), 0.0)


def last_row(x, full):
    kept = lane_of(x.shape) % full != 0
    return jnp.where(kept, pltpu.roll(x, 1, 1), 0.0)


def pair_sum(x, full):
    return next_row(x, full) + last_row(x, full)


def pair_difference(x, full):
    return next_row(x, full) - last_row(x, full)


def along_lanes(base, even, odd, full):
    return base + next_row(even + odd, full) + last_row(even - odd, full)


def wrap_layers(refs, full):
    for ref in refs:
        deep, height = ref.shape[-3] - 2, ref.shape[-2]
        for index in ([()] if len(ref.shape) == 3 else [(c,) for c in range(ref.shape[0])]):
            for r in range(PAD, height - PAD, 8):
                here = (slice(r, r + 8), slice(None))
                group = lane_of((8, LANES)) // full
                below = pltpu.roll(ref[index + (deep,) + here], full, 1)
                ref[index + (0,) + here] = jnp.where(group == 0, 0.0, below)
                above = pltpu.roll(ref[index + (1,) + here], LANES - full, 1)
                ref[index + (deep + 1,) + here] = jnp.where(
                    group == LANES // full - 1, 0.0, above
                )


N5 = 5.0 / 9.0
N2 = 2.0 / 9.0
N3 = 1.0 / 3.0


def full_stencil(z, x, y, full):
    base0 = z["EF"] + z["EG"] + 3.0 * z["G"] + 0.5 * x["DH"]
    even0 = z["F"] + z["G"] + 0.5 * z["EF"] + N5 * z["EG"] + N2 * x["DH"]
    odd0 = 0.5 * y["H"] + N2 * y["EH"]
    base1 = 3.0 * x["EF"] + x["G"] + x["EG"] + 0.5 * z["DH"]
    even1 = x["F"] + x["EF"] + 0.5 * x["G"] + N5 * x["EG"] + N2 * z["DH"]
    odd1 = 0.5 * y["DF"] + N2 * y["DG"]
    shared = y["EF"] + y["G"]
    base2 = shared + 0.5 * y["EG"]
    even2 = shared + 3.0 * y["F"] + N5 * y["EG"]
    odd2 = 0.5 * (x["DF"] + z["H"]) + N2 * (x["DG"] + z["EH"])
    return (
        along_lanes(base0, even0, odd0, full),
        along_lanes(base1, even1, odd1, full),
        along_lanes(base2, even2, odd2, full),
    )


def matrix_stencil(m, full):
    both = m["EF"] + m["EG"]
    shared = m["EF"] + m["G"]
    tail = N5 * m["EG"]
    zz = both + 3.0 * m["G"] + pair_sum(m["F"] + m["G"] + 0.5 * m["EF"] + tail, full)
    xx = 3.0 * m["EF"] + m["G"] + m["EG"] + pair_sum(m["F"] + m["EF"] + 0.5 * m["G"] + tail, full)
    yy = shared + 0.5 * m["EG"] + pair_sum(shared + 3.0 * m["F"] + tail, full)
    zx = 0.5 * m["DH"] + pair_sum(N2 * m["DH"], full)
    zy = pair_difference(0.5 * m["H"] + N2 * m["EH"], full)
    xy = pair_difference(0.5 * m["DF"] + N2 * m["DG"], full)
    return zz, xx, yy, zx, zy, xy


def gradient_stencil(f, full):
    gz = f["H"] + 0.5 * f["EH"] + pair_sum(0.5 * f["H"] + N3 * f["EH"], full)
    gx = f["DF"] + 0.5 * f["DG"] + pair_sum(0.5 * f["DF"] + N3 * f["DG"], full)
    gy = pair_difference(f["F"] + 0.5 * (f["G"] + f["EF"]) + N3 * f["EG"], full)
    return gz, gx, gy


def conduct(own, other):
    return 2.0 * own * other / jnp.maximum(own + other, 0.25)


def choose(label, values):
    out = jnp.zeros(label.shape, f32)
    for k, v in enumerate(values):
        out = jnp.where(label == float(k), v, out)
    return out


def shift_scale(table, count):
    total = table[2 * count]
    for k in range(1, count):
        total = total + table[2 * count + k]
    return total * ((anchor_scale + 2.0 * CENTRE) / count)


def exchanged_lanes(x, y, distance, swap):
    low = (lane_of(x.shape) // distance) % 2 == 0
    y_up = pltpu.roll(y, distance, 1)
    x_down = pltpu.roll(x, LANES - distance, 1)
    first = jnp.where(low, x, y_up)
    second = jnp.where(low, x_down, y)
    return jnp.where(swap, second, first), jnp.where(swap, first, second)


def owner_lanes(values, rows, swap_rows, swap_layers):
    wide = LANES // 2
    a = exchanged_lanes(values[0], values[2], wide, swap_layers)
    b = exchanged_lanes(values[1], values[3], wide, swap_layers)
    return [exchanged_lanes(x, y, rows, swap_rows) for x, y in zip(a, b)]


def pack_vectors(v, outs, warm, full):
    fields, deep, own, _ = v.shape
    rows = full // 2
    gx, gz, _, _ = position()
    shape = (8, LANES)
    swap_rows = jnp.broadcast_to(gx, shape) == 1
    swap_layers = jnp.broadcast_to(gz, shape) == 1

    def piece(f, _):
        for r in range(0, own, 8):
            made = owner_lanes(
                [v[f, i, r : r + 8, :] for i in range(deep)], rows, swap_rows, swap_layers
            )
            for number, out in enumerate(outs):
                out[f, r : r + 8, :] = made[number // 2][number % 2]
        return 0

    lax.fori_loop(0, fields, piece, 0, unroll=2)
    if warm is not None:
        never = jnp.zeros(shape, jnp.bool_)
        for r in range(0, own, 8):
            made = owner_lanes(
                [warm[i, r : r + 8, :] for i in range(deep)], rows, swap_rows, never
            )
            for number in range(2):
                for layer_half in range(2):
                    outs[number][fields + layer_half, r : r + 8, :] = made[layer_half][number]


def power_step(weight, mats, inside, source, dest, v, first_field, square_too, full):
    u, w = source
    deep, width = mats.shape[1], mats.shape[2]
    own = range(HALO, width - HALO, 8)
    tiles = own if dest is None else range(0, width, 8)

    def step(l, accs):
        accs = list(accs)
        for r in tiles:
            here = slice(PAD + r, PAD + r + 8)
            there = slice(r, r + 8)
            found, stencils = [], []
            for ref in (u, w):
                f = [picks(ref.at[c], l, r) for c in range(3)]
                found.append([x["F"] for x in f])
                stencils.append(full_stencil(*f, full))
            old, weighted = found
            cu, cw = stencils
            zz, xx, yy, zx, zy, xy = (mats[k, l, there, :] for k in range(6))
            mixed = (
                zz * old[0] + zx * old[1] + zy * old[2],
                zx * old[0] + xx * old[1] + xy * old[2],
                zy * old[0] + xy * old[1] + yy * old[2],
            )
            m = weight[l, there, :]
            keep = inside[there, :]
            for c in range(3):
                new = (K4 * weighted[c] + mixed[c] - m * cu[c] - cw[c]) * keep
                if dest is not None:
                    dest[0][c, l + 1, here, :] = new
                    dest[1][c, l + 1, here, :] = new * m
                if r in own:
                    v[first_field + c, l, r - HALO : r - HALO + 8, :] = new
                    accs[0] = accs[0] + new * old[c]
                    if square_too:
                        accs[1] = accs[1] + new * new
        return tuple(accs)

    zero = jnp.zeros((8, LANES), f32)
    accs = lax.fori_loop(0, deep, step, (zero,) * (2 if square_too else 1))
    if dest is not None:
        wrap_layers(dest, full)
    return accs


def clear_edges(refs):
    edge = jnp.zeros((PAD, LANES), f32)
    for ref in refs:
        height = ref.shape[-2]
        for index in ([()] if len(ref.shape) == 3 else [(c,) for c in range(ref.shape[0])]):
            for l in range(ref.shape[-3]):
                ref[index + (l, slice(0, PAD))] = edge
                ref[index + (l, slice(height - PAD, height))] = edge


def first_kernel(
    table, block, got, beside,
    weight, mats, inside, u_next, w_next, moments, mine, to_x, to_z, to_both,
    cond, temp_a, temp_b, cap, power, gz, gx, gy, gy_back, expand, strain, prod, u, w, v, warm,
    mod, source, win,
    *, count, full,
):
    pairs, wide = got.shape[1], got.shape[2]
    deep, width = mats.shape[1], mats.shape[2]
    rows = full // 2
    me, _, pos, paired = position()
    tiles = range(0, width, 8)
    kinds = 4
    sources = table.shape[0] - kinds * count

    inv_scale = 1.0 / shift_scale(table, count)
    cond_t = [table[k] for k in range(count)]
    cap_t = [time_step / table[count + k] for k in range(count)]
    mod_t = [table[2 * count + k] for k in range(count)]
    exp_t = [table[3 * count + k] for k in range(count)]
    pow_t = [table[kinds * count + k] for k in range(sources)]

    clear_edges((cond, temp_a, temp_b, mod, strain, prod, u, w, u_next, w_next))
    for l in range(deep):
        gx[l, 0:PAD] = jnp.zeros((PAD, LANES), f32)

    body = pl.multiple_of(HALO * (1 - pos), 8)
    strip = pl.multiple_of((width - HALO) * pos, 8)
    inner = pl.multiple_of((block.shape[2] - wide) * pos, 8)
    for a in range(3):
        for p in range(pairs):
            source[me, a * pairs + p, pl.ds(body, wide), :] = block[a, p, pl.ds(inner, wide), :]
            source[1 - me, a * pairs + p, pl.ds(body, wide), :] = got[a, p]
            for k, half in enumerate((me, 1 - me)):
                value = beside[k, a, p]
                if a == 1:
                    value = jnp.where(paired, value, -1.0)
                source[half, a * pairs + p, pl.ds(strip, HALO), :] = value

    def window(k, _):
        low = (lane_of((8, LANES)) // rows) % 2 == 0
        for r in tiles:
            x, y = source[0, k, r : r + 8, :], source[1, k, r : r + 8, :]
            win[2 * k, r : r + 8, :] = jnp.where(low, x, pltpu.roll(y, rows, 1))
            win[2 * k + 1, r : r + 8, :] = jnp.where(low, pltpu.roll(x, LANES - rows, 1), y)
        return 0

    lax.fori_loop(0, 3 * pairs, window, 0, unroll=2)

    def looked_up(l, _):
        for r in tiles:
            here = slice(PAD + r, PAD + r + 8)
            there = slice(r, r + 8)
            temp_a[l + 1, here, :] = win[l, there, :]
            lab = win[deep + l, there, :]
            src = win[2 * deep + l, there, :]
            cond[l + 1, here, :] = choose(lab, cond_t)
            cap[l, there, :] = choose(lab, cap_t)
            mod[l + 1, here, :] = choose(lab, mod_t)
            expand[l, there, :] = choose(lab, exp_t)
            power[l, there, :] = choose(src, pow_t)
            inside[there, :] = jnp.where(lab >= 0.0, 1.0, 0.0)
        return 0

    lax.fori_loop(0, deep, looked_up, 0)
    wrap_layers((temp_a, cond, mod), full)

    for r in tiles:
        here = slice(PAD + r, PAD + r + 8)
        gz[0, r : r + 8, :] = conduct(cond[0, here, :], cond[1, here, :])

    def faces(l, _):
        for r in tiles:
            here = slice(PAD + r, PAD + r + 8)
            there = slice(r, r + 8)
            a = cond[l + 1, here, :]
            gz[l + 1, there, :] = conduct(a, cond[l + 2, here, :])
            gx[l, here, :] = conduct(a, cond[l + 1, PAD + r + 1 : PAD + r + 9, :])
            gy[l, there, :] = conduct(a, next_row(a, full))
            gy_back[l, there, :] = conduct(a, last_row(a, full))
        return 0

    lax.fori_loop(0, deep, faces, 0)

    def heat(src, dst, last):
        def step(l, _):
            for r in tiles:
                here = slice(PAD + r, PAD + r + 8)
                there = slice(r, r + 8)
                t = src[l + 1, here, :]
                flux = gz[l + 1, there, :] * (src[l + 2, here, :] - t)
                flux += gz[l, there, :] * (src[l, here, :] - t)
                flux += gx[l, here, :] * (src[l + 1, PAD + r + 1 : PAD + r + 9, :] - t)
                flux += gx[l, PAD + r - 1 : PAD + r + 7, :] * (
                    src[l + 1, PAD + r - 1 : PAD + r + 7, :] - t
                )
                flux += gy[l, there, :] * (pltpu.roll(t, LANES - 1, 1) - t)
                flux += gy_back[l, there, :] * (pltpu.roll(t, 1, 1) - t)
                new = t + cap[l, there, :] * (flux + power[l, there, :])
                if last:
                    if HALO <= r < width - HALO:
                        warm[l, r - HALO : r - HALO + 8, :] = new
                    s = expand[l, there, :] * new
                    strain[l + 1, here, :] = s
                    prod[l + 1, here, :] = s * mod[l + 1, here, :]
                else:
                    dst[l + 1, here, :] = new
            return 0

        lax.fori_loop(0, deep, step, 0, unroll=2)

    heat(temp_a, temp_b, False)
    wrap_layers((temp_b,), full)
    heat(temp_b, None, True)
    wrap_layers((strain, prod), full)

    quarter_scale = 0.25 * inv_scale

    def loads(l, acc):
        for r in tiles:
            here = slice(PAD + r, PAD + r + 8)
            there = slice(r, r + 8)
            s = picks(strain, l, r)
            m = picks(mod, l, r)
            q = picks(prod, l, r)
            gs, gm, gq = (gradient_stencil(f, full) for f in (s, m, q))
            for k, entry in enumerate(matrix_stencil(m, full)):
                entry = entry * quarter_scale
                mats[k, l, there, :] = entry - 1.0 if k < 3 else entry
            scaled = m["F"] * quarter_scale
            weight[l, there, :] = scaled
            keep = inside[there, :] * (-0.25 * strain_gain)
            for c in range(3):
                new = (m["F"] * gs[c] + s["F"] * gm[c] + gq[c]) * keep
                u[c, l + 1, here, :] = new
                w[c, l + 1, here, :] = new * scaled
                if HALO <= r < width - HALO:
                    v[c, l, r - HALO : r - HALO + 8, :] = new
                    acc = acc + new * new
        return acc

    moments[0] = lax.fori_loop(0, deep, loads, jnp.zeros((8, LANES), f32))
    wrap_layers((u, w), full)
    cross, square = power_step(
        weight, mats, inside, (u, w), (u_next, w_next), v, 3, True, full
    )
    moments[1] = cross
    moments[2] = square
    pack_vectors(v, (mine, to_x, to_z, to_both), warm, full)


def second_kernel(
    weight, mats, inside, u, w, moments,
    mom_out, mine, to_x, to_z, to_both,
    u_next, w_next, v,
    *, full,
):
    clear_edges((u_next, w_next))
    parts = [moments[k] for k in range(moments.shape[0])]
    parts += power_step(weight, mats, inside, (u, w), (u_next, w_next), v, 0, True, full)
    parts += power_step(weight, mats, inside, (u_next, w_next), None, v, 3, False, full)
    lane1 = lane_of((1, LANES))
    row = jnp.zeros((1, LANES), f32)
    for k, part in enumerate(parts):
        lanes = jnp.sum(part, axis=0, keepdims=True)
        row = jnp.where(lane1 == k, jnp.sum(lanes, axis=1, keepdims=True), row)
    for k in range(mom_out.shape[0]):
        mom_out[k] = row
    pack_vectors(v, (mine, to_x, to_z, to_both), None, full)


def coefficients(mu, scale):
    def inner(a, b):
        total = None
        for i, x in enumerate(a):
            for j, y in enumerate(b):
                term = x * y * mu[i + j]
                total = term if total is None else total + term
        return total

    def added(a, b):
        out = []
        for k in range(max(len(a), len(b))):
            if k >= len(a):
                out.append(b[k])
            elif k >= len(b):
                out.append(a[k])
            else:
                out.append(a[k] + b[k])
        return out

    one = jnp.ones_like(mu[0])
    residual = [one]
    direction = [one]
    solution = []
    norm = mu[0]
    for number in range(ITERS):
        image = added(direction, [jnp.zeros_like(one)] + direction)
        alpha = norm / inner(direction, image)
        solution = added(solution, [alpha * d for d in direction])
        residual = added(residual, [-alpha * d for d in image])
        if number + 1 < ITERS:
            following = inner(residual, residual)
            ratio = following / norm
            direction = added(residual, [ratio * d for d in direction])
            norm = following
    return [s / scale for s in solution], residual


def place_kernel(table, mom, *refs, count, full):
    early, late, outs, board = refs[:4], refs[4:8], refs[8:11], refs[11]
    warm_out, sol_out, res_out = outs
    layers, rows, _ = warm_out.shape
    deep = layers // (LANES // full)
    own = early[2].shape[1]
    _, gz, pos, _ = position()
    shape = (8, LANES)
    total = jnp.broadcast_to(jnp.sum(mom[:, 0, :], axis=0, keepdims=True), shape)
    mu = []
    for k in range(2 * ITERS):
        picked = jnp.where(lane_of(shape) == k, total, 0.0)
        mu.append(jnp.broadcast_to(jnp.sum(picked, axis=1, keepdims=True), shape))
    sol, res = coefficients(mu, shift_scale(table, count))

    def spread(slot, out, lanes, layer0):
        turned = board[slot].T
        for i in range(deep):
            for g in range(2):
                at = (i // 2) * (LANES // 2) + g * full + (i % 2) * rows
                out[layer0 + g * deep + i, :, lanes] = turned[at : at + rows]

    for half in range(2):
        for number in range(2):
            at = pl.multiple_of((pos ^ number) * own, own)
            board[half, pl.ds(at, own), :] = early[number][6 + half]
        spread(half, warm_out, slice(None), half * (layers // 2))
    slot = 2
    for block in range(2):
        lanes = pl.ds(pl.multiple_of((gz ^ block) * LANES, LANES), LANES)
        for c in range(3):
            for number in range(2):
                a, b = early[2 * block + number], late[2 * block + number]
                at = pl.multiple_of((pos ^ block ^ number) * own, own)
                for r in range(0, own, 8):
                    there = slice(r, r + 8)
                    values = (a[c, there, :], a[3 + c, there, :], b[c, there, :], b[3 + c, there, :])
                    x = sol[0] * values[0]
                    y = res[0] * values[0]
                    for k in range(1, ITERS + 1):
                        if k < ITERS:
                            x = x + sol[k] * values[k]
                        y = y + res[k] * values[k]
                    board[slot, pl.ds(at + r, 8), :] = x
                    board[slot + 1, pl.ds(at + r, 8), :] = y
            spread(slot, sol_out.at[(0, 2, 1)[c]], lanes, 0)
            spread(slot + 1, res_out.at[(0, 2, 1)[c]], lanes, 0)
            slot += 2


LIMIT = 28 * 1024 * 1024


def params():
    return pltpu.CompilerParams(vmem_limit_bytes=LIMIT)


def vmem():
    return pl.BlockSpec(memory_space=pltpu.VMEM)


def smem():
    return pl.BlockSpec(memory_space=pltpu.SMEM)


def per_device_fast(temp, label, patch, traits, intensity):
    nx, ny, nz = (lax.axis_size(a) for a in AXES)
    layers, rows, width = temp.shape
    full = rows * nx
    half = layers // 2
    devices = nx * ny * nz

    def number(x, b):
        return x * ny * nz + b

    def everywhere(dx, dz):
        return [
            (number(x, y * nz + z), number(x ^ dx, y * nz + (z ^ dz)))
            for x in range(nx) for y in range(ny) for z in range(nz)
        ]

    def side(x, b):
        return x ^ (b % nz)

    chain = []
    for b in range(1, ny * nz):
        left = [x for x in range(nx) if side(x, b - 1) == 1][0]
        right = [x for x in range(nx) if side(x, b) == 0][0]
        chain += [(number(left, b - 1), number(right, b)), (number(right, b), number(left, b - 1))]

    sds = lambda *s: jax.ShapeDtypeStruct(s, f32)
    held = lambda *s: pltpu.VMEM(s, f32)
    keep = lambda x: pltpu.with_memory_space_constraint(x, pltpu.VMEM)
    there = lambda x: pltpu.with_memory_space_constraint(x, pltpu.HBM)
    count = traits.shape[1]
    entries = traits.size + intensity.size
    groups = LANES // full
    deep = layers // groups
    mid = width // 2
    wide = mid + HALO
    own, to_partner, to_beside, to_across, table = pl.pallas_call(
        pack_rows_kernel,
        out_shape=(
            held(3, deep // 2, width, LANES), held(3, deep // 2, wide, LANES),
            held(3, deep // 2, HALO, LANES), held(3, deep // 2, HALO, LANES),
            held(entries, 8, LANES),
        ),
        in_specs=[smem(), smem(), vmem(), vmem(), vmem()],
        out_specs=(vmem(),) * 5,
        compiler_params=params(),
        name="pack_rows",
    )(there(traits), there(intensity), there(temp), there(label), there(patch))
    own, table = keep(own), keep(table)
    strip = lax.ppermute(to_across, AXES, everywhere(1, 0))
    got = lax.ppermute(to_partner, AXES, everywhere(1, 0))
    beside = lax.ppermute(jnp.stack([to_beside, strip]), AXES, chain)
    got, beside = keep(got), keep(beside)

    span = mid + 2 * HALO
    edged = (deep + 2, span + 2 * PAD, LANES)
    plain = (deep, span, LANES)
    padded = pltpu.VMEM(edged, f32)
    flat = pltpu.VMEM(plain, f32)
    vectors = pltpu.VMEM((3,) + edged, f32)
    packed = pltpu.VMEM((6, deep, mid, LANES), f32)
    first = pl.pallas_call(
        functools.partial(first_kernel, count=count, full=full),
        out_shape=(
            held(*plain), held(6, *plain), held(span, LANES), held(3, *edged), held(3, *edged),
            held(3, 8, LANES),
        ) + tuple(held(k, mid, LANES) for k in (8, 8, 6, 6)),
        in_specs=[vmem()] * 4,
        out_specs=(vmem(),) * 10,
        scratch_shapes=[
            padded, padded, padded, flat, flat,
            pltpu.VMEM((deep + 1, span, LANES), f32),
            pltpu.VMEM((deep, span + 2 * PAD, LANES), f32), flat, flat,
            flat, padded, padded, vectors, vectors,
            packed, pltpu.VMEM((deep, mid, LANES), f32), padded,
            pltpu.VMEM((2, 3 * (deep // 2), span, LANES), f32),
            pltpu.VMEM((3 * deep, span, LANES), f32),
        ],
        compiler_params=params(),
        name="first",
    )(table, own, got, beside)
    carried, early = first[:6], first[6:]

    def exchanged(mine, *pieces):
        moved = [mine]
        for (dx, dz), piece in zip(((1, 0), (0, 1), (1, 1)), pieces):
            moved.append(lax.ppermute(piece, AXES, everywhere(dx, dz)))
        return tuple(keep(x) for x in moved)

    early = exchanged(*early)
    second = pl.pallas_call(
        functools.partial(second_kernel, full=full),
        out_shape=(held(devices, 1, LANES),)
        + tuple(held(6, mid, LANES) for _ in range(4)),
        in_specs=[vmem()] * 6,
        out_specs=(vmem(),) * 5,
        scratch_shapes=[vectors, vectors, packed],
        compiler_params=params(),
        name="second",
    )(*(keep(x) for x in carried))
    late = exchanged(*second[1:])
    mom = lax.all_to_all(second[0], AXES, 0, 0, tiled=True)
    mom = keep(mom)
    return pl.pallas_call(
        functools.partial(place_kernel, count=count, full=full),
        out_shape=(
            sds(layers, rows, width),
            sds(3, half, rows, nz * width),
            sds(3, half, rows, nz * width),
        ),
        in_specs=[vmem()] * 10,
        out_specs=(vmem(),) * 3,
        scratch_shapes=[pltpu.VMEM((14, width, LANES), f32)],
        compiler_params=params(),
        name="place",
    )(table, mom, *early, *late)


def padded(value, sides, width):
    for axis, dim in sides:
        devices, length = (lax.axis_size(axis), value.shape[dim])
        up = [(i, (i + 1) % devices) for i in range(devices - 1)]
        down = [(j, i) for i, j in up]
        last = lax.slice_in_dim(value, length - width, length, axis=dim)
        initial = lax.slice_in_dim(value, 0, width, axis=dim)
        before = lax.ppermute(last, axis, up)
        after = lax.ppermute(initial, axis, down)
        value = jnp.concatenate([before, value, after], axis=dim)
    return value


def lookup(identity, table, count):
    summed = jnp.zeros(identity.shape, jnp.float32)
    for number in range(count):
        summed = summed + jnp.where(identity == number, table[number], jnp.float32(0.0))
    return summed


def heat_step(padded_temp, padded_cond, power, inverse_cap):
    centre = padded_temp[:, 1:-1, 1:-1]
    own = padded_cond[:, 1:-1, 1:-1]
    layers, rows, columns = centre.shape
    heat_flux = jnp.zeros_like(centre)
    for row_offset, column_offset in ((0, 1), (2, 1), (1, 0), (1, 2)):
        neighbour = padded_temp[
            :, row_offset : row_offset + rows, column_offset : column_offset + columns
        ]
        other = padded_cond[
            :, row_offset : row_offset + rows, column_offset : column_offset + columns
        ]
        heat_flux = heat_flux + conduct(own, other) * (neighbour - centre)
    vertical_temp = jnp.pad(centre, ((1, 1), (0, 0), (0, 0)))
    vertical_cond = jnp.pad(own, ((1, 1), (0, 0), (0, 0)))
    for layer_offset in (0, 2):
        other = vertical_cond[layer_offset : layer_offset + layers]
        neighbour = vertical_temp[layer_offset : layer_offset + layers]
        heat_flux = heat_flux + conduct(own, other) * (neighbour - centre)
    return centre + time_step * inverse_cap * (heat_flux + power)


def neighbour_offsets():
    listed = []
    for along_z in (-1, 0, 1):
        for along_x in (-1, 0, 1):
            for along_y in (-1, 0, 1):
                if along_z != 0 or along_x != 0 or along_y != 0:
                    listed.append((along_z, along_x, along_y))
    return listed


def apply_operator(field, padded_field, modulus, padded_modulus):
    layers, rows, columns = modulus.shape
    parts = [
        anchor_scale * modulus * field[0],
        anchor_scale * modulus * field[1],
        anchor_scale * modulus * field[2],
    ]
    for along_z, along_x, along_y in neighbour_offsets():
        length_sq = along_z * along_z + along_x * along_x + along_y * along_y
        window = (
            slice(1 + along_z, 1 + along_z + layers),
            slice(1 + along_x, 1 + along_x + rows),
            slice(1 + along_y, 1 + along_y + columns),
        )
        weight = 0.5 / length_sq * (modulus + padded_modulus[window])
        change = [field[index_c] - padded_field[index_c][window] for index_c in range(3)]
        projected = (along_z * change[0] + along_x * change[1] + along_y * change[2]) / length_sq
        for index_c, direction_part in enumerate((along_z, along_x, along_y)):
            parts[index_c] = parts[index_c] + weight * (
                0.5 * change[index_c] + direction_part * projected
            )
    return jnp.stack(parts)


def thermal_load(modulus, padded_modulus, strain, padded_strain):
    layers, rows, columns = modulus.shape
    parts = [jnp.zeros_like(modulus), jnp.zeros_like(modulus), jnp.zeros_like(modulus)]
    for along_z, along_x, along_y in neighbour_offsets():
        length_sq = along_z * along_z + along_x * along_x + along_y * along_y
        window = (
            slice(1 + along_z, 1 + along_z + layers),
            slice(1 + along_x, 1 + along_x + rows),
            slice(1 + along_y, 1 + along_y + columns),
        )
        weight = 0.5 / length_sq * (modulus + padded_modulus[window])
        pushing = weight * (0.5 * (strain + padded_strain[window]))
        for index_c, direction_part in enumerate((along_z, along_x, along_y)):
            if direction_part != 0:
                parts[index_c] = parts[index_c] - strain_gain * direction_part * pushing
    return jnp.stack(parts)


def two_products(residual, image):
    return lax.psum((jnp.sum(residual * residual), jnp.sum(residual * image)), ("gx", "gy", "gz"))


def per_device_plain(
    starting_kelvin, substance_label, voxel_source_patch, substance_traits, patch_source_intensity
):
    count = substance_traits.shape[1]
    diffusive_coefficient = lookup(substance_label, substance_traits[0], count)
    inverse_cap = 1.0 / lookup(substance_label, substance_traits[1], count)
    power = lookup(voxel_source_patch, patch_source_intensity, patch_source_intensity.shape[0])
    padded_array = padded(
        jnp.stack([starting_kelvin, diffusive_coefficient]), (("gx", 2), (("gy", "gz"), 3)), 1
    )
    padded_cond = padded_array[1]
    warmed_result = heat_step(padded_array[0], padded_cond, power, inverse_cap)
    number = 0
    extended = padded(warmed_result, (("gx", 1), (("gy", "gz"), 2)), 1)
    warmed_result = heat_step(extended, padded_cond, power, inverse_cap)
    modulus = lookup(substance_label, substance_traits[2], count)
    strain = lookup(substance_label, substance_traits[3], count) * warmed_result
    fields = jnp.stack([modulus, strain])
    vertical_cycle = ((0, 0), (1, 1), (0, 0), (0, 0))
    padded_fields = jnp.pad(padded(fields, (("gx", 2), (("gy", "gz"), 3)), 1), vertical_cycle)

    def extend(field):
        return jnp.pad(padded(field, (("gx", 2), (("gy", "gz"), 3)), 1), vertical_cycle)

    modulus = fields[0]
    padded_modulus = padded_fields[0]
    load = thermal_load(modulus, padded_modulus, fields[1], padded_fields[1])

    def operate(field):
        return apply_operator(field, extend(field), modulus, padded_modulus)

    solution = jnp.zeros_like(load)
    residual = load
    image = operate(residual)
    norm_now, product = two_products(residual, image)
    alpha = norm_now / product
    direction, along_image = (residual, image)
    for number in range(ITERS):
        solution = solution + alpha * direction
        residual = residual - alpha * along_image
        if number + 1 < ITERS:
            image = operate(residual)
            norm_next, product = two_products(residual, image)
            ratio = norm_next / norm_now
            alpha = norm_next / (product - ratio * norm_next / alpha)
            direction = residual + ratio * direction
            along_image = image + ratio * along_image
            norm_now = norm_next
    joined = lax.all_to_all(
        jnp.concatenate([solution, residual]), "gz", split_axis=1, concat_axis=3, tiled=True
    )
    solution = joined[:3]
    residual = joined[3:]
    return (warmed_result, solution, residual)


def solution(mesh):
    in_specs = (
        P(None, "gx", ("gy", "gz")),
        P(None, "gx", ("gy", "gz")),
        P(None, "gx", ("gy", "gz")),
        P(),
        P(),
    )
    out_specs = (P(None, "gx", ("gy", "gz")), P(None, "gz", "gx", "gy"), P(None, "gz", "gx", "gy"))

    def per_device(temp, label, patch, traits, intensity):
        layers, rows, width = temp.shape
        fits = (
            mesh.shape["gx"] == 2
            and mesh.shape["gz"] == 2
            and width == LANES
            and rows % 8 == 0
            and LANES == 4 * 2 * rows
            and layers == 4 * 4
        )
        run = per_device_fast if fits else per_device_plain
        return run(temp, label, patch, traits, intensity)

    return jax.shard_map(
        per_device, mesh=mesh, in_specs=in_specs, out_specs=out_specs, check_vma=False
    )
```

```python
import functools

import jax
import jax.numpy as jnp
from jax import lax
from jax.experimental import pallas as pl
from jax.experimental.pallas import tpu as pltpu
from jax.sharding import PartitionSpec as P


ITERS = 3
HALO = 8
LANES = 128
PAD = 8
AXES = ("gx", "gy", "gz")

time_step = 0.03
anchor_scale = 0.5
strain_gain = 2.0
CENTRE = 55.0 / 9.0
K4 = 4.0 * (anchor_scale + CENTRE)

f32 = jnp.float32


def position():
    gx, gy, gz = (lax.axis_index(a) for a in AXES)
    ny, nz = lax.axis_size("gy"), lax.axis_size("gz")
    pos = gx ^ gz
    block = gy * nz + gz
    edge = jnp.where(pos == 0, 0, ny * nz - 1)
    return gx, gz, pos, block != edge


def lane_of(shape):
    return lax.broadcasted_iota(jnp.int32, shape, 1)


def pack_rows_kernel(
    traits, intensity, temp, label, patch, block, out, beside, across, table
):
    layers, rows, width = temp.shape
    groups = LANES // (2 * rows)
    deep = layers // groups
    pos = position()[2]
    kinds, count = traits.shape
    for k in range(kinds):
        for m in range(count):
            table[k * count + m] = jnp.full((8, LANES), traits[k, m], f32)
    for k in range(intensity.shape[0]):
        table[kinds * count + k] = jnp.full((8, LANES), intensity[k], f32)
    wide = width // 2 + HALO
    inner = pl.multiple_of((width - wide) * (1 - pos), 8)
    near = pl.multiple_of((width - HALO) * pos, 8)
    far = pl.multiple_of((width - HALO) * (1 - pos), 8)
    for a, ref in enumerate((temp, label, patch)):
        for p in range(deep // 2):
            parts = [ref[g * deep + 2 * p + j] for g in range(groups) for j in range(2)]
            block[a, p] = jnp.concatenate(parts, axis=0).astype(f32).T
            out[a, p] = block[a, p, pl.ds(inner, wide), :]
            beside[a, p] = block[a, p, pl.ds(near, HALO), :]
            across[a, p] = block[a, p, pl.ds(far, HALO), :]


def picks(ref, l, row):
    def at(dz, dx):
        return ref[l + 1 + dz, PAD + row + dx : PAD + row + dx + 8, :]

    out = {}
    for dx in (-1, 0, 1):
        up, mid, down = at(1, dx), at(0, dx), at(-1, dx)
        out["F", dx] = mid
        out["G", dx] = up + down
        out["H", dx] = up - down
    res = {}
    for k in "FGH":
        res[k] = out[k, 0]
        res["E" + k] = out[k, 1] + out[k, -1]
        res["D" + k] = out[k, 1] - out[k, -1]
    return res


def next_row(x, full):
    kept = lane_of(x.shape) % full != full - 1
    return jnp.where(kept, pltpu.roll(x, LANES - 1, 1), 0.0)


def last_row(x, full):
    kept = lane_of(x.shape) % full != 0
    return jnp.where(kept, pltpu.roll(x, 1, 1), 0.0)


def pair_sum(x, full):
    return next_row(x, full) + last_row(x, full)


def pair_difference(x, full):
    return next_row(x, full) - last_row(x, full)


def along_lanes(base, even, odd, full):
    return base + next_row(even + odd, full) + last_row(even - odd, full)


def wrap_layers(refs, full):
    for ref in refs:
        deep, height = ref.shape[-3] - 2, ref.shape[-2]
        for index in ([()] if len(ref.shape) == 3 else [(c,) for c in range(ref.shape[0])]):
            for r in range(PAD, height - PAD, 8):
                here = (slice(r, r + 8), slice(None))
                group = lane_of((8, LANES)) // full
                below = pltpu.roll(ref[index + (deep,) + here], full, 1)
                ref[index + (0,) + here] = jnp.where(group == 0, 0.0, below)
                above = pltpu.roll(ref[index + (1,) + here], LANES - full, 1)
                ref[index + (deep + 1,) + here] = jnp.where(
                    group == LANES // full - 1, 0.0, above
                )


N5 = 5.0 / 9.0
N2 = 2.0 / 9.0
N3 = 1.0 / 3.0


def full_stencil(z, x, y, full):
    base0 = z["EF"] + z["EG"] + 3.0 * z["G"] + 0.5 * x["DH"]
    even0 = z["F"] + z["G"] + 0.5 * z["EF"] + N5 * z["EG"] + N2 * x["DH"]
    odd0 = 0.5 * y["H"] + N2 * y["EH"]
    base1 = 3.0 * x["EF"] + x["G"] + x["EG"] + 0.5 * z["DH"]
    even1 = x["F"] + x["EF"] + 0.5 * x["G"] + N5 * x["EG"] + N2 * z["DH"]
    odd1 = 0.5 * y["DF"] + N2 * y["DG"]
    shared = y["EF"] + y["G"]
    base2 = shared + 0.5 * y["EG"]
    even2 = shared + 3.0 * y["F"] + N5 * y["EG"]
    odd2 = 0.5 * (x["DF"] + z["H"]) + N2 * (x["DG"] + z["EH"])
    return (
        along_lanes(base0, even0, odd0, full),
        along_lanes(base1, even1, odd1, full),
        along_lanes(base2, even2, odd2, full),
    )


def matrix_stencil(m, full):
    both = m["EF"] + m["EG"]
    shared = m["EF"] + m["G"]
    tail = N5 * m["EG"]
    zz = both + 3.0 * m["G"] + pair_sum(m["F"] + m["G"] + 0.5 * m["EF"] + tail, full)
    xx = 3.0 * m["EF"] + m["G"] + m["EG"] + pair_sum(m["F"] + m["EF"] + 0.5 * m["G"] + tail, full)
    yy = shared + 0.5 * m["EG"] + pair_sum(shared + 3.0 * m["F"] + tail, full)
    zx = 0.5 * m["DH"] + pair_sum(N2 * m["DH"], full)
    zy = pair_difference(0.5 * m["H"] + N2 * m["EH"], full)
    xy = pair_difference(0.5 * m["DF"] + N2 * m["DG"], full)
    return zz, xx, yy, zx, zy, xy


def gradient_stencil(f, full):
    gz = f["H"] + 0.5 * f["EH"] + pair_sum(0.5 * f["H"] + N3 * f["EH"], full)
    gx = f["DF"] + 0.5 * f["DG"] + pair_sum(0.5 * f["DF"] + N3 * f["DG"], full)
    gy = pair_difference(f["F"] + 0.5 * (f["G"] + f["EF"]) + N3 * f["EG"], full)
    return gz, gx, gy


def conduct(own, other):
    return 2.0 * own * other / jnp.maximum(own + other, 0.25)


def choose(label, values):
    out = jnp.zeros(label.shape, f32)
    for k, v in enumerate(values):
        out = jnp.where(label == float(k), v, out)
    return out


def shift_scale(table, count):
    total = table[2 * count]
    for k in range(1, count):
        total = total + table[2 * count + k]
    return total * ((anchor_scale + 2.0 * CENTRE) / count)


def exchanged_lanes(x, y, distance, swap):
    low = (lane_of(x.shape) // distance) % 2 == 0
    y_up = pltpu.roll(y, distance, 1)
    x_down = pltpu.roll(x, LANES - distance, 1)
    first = jnp.where(low, x, y_up)
    second = jnp.where(low, x_down, y)
    return jnp.where(swap, second, first), jnp.where(swap, first, second)


def owner_lanes(values, rows, swap_rows, swap_layers):
    wide = LANES // 2
    a = exchanged_lanes(values[0], values[2], wide, swap_layers)
    b = exchanged_lanes(values[1], values[3], wide, swap_layers)
    return [exchanged_lanes(x, y, rows, swap_rows) for x, y in zip(a, b)]


def packer(v, outs, warm, full):
    deep = v.shape[1]
    rows = full // 2
    gx, gz, _, _ = position()
    shape = (8, LANES)
    swap_rows = jnp.broadcast_to(gx, shape) == 1
    swap_layers = jnp.broadcast_to(gz, shape) == 1
    never = jnp.zeros(shape, jnp.bool_)

    def pack(fields, r, with_warm):
        here = pl.ds(r, 8)
        for f in fields:
            made = owner_lanes(
                [v[f, i, here, :] for i in range(deep)], rows, swap_rows, swap_layers
            )
            for number, out in enumerate(outs):
                out[f, here, :] = made[number // 2][number % 2]
        if with_warm:
            made = owner_lanes([warm[i, here, :] for i in range(deep)], rows, swap_rows, never)
            for number in range(2):
                for layer_half in range(2):
                    outs[number][v.shape[0] + layer_half, here, :] = made[layer_half][number]

    return pack


def pack_all(pack, fields, own):
    def step(t, _):
        pack(fields, pl.multiple_of(8 * t, 8), False)
        return 0

    lax.fori_loop(0, own // 8, step, 0, unroll=4)


def power_step(weight, mats, inside, source, dest, v, first_field, square_too, full, beside):
    u, w = source
    deep, width = mats.shape[1], mats.shape[2]
    own = range(HALO, width - HALO, 8)
    tiles = own if dest is None else range(0, width, 8)

    def step(l, accs):
        accs = list(accs)
        if beside is not None:
            beside(l)
        for r in tiles:
            here = slice(PAD + r, PAD + r + 8)
            there = slice(r, r + 8)
            found, stencils = [], []
            for ref in (u, w):
                f = [picks(ref.at[c], l, r) for c in range(3)]
                found.append([x["F"] for x in f])
                stencils.append(full_stencil(*f, full))
            old, weighted = found
            cu, cw = stencils
            zz, xx, yy, zx, zy, xy = (mats[k, l, there, :] for k in range(6))
            mixed = (
                zz * old[0] + zx * old[1] + zy * old[2],
                zx * old[0] + xx * old[1] + xy * old[2],
                zy * old[0] + xy * old[1] + yy * old[2],
            )
            m = weight[l, there, :]
            keep = inside[there, :]
            for c in range(3):
                new = (K4 * weighted[c] + mixed[c] - m * cu[c] - cw[c]) * keep
                if dest is not None:
                    dest[0][c, l + 1, here, :] = new
                    dest[1][c, l + 1, here, :] = new * m
                if r in own:
                    v[first_field + c, l, r - HALO : r - HALO + 8, :] = new
                    accs[0] = accs[0] + new * old[c]
                    if square_too:
                        accs[1] = accs[1] + new * new
        return tuple(accs)

    zero = jnp.zeros((8, LANES), f32)
    accs = lax.fori_loop(0, deep, step, (zero,) * (2 if square_too else 1))
    if dest is not None:
        wrap_layers(dest, full)
    return accs


def clear_edges(refs):
    edge = jnp.zeros((PAD, LANES), f32)
    for ref in refs:
        height = ref.shape[-2]
        for index in ([()] if len(ref.shape) == 3 else [(c,) for c in range(ref.shape[0])]):
            for l in range(ref.shape[-3]):
                ref[index + (l, slice(0, PAD))] = edge
                ref[index + (l, slice(height - PAD, height))] = edge


def first_kernel(
    table, block, got, near_strip, far_strip,
    weight, mats, inside, u_next, w_next, moments, mine, to_x, to_z, to_both,
    cond, temp_a, temp_b, cap, power, gz, gx, gy, gy_back, expand, strain, prod, u, w, v, warm,
    mod, source, win,
    *, count, full,
):
    pairs, wide = got.shape[1], got.shape[2]
    deep, width = mats.shape[1], mats.shape[2]
    rows = full // 2
    me, _, pos, paired = position()
    tiles = range(0, width, 8)
    kinds = 4
    sources = table.shape[0] - kinds * count

    inv_scale = 1.0 / shift_scale(table, count)
    cond_t = [table[k] for k in range(count)]
    cap_t = [time_step / table[count + k] for k in range(count)]
    mod_t = [table[2 * count + k] for k in range(count)]
    exp_t = [table[3 * count + k] for k in range(count)]
    pow_t = [table[kinds * count + k] for k in range(sources)]

    clear_edges((cond, temp_a, temp_b, mod, strain, prod, u, w, u_next, w_next))
    for l in range(deep):
        gx[l, 0:PAD] = jnp.zeros((PAD, LANES), f32)

    body = pl.multiple_of(HALO * (1 - pos), 8)
    strip = pl.multiple_of((width - HALO) * pos, 8)
    inner = pl.multiple_of((block.shape[2] - wide) * pos, 8)
    for a in range(3):
        for p in range(pairs):
            source[me, a * pairs + p, pl.ds(body, wide), :] = block[a, p, pl.ds(inner, wide), :]
            source[1 - me, a * pairs + p, pl.ds(body, wide), :] = got[a, p]
            for half, ref in ((me, near_strip), (1 - me, far_strip)):
                value = ref[a, p]
                if a == 1:
                    value = jnp.where(paired, value, -1.0)
                source[half, a * pairs + p, pl.ds(strip, HALO), :] = value

    def window(k, _):
        low = (lane_of((8, LANES)) // rows) % 2 == 0
        for r in tiles:
            x, y = source[0, k, r : r + 8, :], source[1, k, r : r + 8, :]
            win[2 * k, r : r + 8, :] = jnp.where(low, x, pltpu.roll(y, rows, 1))
            win[2 * k + 1, r : r + 8, :] = jnp.where(low, pltpu.roll(x, LANES - rows, 1), y)
        return 0

    lax.fori_loop(0, 3 * pairs, window, 0, unroll=2)

    def looked_up(l, _):
        for r in tiles:
            here = slice(PAD + r, PAD + r + 8)
            there = slice(r, r + 8)
            temp_a[l + 1, here, :] = win[l, there, :]
            lab = win[deep + l, there, :]
            src = win[2 * deep + l, there, :]
            cond[l + 1, here, :] = choose(lab, cond_t)
            cap[l, there, :] = choose(lab, cap_t)
            mod[l + 1, here, :] = choose(lab, mod_t)
            expand[l, there, :] = choose(lab, exp_t)
            power[l, there, :] = choose(src, pow_t)
            inside[there, :] = jnp.where(lab >= 0.0, 1.0, 0.0)
        return 0

    lax.fori_loop(0, deep, looked_up, 0)
    wrap_layers((temp_a, cond, mod), full)

    for r in tiles:
        here = slice(PAD + r, PAD + r + 8)
        gz[0, r : r + 8, :] = conduct(cond[0, here, :], cond[1, here, :])

    def faces(l, _):
        for r in tiles:
            here = slice(PAD + r, PAD + r + 8)
            there = slice(r, r + 8)
            a = cond[l + 1, here, :]
            gz[l + 1, there, :] = conduct(a, cond[l + 2, here, :])
            gx[l, here, :] = conduct(a, cond[l + 1, PAD + r + 1 : PAD + r + 9, :])
            gy[l, there, :] = conduct(a, next_row(a, full))
            gy_back[l, there, :] = conduct(a, last_row(a, full))
        return 0

    lax.fori_loop(0, deep, faces, 0)

    def heat(src, dst, last):
        def step(l, _):
            for r in tiles:
                here = slice(PAD + r, PAD + r + 8)
                there = slice(r, r + 8)
                t = src[l + 1, here, :]
                flux = gz[l + 1, there, :] * (src[l + 2, here, :] - t)
                flux += gz[l, there, :] * (src[l, here, :] - t)
                flux += gx[l, here, :] * (src[l + 1, PAD + r + 1 : PAD + r + 9, :] - t)
                flux += gx[l, PAD + r - 1 : PAD + r + 7, :] * (
                    src[l + 1, PAD + r - 1 : PAD + r + 7, :] - t
                )
                flux += gy[l, there, :] * (pltpu.roll(t, LANES - 1, 1) - t)
                flux += gy_back[l, there, :] * (pltpu.roll(t, 1, 1) - t)
                new = t + cap[l, there, :] * (flux + power[l, there, :])
                if last:
                    if HALO <= r < width - HALO:
                        warm[l, r - HALO : r - HALO + 8, :] = new
                    s = expand[l, there, :] * new
                    strain[l + 1, here, :] = s
                    prod[l + 1, here, :] = s * mod[l + 1, here, :]
                else:
                    dst[l + 1, here, :] = new
            return 0

        lax.fori_loop(0, deep, step, 0, unroll=4)

    heat(temp_a, temp_b, False)
    wrap_layers((temp_b,), full)
    heat(temp_b, None, True)
    wrap_layers((strain, prod), full)

    quarter_scale = 0.25 * inv_scale

    def loads(l, acc):
        for r in tiles:
            here = slice(PAD + r, PAD + r + 8)
            there = slice(r, r + 8)
            s = picks(strain, l, r)
            m = picks(mod, l, r)
            q = picks(prod, l, r)
            gs, gm, gq = (gradient_stencil(f, full) for f in (s, m, q))
            for k, entry in enumerate(matrix_stencil(m, full)):
                entry = entry * quarter_scale
                mats[k, l, there, :] = entry - 1.0 if k < 3 else entry
            scaled = m["F"] * quarter_scale
            weight[l, there, :] = scaled
            keep = inside[there, :] * (-0.25 * strain_gain)
            for c in range(3):
                new = (m["F"] * gs[c] + s["F"] * gm[c] + gq[c]) * keep
                u[c, l + 1, here, :] = new
                w[c, l + 1, here, :] = new * scaled
                if HALO <= r < width - HALO:
                    v[c, l, r - HALO : r - HALO + 8, :] = new
                    acc = acc + new * new
        return acc

    moments[0] = lax.fori_loop(0, deep, loads, jnp.zeros((8, LANES), f32))
    wrap_layers((u, w), full)
    pack = packer(v, (mine, to_x, to_z, to_both), warm, full)
    own = v.shape[2]
    share = own // (8 * deep)

    def beside(l):
        for k in range(share):
            pack(range(3), pl.multiple_of((l * share + k) * 8, 8), True)

    cross, square = power_step(
        weight, mats, inside, (u, w), (u_next, w_next), v, 3, True, full, beside
    )
    moments[1] = cross
    moments[2] = square
    pack_all(pack, range(3, 6), own)


def second_kernel(
    weight, mats, inside, u, w, moments,
    mom_out, mine, to_x, to_z, to_both,
    u_next, w_next, v,
    *, full,
):
    clear_edges((u_next, w_next))
    parts = [moments[k] for k in range(moments.shape[0])]
    parts += power_step(
        weight, mats, inside, (u, w), (u_next, w_next), v, 0, True, full, None
    )
    pack = packer(v, (mine, to_x, to_z, to_both), None, full)
    own = v.shape[2]
    share = own // (8 * mats.shape[1])

    def beside(l):
        for k in range(share):
            pack(range(3), pl.multiple_of((l * share + k) * 8, 8), False)

    parts += power_step(
        weight, mats, inside, (u_next, w_next), None, v, 3, False, full, beside
    )
    lane1 = lane_of((1, LANES))
    row = jnp.zeros((1, LANES), f32)
    for k, part in enumerate(parts):
        lanes = jnp.sum(part, axis=0, keepdims=True)
        row = jnp.where(lane1 == k, jnp.sum(lanes, axis=1, keepdims=True), row)
    for k in range(mom_out.shape[0]):
        mom_out[k] = row
    pack_all(pack, range(3, 6), own)


def coefficients(mu, scale):
    def inner(a, b):
        total = None
        for i, x in enumerate(a):
            for j, y in enumerate(b):
                term = x * y * mu[i + j]
                total = term if total is None else total + term
        return total

    def added(a, b):
        out = []
        for k in range(max(len(a), len(b))):
            if k >= len(a):
                out.append(b[k])
            elif k >= len(b):
                out.append(a[k])
            else:
                out.append(a[k] + b[k])
        return out

    one = jnp.ones_like(mu[0])
    residual = [one]
    direction = [one]
    solution = []
    norm = mu[0]
    for number in range(ITERS):
        image = added(direction, [jnp.zeros_like(one)] + direction)
        alpha = norm / inner(direction, image)
        solution = added(solution, [alpha * d for d in direction])
        residual = added(residual, [-alpha * d for d in image])
        if number + 1 < ITERS:
            following = inner(residual, residual)
            ratio = following / norm
            direction = added(residual, [ratio * d for d in direction])
            norm = following
    return [s / scale for s in solution], residual


def place_kernel(table, mom, *refs, count, full):
    early, late, outs, board = refs[:4], refs[4:8], refs[8:11], refs[11]
    warm_out, sol_out, res_out = outs
    layers, rows, _ = warm_out.shape
    deep = layers // (LANES // full)
    own = early[2].shape[1]
    _, gz, pos, _ = position()
    shape = (8, LANES)
    total = jnp.broadcast_to(jnp.sum(mom[:, 0, :], axis=0, keepdims=True), shape)
    mu = []
    for k in range(2 * ITERS):
        picked = jnp.where(lane_of(shape) == k, total, 0.0)
        mu.append(jnp.broadcast_to(jnp.sum(picked, axis=1, keepdims=True), shape))
    sol, res = coefficients(mu, shift_scale(table, count))

    def spread(slot, out, lanes, layer0):
        turned = board[slot].T
        for i in range(deep):
            for g in range(2):
                at = (i // 2) * (LANES // 2) + g * full + (i % 2) * rows
                out[layer0 + g * deep + i, :, lanes] = turned[at : at + rows]

    for half in range(2):
        for number in range(2):
            at = pl.multiple_of((pos ^ number) * own, own)
            board[half, pl.ds(at, own), :] = early[number][6 + half]
        spread(half, warm_out, slice(None), half * (layers // 2))
    slot = 2
    for block in range(2):
        lanes = pl.ds(pl.multiple_of((gz ^ block) * LANES, LANES), LANES)
        for c in range(3):
            for number in range(2):
                a, b = early[2 * block + number], late[2 * block + number]
                at = pl.multiple_of((pos ^ block ^ number) * own, own)
                for r in range(0, own, 8):
                    there = slice(r, r + 8)
                    values = (a[c, there, :], a[3 + c, there, :], b[c, there, :], b[3 + c, there, :])
                    x = sol[0] * values[0]
                    y = res[0] * values[0]
                    for k in range(1, ITERS + 1):
                        if k < ITERS:
                            x = x + sol[k] * values[k]
                        y = y + res[k] * values[k]
                    board[slot, pl.ds(at + r, 8), :] = x
                    board[slot + 1, pl.ds(at + r, 8), :] = y
            spread(slot, sol_out.at[(0, 2, 1)[c]], lanes, 0)
            spread(slot + 1, res_out.at[(0, 2, 1)[c]], lanes, 0)
            slot += 2


LIMIT = 28 * 1024 * 1024


def params():
    return pltpu.CompilerParams(vmem_limit_bytes=LIMIT)


def vmem():
    return pl.BlockSpec(memory_space=pltpu.VMEM)


def smem():
    return pl.BlockSpec(memory_space=pltpu.SMEM)


def per_device_fast(temp, label, patch, traits, intensity):
    nx, ny, nz = (lax.axis_size(a) for a in AXES)
    layers, rows, width = temp.shape
    full = rows * nx
    half = layers // 2
    devices = nx * ny * nz

    def number(x, b):
        return x * ny * nz + b

    def everywhere(dx, dz):
        return [
            (number(x, y * nz + z), number(x ^ dx, y * nz + (z ^ dz)))
            for x in range(nx) for y in range(ny) for z in range(nz)
        ]

    def side(x, b):
        return x ^ (b % nz)

    chain = []
    for b in range(1, ny * nz):
        left = [x for x in range(nx) if side(x, b - 1) == 1][0]
        right = [x for x in range(nx) if side(x, b) == 0][0]
        chain += [(number(left, b - 1), number(right, b)), (number(right, b), number(left, b - 1))]

    cross = []
    for x in range(nx):
        for b in range(ny * nz):
            toward = b - 1 if side(x, b) == 0 else b + 1
            if 0 <= toward < ny * nz:
                cross.append((number(x ^ 1, toward), number(x, b)))

    sds = lambda *s: jax.ShapeDtypeStruct(s, f32)
    held = lambda *s: pltpu.VMEM(s, f32)
    keep = lambda x: pltpu.with_memory_space_constraint(x, pltpu.VMEM)
    there = lambda x: pltpu.with_memory_space_constraint(x, pltpu.HBM)
    count = traits.shape[1]
    entries = traits.size + intensity.size
    groups = LANES // full
    deep = layers // groups
    mid = width // 2
    wide = mid + HALO
    own, to_partner, to_beside, to_across, table = pl.pallas_call(
        pack_rows_kernel,
        out_shape=(
            held(3, deep // 2, width, LANES), held(3, deep // 2, wide, LANES),
            held(3, deep // 2, HALO, LANES), held(3, deep // 2, HALO, LANES),
            held(entries, 8, LANES),
        ),
        in_specs=[smem(), smem(), vmem(), vmem(), vmem()],
        out_specs=(vmem(),) * 5,
        compiler_params=params(),
        name="pack_rows",
    )(there(traits), there(intensity), there(temp), there(label), there(patch))
    own, table = keep(own), keep(table)
    got = lax.ppermute(to_partner, AXES, everywhere(1, 0))
    across = lax.ppermute(to_across, AXES, cross)
    beside = lax.ppermute(to_beside, AXES, chain)
    got, across, beside = keep(got), keep(across), keep(beside)

    span = mid + 2 * HALO
    edged = (deep + 2, span + 2 * PAD, LANES)
    plain = (deep, span, LANES)
    padded = pltpu.VMEM(edged, f32)
    flat = pltpu.VMEM(plain, f32)
    vectors = pltpu.VMEM((3,) + edged, f32)
    packed = pltpu.VMEM((6, deep, mid, LANES), f32)
    first = pl.pallas_call(
        functools.partial(first_kernel, count=count, full=full),
        out_shape=(
            held(*plain), held(6, *plain), held(span, LANES), held(3, *edged), held(3, *edged),
            held(3, 8, LANES),
        ) + tuple(held(k, mid, LANES) for k in (8, 8, 6, 6)),
        in_specs=[vmem()] * 5,
        out_specs=(vmem(),) * 10,
        scratch_shapes=[
            padded, padded, padded, flat, flat,
            pltpu.VMEM((deep + 1, span, LANES), f32),
            pltpu.VMEM((deep, span + 2 * PAD, LANES), f32), flat, flat,
            flat, padded, padded, vectors, vectors,
            packed, pltpu.VMEM((deep, mid, LANES), f32), padded,
            pltpu.VMEM((2, 3 * (deep // 2), span, LANES), f32),
            pltpu.VMEM((3 * deep, span, LANES), f32),
        ],
        compiler_params=params(),
        name="first",
    )(table, own, got, beside, across)
    carried, early = first[:6], first[6:]

    def exchanged(mine, *pieces):
        moved = [mine]
        for (dx, dz), piece in zip(((1, 0), (0, 1), (1, 1)), pieces):
            moved.append(lax.ppermute(piece, AXES, everywhere(dx, dz)))
        return tuple(keep(x) for x in moved)

    early = exchanged(*early)
    second = pl.pallas_call(
        functools.partial(second_kernel, full=full),
        out_shape=(held(devices, 1, LANES),)
        + tuple(held(6, mid, LANES) for _ in range(4)),
        in_specs=[vmem()] * 6,
        out_specs=(vmem(),) * 5,
        scratch_shapes=[vectors, vectors, packed],
        compiler_params=params(),
        name="second",
    )(*(keep(x) for x in carried))
    late = exchanged(*second[1:])
    mom = lax.all_to_all(second[0], AXES, 0, 0, tiled=True)
    mom = keep(mom)
    return pl.pallas_call(
        functools.partial(place_kernel, count=count, full=full),
        out_shape=(
            sds(layers, rows, width),
            sds(3, half, rows, nz * width),
            sds(3, half, rows, nz * width),
        ),
        in_specs=[vmem()] * 10,
        out_specs=(vmem(),) * 3,
        scratch_shapes=[pltpu.VMEM((14, width, LANES), f32)],
        compiler_params=params(),
        name="place",
    )(table, mom, *early, *late)


def padded(value, sides, width):
    for axis, dim in sides:
        devices, length = (lax.axis_size(axis), value.shape[dim])
        up = [(i, (i + 1) % devices) for i in range(devices - 1)]
        down = [(j, i) for i, j in up]
        last = lax.slice_in_dim(value, length - width, length, axis=dim)
        initial = lax.slice_in_dim(value, 0, width, axis=dim)
        before = lax.ppermute(last, axis, up)
        after = lax.ppermute(initial, axis, down)
        value = jnp.concatenate([before, value, after], axis=dim)
    return value


def lookup(identity, table, count):
    summed = jnp.zeros(identity.shape, jnp.float32)
    for number in range(count):
        summed = summed + jnp.where(identity == number, table[number], jnp.float32(0.0))
    return summed


def heat_step(padded_temp, padded_cond, power, inverse_cap):
    centre = padded_temp[:, 1:-1, 1:-1]
    own = padded_cond[:, 1:-1, 1:-1]
    layers, rows, columns = centre.shape
    heat_flux = jnp.zeros_like(centre)
    for row_offset, column_offset in ((0, 1), (2, 1), (1, 0), (1, 2)):
        neighbour = padded_temp[
            :, row_offset : row_offset + rows, column_offset : column_offset + columns
        ]
        other = padded_cond[
            :, row_offset : row_offset + rows, column_offset : column_offset + columns
        ]
        heat_flux = heat_flux + conduct(own, other) * (neighbour - centre)
    vertical_temp = jnp.pad(centre, ((1, 1), (0, 0), (0, 0)))
    vertical_cond = jnp.pad(own, ((1, 1), (0, 0), (0, 0)))
    for layer_offset in (0, 2):
        other = vertical_cond[layer_offset : layer_offset + layers]
        neighbour = vertical_temp[layer_offset : layer_offset + layers]
        heat_flux = heat_flux + conduct(own, other) * (neighbour - centre)
    return centre + time_step * inverse_cap * (heat_flux + power)


def neighbour_offsets():
    listed = []
    for along_z in (-1, 0, 1):
        for along_x in (-1, 0, 1):
            for along_y in (-1, 0, 1):
                if along_z != 0 or along_x != 0 or along_y != 0:
                    listed.append((along_z, along_x, along_y))
    return listed


def apply_operator(field, padded_field, modulus, padded_modulus):
    layers, rows, columns = modulus.shape
    parts = [
        anchor_scale * modulus * field[0],
        anchor_scale * modulus * field[1],
        anchor_scale * modulus * field[2],
    ]
    for along_z, along_x, along_y in neighbour_offsets():
        length_sq = along_z * along_z + along_x * along_x + along_y * along_y
        window = (
            slice(1 + along_z, 1 + along_z + layers),
            slice(1 + along_x, 1 + along_x + rows),
            slice(1 + along_y, 1 + along_y + columns),
        )
        weight = 0.5 / length_sq * (modulus + padded_modulus[window])
        change = [field[index_c] - padded_field[index_c][window] for index_c in range(3)]
        projected = (along_z * change[0] + along_x * change[1] + along_y * change[2]) / length_sq
        for index_c, direction_part in enumerate((along_z, along_x, along_y)):
            parts[index_c] = parts[index_c] + weight * (
                0.5 * change[index_c] + direction_part * projected
            )
    return jnp.stack(parts)


def thermal_load(modulus, padded_modulus, strain, padded_strain):
    layers, rows, columns = modulus.shape
    parts = [jnp.zeros_like(modulus), jnp.zeros_like(modulus), jnp.zeros_like(modulus)]
    for along_z, along_x, along_y in neighbour_offsets():
        length_sq = along_z * along_z + along_x * along_x + along_y * along_y
        window = (
            slice(1 + along_z, 1 + along_z + layers),
            slice(1 + along_x, 1 + along_x + rows),
            slice(1 + along_y, 1 + along_y + columns),
        )
        weight = 0.5 / length_sq * (modulus + padded_modulus[window])
        pushing = weight * (0.5 * (strain + padded_strain[window]))
        for index_c, direction_part in enumerate((along_z, along_x, along_y)):
            if direction_part != 0:
                parts[index_c] = parts[index_c] - strain_gain * direction_part * pushing
    return jnp.stack(parts)


def two_products(residual, image):
    return lax.psum((jnp.sum(residual * residual), jnp.sum(residual * image)), ("gx", "gy", "gz"))


def per_device_plain(
    starting_kelvin, substance_label, voxel_source_patch, substance_traits, patch_source_intensity
):
    count = substance_traits.shape[1]
    diffusive_coefficient = lookup(substance_label, substance_traits[0], count)
    inverse_cap = 1.0 / lookup(substance_label, substance_traits[1], count)
    power = lookup(voxel_source_patch, patch_source_intensity, patch_source_intensity.shape[0])
    padded_array = padded(
        jnp.stack([starting_kelvin, diffusive_coefficient]), (("gx", 2), (("gy", "gz"), 3)), 1
    )
    padded_cond = padded_array[1]
    warmed_result = heat_step(padded_array[0], padded_cond, power, inverse_cap)
    number = 0
    extended = padded(warmed_result, (("gx", 1), (("gy", "gz"), 2)), 1)
    warmed_result = heat_step(extended, padded_cond, power, inverse_cap)
    modulus = lookup(substance_label, substance_traits[2], count)
    strain = lookup(substance_label, substance_traits[3], count) * warmed_result
    fields = jnp.stack([modulus, strain])
    vertical_cycle = ((0, 0), (1, 1), (0, 0), (0, 0))
    padded_fields = jnp.pad(padded(fields, (("gx", 2), (("gy", "gz"), 3)), 1), vertical_cycle)

    def extend(field):
        return jnp.pad(padded(field, (("gx", 2), (("gy", "gz"), 3)), 1), vertical_cycle)

    modulus = fields[0]
    padded_modulus = padded_fields[0]
    load = thermal_load(modulus, padded_modulus, fields[1], padded_fields[1])

    def operate(field):
        return apply_operator(field, extend(field), modulus, padded_modulus)

    solution = jnp.zeros_like(load)
    residual = load
    image = operate(residual)
    norm_now, product = two_products(residual, image)
    alpha = norm_now / product
    direction, along_image = (residual, image)
    for number in range(ITERS):
        solution = solution + alpha * direction
        residual = residual - alpha * along_image
        if number + 1 < ITERS:
            image = operate(residual)
            norm_next, product = two_products(residual, image)
            ratio = norm_next / norm_now
            alpha = norm_next / (product - ratio * norm_next / alpha)
            direction = residual + ratio * direction
            along_image = image + ratio * along_image
            norm_now = norm_next
    joined = lax.all_to_all(
        jnp.concatenate([solution, residual]), "gz", split_axis=1, concat_axis=3, tiled=True
    )
    solution = joined[:3]
    residual = joined[3:]
    return (warmed_result, solution, residual)


def solution(mesh):
    in_specs = (
        P(None, "gx", ("gy", "gz")),
        P(None, "gx", ("gy", "gz")),
        P(None, "gx", ("gy", "gz")),
        P(),
        P(),
    )
    out_specs = (P(None, "gx", ("gy", "gz")), P(None, "gz", "gx", "gy"), P(None, "gz", "gx", "gy"))

    def per_device(temp, label, patch, traits, intensity):
        layers, rows, width = temp.shape
        fits = (
            mesh.shape["gx"] == 2
            and mesh.shape["gz"] == 2
            and width == LANES
            and rows % 8 == 0
            and LANES == 4 * 2 * rows
            and layers == 4 * 4
        )
        run = per_device_fast if fits else per_device_plain
        return run(temp, label, patch, traits, intensity)

    return jax.shard_map(
        per_device, mesh=mesh, in_specs=in_specs, out_specs=out_specs, check_vma=False
    )
```
